32 devices in a mesh: node: 8 (over y, x, core), local: 4 (over z).
Axes of the slice: x: 2, y: 2, z: 4, core: 2. Of those that a mesh axis runs over, the one named last changes fastest.
Arguments:
- vit_tiles: bfloat16 [8, 4, 128, 12800], P('node', 'local'), may hold values from -6 to 6
- tile_counts: int32 [8, 1], P('node'), may hold values from 1 to 2
- block_of_piece: int32 [8, 2], P('node'), may hold values from 0 to 7, as said below
- segment_ids: int32 [8, 8, 256], P('node', None, 'local'), may hold values from 0 to 15, as said below
- text_rows: bfloat16 [8, 8, 256, 3584], P('node', None, 'local'), may hold values from -6 to 6
- cotangent: bfloat16 [8, 8, 256, 512], P('node', None, 'local'), may hold values from -6 to 6
- proj_weight: bfloat16 [12800, 3584], P('local', 'node'), may hold values from -0.0546875 to 0.0546875
- proj_bias: float32 [3584], replicated, may hold values from -3 to 3
- out_weight: bfloat16 [3584, 3584], P(None, 'local'), may hold values from -0.09375 to 0.09375
- out_bias: float32 [3584], replicated, may hold values from -3 to 3
- ln_gain: float32 [12800], replicated, may hold values from 0.25 to 1.75
- ln_bias: float32 [12800], replicated, may hold values from -2 to 2
- norm_gain: float32 [3584], replicated, may hold values from 0.25 to 1.75
- v_weight: bfloat16 [3584, 512], P(('node', 'local')), may hold values from -0.09375 to 0.09375
Outputs:
- hidden_grad: bfloat16 [8, 8, 256, 3584], P('node', None, 'local')
- value_weight_grad: float32 [3584, 512], P(('node', 'local'))
- value_bias_grad: float32 [512], replicated
- norm_gain_grad: float32 [3584], replicated
The draws below stay inside these ranges and needn't reach their ends.
Inputs may be any that keep to these rules, and one draw needn't show every extreme that they name: `block_of_piece`: within one sequence the entries are distinct. `segment_ids`: along each sequence, read block by block, the ids never fall; every sequence has exactly 16 documents.
All inputs are finite; a program needn't handle non-finite values.
Results may differ from the reference program's by a relative error of at most 0.017.
Values may be sent and summed in bfloat16 or wider, within the bound.
A program may use at most 128 MiB of HBM per device.

```python
import jax
import jax.numpy as jnp
from jax import lax

VW = 12800
D = 3584
KV = 512
TILE_TOK = 256
SLOTS = 2
BLOCKS = 8
DOCS = 16
HALF = 128
PIECES = 2
IMAGES = 1
N_NODE = 8
N_LOCAL = 4


def draw_block_of_piece(key, part):
    node_keys = jax.random.split(jax.random.fold_in(key, 11), N_NODE)

    def one_node(node_key):
        return jax.random.permutation(node_key, BLOCKS)[:PIECES].astype(jnp.int32)
    return jax.vmap(one_node)(node_keys)


def draw_segment_ids(key, part):
    node_keys = jax.random.split(jax.random.fold_in(key, 23), N_NODE)
    length = BLOCKS * TILE_TOK

    def one_node(node_key):
        starts = jax.random.permutation(node_key, length - 1)[:DOCS - 1] + 1
        boundary = jnp.zeros((length,), jnp.int32).at[starts].set(1)
        return jnp.cumsum(boundary).astype(jnp.int32).reshape(BLOCKS, TILE_TOK)
    return jax.vmap(one_node)(node_keys)


def set_ends(result, stream_key, smallest, top_value):
    shape = result.shape
    place = [jax.random.randint(jax.random.fold_in(stream_key, axis), (), 0, shape[axis]) for axis in range(len(shape))]
    result = result.at[tuple(place)].set(smallest)
    longest = shape.index(max(shape))
    place[longest] = (place[longest] + 1) % shape[longest]
    return result.at[tuple(place)].set(top_value)


def block_levels(stream_key, shape, cuts, smallest, high):
    factor_of, own = 1.0, jax.random.fold_in(stream_key, 6)
    for dim, parts in cuts:
        steps = jnp.exp(jax.random.uniform(jax.random.fold_in(own, dim), (parts,), jnp.float32, smallest / len(cuts), high / len(cuts)))
        factor_of = factor_of * jnp.repeat(steps, shape[dim] // parts).reshape([-1 if axis == dim else 1 for axis in range(len(shape))])
    return factor_of


def scatter_about(stream_key, dims, scale, most, shards=(), kind=jnp.bfloat16):
    result = jax.random.normal(stream_key, dims, jnp.float32) * scale
    if len(shards) > 0:
        result = block_levels(stream_key, dims, shards, -0.22, 0.18) * result
    return jnp.clip(result, min=-most, max=most).astype(kind)


def setup_inputs(seed: int = 0) -> dict:
    streams_of = jax.random.split(jax.random.key(seed), 15)
    return {
        "vit_tiles": scatter_about(streams_of[0], (N_NODE, N_LOCAL, HALF, VW), 1.0, 6.0, ((0, 8), (1, 4))),
        "tile_counts": set_ends(jax.random.randint(streams_of[1], (N_NODE, IMAGES), 1, SLOTS + 1), jax.random.fold_in(streams_of[1], 1), 1, SLOTS).astype(jnp.int32),
        "block_of_piece": draw_block_of_piece(jax.random.fold_in(streams_of[14], 71), 0),
        "segment_ids": draw_segment_ids(jax.random.fold_in(streams_of[14], 71), 0),
        "text_rows": scatter_about(streams_of[4], (N_NODE, BLOCKS, TILE_TOK, D), 1.0, 6.0, ((0, 8), (2, 4))),
        "cotangent": scatter_about(streams_of[5], (N_NODE, BLOCKS, TILE_TOK, KV), 1.0, 6.0, ((0, 8), (2, 4))),
        "proj_weight": scatter_about(streams_of[6], (VW, D), VW ** -0.5, 0.0546875, ((0, 4), (1, 8))),
        "proj_bias": scatter_about(streams_of[7], (D,), 0.5, 3.0, (), jnp.float32),
        "out_weight": scatter_about(streams_of[8], (D, D), D ** -0.5, 0.09375, ((1, 4),)),
        "out_bias": scatter_about(streams_of[9], (D,), 0.5, 3.0, (), jnp.float32),
        "ln_gain": jnp.clip(1.0 + 0.15 * jax.random.normal(streams_of[10], (VW,), jnp.float32), 0.25, 1.75),
        "ln_bias": scatter_about(streams_of[11], (VW,), 0.4, 2.0, (), jnp.float32),
        "norm_gain": jnp.clip(1.0 + 0.15 * jax.random.normal(streams_of[12], (D,), jnp.float32), 0.25, 1.75),
        "v_weight": scatter_about(streams_of[13], (D, KV), D ** -0.5, 0.09375, ((0, 32),)),
    }


def layer_norm(vit_rows, scale_vec, shift_vec):
    values = vit_rows.astype(jnp.float32)
    average = lax.optimization_barrier(jnp.mean(values, -1, keepdims=True))
    centred = values - average
    variance = lax.optimization_barrier(jnp.mean(centred * centred, -1, keepdims=True))
    return (centred * lax.rsqrt(variance + 1e-05) * scale_vec + shift_vec).astype(jnp.bfloat16)

def reference(vit_tiles, tile_counts, block_of_piece, segment_ids, text_rows, cotangent, proj_weight, proj_bias, out_weight, out_bias, ln_gain, ln_bias, norm_gain, v_weight):
    piece_total = N_LOCAL // 2
    slice_width = VW // N_LOCAL
    half_rows = TILE_TOK // 2
    run_rows = TILE_TOK // (2 * N_LOCAL)

    def one_sequence(sequence):
        normed = layer_norm(vit_tiles[sequence].reshape(N_LOCAL * half_rows, VW), ln_gain, ln_bias)
        preact = jnp.zeros((N_LOCAL * half_rows, D), jnp.float32)
        for slice_index in range(N_LOCAL):
            lower = slice_index * slice_width
            term = jnp.dot(normed[:, lower:lower + slice_width], proj_weight[lower:lower + slice_width], preferred_element_type=jnp.float32)
            term = lax.optimization_barrier(term.astype(jnp.bfloat16))
            preact = preact + term.astype(jnp.float32)
        middle = jax.nn.gelu(preact + proj_bias, approximate=False).astype(jnp.bfloat16)
        projected = (jnp.dot(middle, out_weight, preferred_element_type=jnp.float32) + out_bias).astype(jnp.bfloat16)
        projected = projected.reshape(piece_total, 2, N_LOCAL, run_rows, D).transpose(0, 2, 1, 3, 4).reshape(piece_total, TILE_TOK, D)
        filled = jnp.arange(piece_total, dtype=jnp.int32) % SLOTS < jnp.repeat(tile_counts[sequence], SLOTS)
        chosen = (block_of_piece[sequence][None, :] == jnp.arange(BLOCKS, dtype=jnp.int32)[:, None]) & filled[None, :]
        placed = jnp.einsum('bp,ptd->btd', chosen.astype(jnp.float32), projected.astype(jnp.float32))
        is_image = lax.optimization_barrier(jnp.sum(chosen.astype(jnp.int32), 1)) > 0
        hidden = jnp.where(is_image[:, None, None], placed.astype(jnp.bfloat16), text_rows[sequence])
        doc_ids = segment_ids[sequence].reshape(-1)
        doc_sizes = lax.optimization_barrier(jnp.sum((doc_ids[:, None] == jnp.arange(DOCS, dtype=jnp.int32)[None, :]).astype(jnp.float32), 0))
        doc_weight = BLOCKS * TILE_TOK / (DOCS * doc_sizes)
        token_weight = doc_weight[doc_ids]
        value_grad = (cotangent[sequence].reshape(-1, KV).astype(jnp.float32) * token_weight[:, None]).astype(jnp.bfloat16)
        hidden_f = hidden.reshape(-1, D).astype(jnp.float32)
        inv_rms = lax.rsqrt(lax.optimization_barrier(jnp.mean(hidden_f * hidden_f, -1, keepdims=True)) + 1e-06)
        normed_input = (hidden_f * inv_rms * norm_gain).astype(jnp.bfloat16)
        grad_normed = lax.dot_general(value_grad, v_weight, (((1,), (1,)), ((), ())), preferred_element_type=jnp.float32)
        gain_part = lax.optimization_barrier(jnp.sum(grad_normed * hidden_f * inv_rms, 0))
        scaled = grad_normed * norm_gain
        grad_hidden = inv_rms * scaled - hidden_f * (inv_rms * inv_rms * inv_rms) * lax.optimization_barrier(jnp.mean(scaled * hidden_f, -1, keepdims=True))
        weight_part = lax.dot_general(normed_input, value_grad, (((0,), (0,)), ((), ())), preferred_element_type=jnp.float32)
        bias_part = lax.optimization_barrier(jnp.sum(value_grad.astype(jnp.float32), 0))
        return (grad_hidden.astype(jnp.bfloat16).reshape(BLOCKS, TILE_TOK, D), weight_part, bias_part, gain_part)
    grad_hidden, weight_parts, bias_parts, gain_parts = lax.map(one_sequence, jnp.arange(N_NODE, dtype=jnp.int32))
    return (grad_hidden, lax.optimization_barrier(jnp.sum(weight_parts, 0)) / N_NODE, lax.optimization_barrier(jnp.sum(bias_parts, 0)) / N_NODE, lax.optimization_barrier(jnp.sum(gain_parts, 0)) / N_NODE)
```

```python
import functools

import jax
import jax.numpy as jnp
from jax import lax
from jax.experimental import pallas as pl
from jax.experimental.pallas import tpu as pltpu
from jax.sharding import PartitionSpec as P

SLOTS = 2
DOCS = 16
LANES = 128
COLUMN_BIT = 2
SPLITS = 2
SPREAD = 2
MESH = pl.DeviceIdType.MESH


def flip(index, bit):
    return index + bit - 2 * bit * lax.rem(lax.div(index, bit), 2)


def bits_below(count):
    return [1 << b for b in range(count.bit_length() - 1)]


def row_masks(node_count):
    bits = [b for b in bits_below(node_count) if b != COLUMN_BIT]
    masks = [m for m in range(node_count) if not m & COLUMN_BIT]
    return bits, masks


def toggled(index, mask):
    for b in range(mask.bit_length()):
        if mask >> b & 1:
            index = flip(index, 1 << b)
    return index


def visit_order(index, step, count):
    if count == 4:
        middle = lax.rem(lax.div(index + 1, 2), 2)
        step = step + middle * lax.div(step, 2) * (5 - 2 * step)
    total = 0
    for bit in bits_below(count):
        total = total + bit * lax.rem(lax.div(index, bit) + lax.div(step, bit), 2)
    return total


def slice_kernel(local_count, x_ref, scale_ref, shift_ref, out_ref):
    values = x_ref[...].astype(jnp.float32)
    average = jnp.mean(values, -1, keepdims=True)
    centred = values - average
    variance = jnp.mean(centred * centred, -1, keepdims=True)
    normed = centred * lax.rsqrt(variance + 1e-05) * scale_ref[...] + shift_ref[...]
    depth = out_ref.shape[2]
    for k in range(local_count):
        out_ref[k] = normed[:, k * depth : (k + 1) * depth].astype(jnp.bfloat16)


def slices(vit_rows, scale_vec, shift_vec, local_count):
    half_rows, width = vit_rows.shape
    depth = width // local_count
    step_rows = 16
    one_row = pl.BlockSpec((1, width), lambda i: (0, 0))
    return pl.pallas_call(
        functools.partial(slice_kernel, local_count),
        grid=(half_rows // step_rows,),
        in_specs=[pl.BlockSpec((step_rows, width), lambda i: (i, 0)), one_row, one_row],
        out_specs=pl.BlockSpec((local_count, step_rows, depth), lambda i: (0, i, 0)),
        out_shape=jax.ShapeDtypeStruct((local_count, half_rows, depth), jnp.bfloat16),
        cost_estimate=pl.CostEstimate(
            flops=10 * vit_rows.size, bytes_accessed=4 * vit_rows.size, transcendentals=0
        ),
    )(vit_rows, scale_vec[None, :], shift_vec[None, :])


def project_kernel(
    node_count,
    local_count,
    x_ref,
    w_ref,
    bias_ref,
    out_w_ref,
    count_ref,
    mid_ref,
    spread_ref,
    size_ref,
    rows,
    weights,
    part,
    from_low,
    from_high,
    total,
    final,
    landed,
    counts,
    w_sems,
    own_sems,
    hop_sem,
    recv_sem,
    fwd_sem,
    up_send,
    up_recv,
    down_send,
    down_recv,
    swap_send,
    swap_recv,
    line_send,
    spread_send,
    spread_recv,
    count_send,
    count_recv,
):
    node = lax.axis_index("node")
    me = lax.axis_index("local")
    last = local_count - 1
    bits, masks = row_masks(node_count)
    all_bits = bits_below(node_count)
    group = len(masks)
    half_rows = x_ref.shape[1]
    depth = x_ref.shape[2]
    shard = w_ref.shape[0]
    piece = half_rows // SPLITS
    run = half_rows // local_count
    side = lax.rem(lax.div(node, COLUMN_BIT), 2)
    above = lax.rem(me + 1, local_count)
    below = lax.rem(me + last, local_count)

    barrier = pltpu.get_barrier_semaphore()
    for step in range(1, local_count):
        pl.semaphore_signal(
            barrier, 1, device_id={"local": visit_order(me, step, local_count)}, device_id_type=MESH
        )
    for mask in [COLUMN_BIT] + masks[1:]:
        pl.semaphore_signal(
            barrier, 1, device_id={"node": toggled(node, mask)}, device_id_type=MESH
        )
    pl.semaphore_wait(barrier, local_count - 1 + group)

    shard_rows = pl.ds(pl.multiple_of(side * shard, 8), shard)
    w_copy = pltpu.make_async_remote_copy(
        w_ref,
        weights.at[shard_rows],
        w_sems.at[0],
        w_sems.at[1],
        device_id={"node": flip(node, COLUMN_BIT)},
        device_id_type=MESH,
    )
    w_copy.start()

    def count_copy(target, source):
        return pltpu.make_async_remote_copy(
            count_ref,
            counts.at[source],
            count_send.at[target],
            count_recv.at[source],
            device_id={"local": target},
            device_id_type=MESH,
        )

    for step in range(1, local_count):
        count_copy(visit_order(me, step, local_count), me).start()

    def part_rows(s):
        return pl.ds(pl.multiple_of(s * piece, 16), piece)

    def hop(target, source, s):
        return pltpu.make_async_remote_copy(
            x_ref.at[target, part_rows(s)],
            rows.at[source, 0, part_rows(s)],
            hop_sem.at[target, s],
            recv_sem.at[source, 0, s],
            device_id={"local": target},
            device_id_type=MESH,
        )

    def forward_bits(mask):
        return [b for b in reversed(bits) if mask == 0 or b < (mask & -mask)]

    def forward(slot, g, bit, s, origin):
        src = x_ref.at[slot, part_rows(s)] if origin else rows.at[slot, g, part_rows(s)]
        return pltpu.make_async_remote_copy(
            src,
            rows.at[slot, masks.index(masks[g] | bit), part_rows(s)],
            fwd_sem.at[slot, g, bits.index(bit), s],
            recv_sem.at[slot, masks.index(masks[g] | bit), s],
            device_id={"node": flip(node, bit)},
            device_id_type=MESH,
        )

    def wait_rows(slot, g, s):
        pltpu.make_async_remote_copy(
            rows.at[slot, g, part_rows(s)],
            rows.at[slot, g, part_rows(s)],
            hop_sem.at[slot, s],
            recv_sem.at[slot, g, s],
            device_id={"node": flip(node, 1)},
            device_id_type=MESH,
        ).wait_recv()

    for bit in forward_bits(0):
        for s in range(SPLITS):
            forward(me, 0, bit, s, True).start()
    for step in range(1, local_count):
        for s in range(SPLITS):
            hop(visit_order(me, step, local_count), me, s).start()
    own_w = pltpu.make_async_copy(w_ref, weights.at[shard_rows], own_sems.at[0])
    own_w.start()
    own_x = pltpu.make_async_copy(x_ref.at[me], rows.at[me, 0], own_sems.at[1])
    own_x.start()

    strip = shard // SPREAD

    def strip_rows(s, base=0):
        return pl.ds(pl.multiple_of(base + s * strip, 8), strip)

    def held(mask, slot, s, source_mask=None):
        other = (mask if source_mask is None else source_mask) // COLUMN_BIT % 2
        return spread_ref.at[
            masks.index(mask & ~COLUMN_BIT),
            slot,
            strip_rows(s, shard * (other + side * (1 - 2 * other))),
        ]

    def line(source, s, upward, origin):
        src = (
            out_w_ref.at[strip_rows(s, node * shard)]
            if origin
            else held(0, source, s)
        )
        return pltpu.make_async_remote_copy(
            src,
            held(0, source, s),
            line_send.at[source, upward, s],
            spread_recv.at[source, 0, s],
            device_id={"local": above if upward else below},
            device_id_type=MESH,
        )

    @pl.when(me < last)
    def _():
        for s in range(SPREAD):
            line(me, s, 1, True).start()

    @pl.when(me > 0)
    def _():
        for s in range(SPREAD):
            line(me, s, 0, True).start()

    def spread_order(s):
        wide = [b for b in all_bits if b > 1]
        return wide[s % len(wide) :] + wide[: s % len(wide)] + [1]

    def spread_bits(mask, s):
        order = spread_order(s)
        held = [i for i, b in enumerate(order) if mask & b]
        return order[held[-1] + 1 :] if held else order

    def spread(slot, mask, bit, s):
        return pltpu.make_async_remote_copy(
            held(mask, slot, s),
            held(mask | bit, slot, s, mask),
            spread_send.at[slot, mask, bit.bit_length() - 1, s],
            spread_recv.at[slot, mask | bit, s],
            device_id={"node": flip(node, bit)},
            device_id_type=MESH,
        )

    def wait_strip(slot, mask, s):
        pltpu.make_async_remote_copy(
            held(mask, slot, s),
            held(mask, slot, s),
            line_send.at[slot, 0, s],
            spread_recv.at[slot, mask, s],
            device_id={"node": flip(node, 1)},
            device_id_type=MESH,
        ).wait_recv()

    def take_line(step):
        slot = visit_order(me, step, local_count)
        for s in range(SPREAD):
            wait_strip(slot, 0, s)

            @pl.when((slot < me) & (me < last))
            def _():
                line(slot, s, 1, False).start()

            @pl.when((slot > me) & (me > 0))
            def _():
                line(slot, s, 0, False).start()

            for bit in spread_bits(0, s):
                spread(slot, 0, bit, s).start()

    def pass_on(step):
        slot = visit_order(me, step, local_count)
        for size in range(1, len(all_bits)):
            for s in range(SPREAD):
                for mask in range(1, node_count):
                    if bin(mask).count("1") == size and spread_bits(mask, s):
                        wait_strip(slot, mask, s)
                        for bit in spread_bits(mask, s):
                            spread(slot, mask, bit, s).start()

    relays = [g for g in range(1, group) if forward_bits(masks[g])]
    leaves = [g for g in range(1, group) if not forward_bits(masks[g])]

    def relay(step):
        slot = visit_order(me, step, local_count)
        for g in sorted(relays, key=lambda g: -(masks[g] & -masks[g])):
            for s in range(SPLITS):
                wait_rows(slot, g, s)
                for bit in forward_bits(masks[g]):
                    forward(slot, g, bit, s, False).start()

    def arrive(step):
        slot = visit_order(me, step, local_count)
        for s in range(SPLITS):
            wait_rows(slot, 0, s)
            for bit in forward_bits(0):
                forward(slot, 0, bit, s, False).start()
        relay(step - 1)

    def up(q, j):
        return pltpu.make_async_remote_copy(
            part.at[q, j],
            from_low.at[q, j],
            up_send.at[q, j],
            up_recv.at[q, j],
            device_id={"local": above},
            device_id_type=MESH,
        )

    def down(q, j):
        return pltpu.make_async_remote_copy(
            part.at[q, j],
            from_high.at[q, j],
            down_send.at[q, j],
            down_recv.at[q, j],
            device_id={"local": below},
            device_id_type=MESH,
        )

    def add_in(q, j, landing):
        part[q, j] = (
            part[q, j].astype(jnp.float32) + landing[q, j].astype(jnp.float32)
        ).astype(jnp.bfloat16)

    def reduce_round(r):
        def one(i, carry):
            q_up = last - i
            q_down = i
            j_up = r
            j_down = last - r

            @pl.when(q_up > me)
            def _():
                @pl.when(me > 0)
                def _():
                    up(q_up, j_up).wait_recv()
                    add_in(q_up, j_up, from_low)

                up(q_up, j_up).start()

            @pl.when(q_down < me)
            def _():
                @pl.when(me < last)
                def _():
                    down(q_down, j_down).wait_recv()
                    add_in(q_down, j_down, from_high)

                down(q_down, j_down).start()

            return carry

        lax.fori_loop(0, last, one, 0)

    at_end = (me == 0) | (me == last)

    def multiply(step, carry):
        slot = visit_order(me, step, local_count)

        @pl.when(step == last)
        def _():
            relay(last)

        for g in leaves:
            for s in range(SPLITS):
                wait_rows(slot, g, s)
        lhs = rows.at[slot]
        main = depth // 256 * 256
        term = jnp.zeros((group * half_rows, 2 * shard), jnp.float32)
        for lower, upper in ((0, main), (main, depth)):
            if upper > lower:
                term += lax.dot_general(
                    lhs[:, :, lower:upper].reshape(group * half_rows, upper - lower),
                    weights[:, lower:upper],
                    (((1,), (1,)), ((), ())),
                    preferred_element_type=jnp.float32,
                )
        term = term.astype(jnp.bfloat16)
        for q in range(local_count):
            for g in range(group):
                part[q, slot, g * run : (g + 1) * run, :] = term[
                    g * half_rows + q * run : g * half_rows + (q + 1) * run
                ]

        @pl.when(at_end)
        def _():
            reduce_round(step)

        return carry

    for step in range(1, max(2, last)):
        arrive(step)
    own_w.wait()
    own_x.wait()
    w_copy.wait_recv()
    lax.fori_loop(0, 1, multiply, 0)
    for step in range(max(2, last), local_count):
        arrive(step)
    lax.fori_loop(1, local_count, multiply, 0)

    for step in range(1, local_count):
        take_line(step)
        if step > 1:
            pass_on(step - 1)
        if step > 1:

            @pl.when(jnp.logical_not(at_end))
            def _():
                reduce_round(step - 2)

    pass_on(last)

    @pl.when(jnp.logical_not(at_end))
    def _():
        for r in range(last - 1, local_count):
            reduce_round(r)

    def swap(j, g):
        return pltpu.make_async_remote_copy(
            final.at[j, pl.ds(g * run, run)],
            landed.at[g, pl.ds(pl.multiple_of(j * run, 16), run)],
            swap_send.at[j, g],
            swap_recv.at[j, g],
            device_id={"node": toggled(node, masks[g])},
            device_id_type=MESH,
        )

    def finish(step, carry):
        j = visit_order(last - me, step, local_count)
        total[...] = part[me, j].astype(jnp.float32)

        @pl.when(me > 0)
        def _():
            up(me, j).wait_recv()
            total[...] += from_low[me, j].astype(jnp.float32)

        @pl.when(me < last)
        def _():
            down(me, j).wait_recv()
            total[...] += from_high[me, j].astype(jnp.float32)

        value = total[...] + bias_ref[...]
        final[j] = (0.5 * value * (1.0 + lax.erf(value * (0.5**0.5)))).astype(jnp.bfloat16)
        for g in reversed(range(1, group)):
            swap(j, g).start()
        mid_ref[0, pl.ds(pl.multiple_of(j * run, 16), run), :] = final[j, 0:run, :]
        return carry

    lax.fori_loop(0, local_count, finish, 0)

    counts_all = count_ref[...]
    for step in range(1, local_count):
        source = visit_order(me, step, local_count)
        count_copy(source, source).wait_recv()
        counts_all += counts[source]
        count_copy(source, me).wait_send()
    size_ref[...] = counts_all

    def settle(j, carry):
        for g in range(1, group):
            swap(j, g).wait()
        return carry

    lax.fori_loop(0, local_count, settle, 0)
    for g in range(1, group):
        mid_ref[g] = landed[g]

    w_copy.wait_send()
    for step in range(1, local_count):
        for s in range(SPLITS):
            hop(visit_order(me, step, local_count), me, s).wait_send()

    def drain(slot, carry):
        for g in range(group):
            for bit in forward_bits(masks[g]):
                for s in range(SPLITS):
                    forward(slot, g, bit, s, False).wait_send()

        for s in range(SPREAD):

            @pl.when((slot <= me) & (me < last))
            def _():
                line(slot, s, 1, False).wait_send()

            @pl.when((slot >= me) & (me > 0))
            def _():
                line(slot, s, 0, False).wait_send()

        @pl.when(slot != me)
        def _():
            for s in range(SPREAD):
                for mask in range(node_count):
                    if mask and not spread_bits(mask, s):
                        wait_strip(slot, mask, s)
                    for bit in spread_bits(mask, s):
                        spread(slot, mask, bit, s).wait_send()

        def drain_sums(j, inner):
            @pl.when(slot > me)
            def _():
                up(slot, j).wait_send()

            @pl.when(slot < me)
            def _():
                down(slot, j).wait_send()

            return inner

        lax.fori_loop(0, local_count, drain_sums, 0)
        return carry

    lax.fori_loop(0, local_count, drain, 0)


def project(x_slices, weight, bias_pair, out_weight, counts, node_count, local_count):
    _, half_rows, depth = x_slices.shape
    cols = weight.shape[0]
    bits, masks = row_masks(node_count)
    group = len(masks)
    run = half_rows // local_count
    sums = (local_count, local_count, group * run, 2 * cols)
    dma = pltpu.SemaphoreType.DMA
    grid = (local_count, local_count)
    anywhere = pl.BlockSpec(memory_space=pl.ANY)
    vmem = pl.BlockSpec(memory_space=pltpu.VMEM)
    all_bits = len(bits_below(node_count))
    return pl.pallas_call(
        functools.partial(project_kernel, node_count, local_count),
        out_shape=[
            jax.ShapeDtypeStruct((group, half_rows, 2 * cols), jnp.bfloat16),
            jax.ShapeDtypeStruct(
                (group, local_count, 2 * cols, out_weight.shape[1]), jnp.bfloat16
            ),
            jax.ShapeDtypeStruct(counts.shape, jnp.float32),
        ],
        in_specs=[anywhere, anywhere, vmem, anywhere, vmem],
        out_specs=[vmem, anywhere, vmem],
        scratch_shapes=[
            pltpu.VMEM((local_count, group, half_rows, depth), jnp.bfloat16),
            pltpu.VMEM((2 * cols, depth), jnp.bfloat16),
            pltpu.VMEM(sums, jnp.bfloat16),
            pltpu.VMEM(sums, jnp.bfloat16),
            pltpu.VMEM(sums, jnp.bfloat16),
            pltpu.VMEM(sums[2:], jnp.float32),
            pltpu.VMEM(sums[1:], jnp.bfloat16),
            pltpu.VMEM((group, half_rows, 2 * cols), jnp.bfloat16),
            pltpu.VMEM((local_count,) + counts.shape, jnp.float32),
            dma((2,)),
            dma((2,)),
            dma((local_count, SPLITS)),
            dma((local_count, group, SPLITS)),
            dma((local_count, group, len(bits), SPLITS)),
            dma(grid),
            dma(grid),
            dma(grid),
            dma(grid),
            dma((local_count, group)),
            dma((local_count, group)),
            dma((local_count, 2, SPREAD)),
            dma((local_count, node_count, all_bits, SPREAD)),
            dma((local_count, node_count, SPREAD)),
            dma((local_count,)),
            dma((local_count,)),
        ],
        compiler_params=pltpu.CompilerParams(
            collective_id=0, has_side_effects=True, vmem_limit_bytes=58 * 2**20
        ),
        cost_estimate=pl.CostEstimate(
            flops=4 * local_count * group * half_rows * depth * cols,
            bytes_accessed=2 * (x_slices.size + weight.size),
            transcendentals=0,
        ),
    )(x_slices, weight, bias_pair, out_weight, counts)


def second_kernel(local_count, place_ref, mid_ref, own_ref, weight_ref, bias_ref, out_ref, total):
    group, _, depth = mid_ref.shape
    width = weight_ref.shape[3]
    column = lax.rem(place_ref[0] + pl.program_id(0), local_count)
    main = depth // 256 * 256

    def product(pick):
        sum_rows = jnp.zeros(total.shape, jnp.float32)
        for g in range(group):
            rhs = pick(g)
            for lower, upper in ((0, main), (main, depth)):
                if upper > lower:
                    sum_rows += jnp.dot(
                        mid_ref[g, :, lower:upper],
                        rhs[lower:upper],
                        preferred_element_type=jnp.float32,
                    )
        total[...] = sum_rows

    @pl.when(pl.program_id(0) == 0)
    def _():
        product(
            lambda g: jnp.concatenate(
                [own_ref[place_ref[1 + g]], own_ref[place_ref[1 + g] + COLUMN_BIT]], 0
            )
        )

    @pl.when(pl.program_id(0) > 0)
    def _():
        product(lambda g: weight_ref[g, 0])

    for z in range(local_count):

        @pl.when(column == z)
        def _():
            value = total[...] + bias_ref[:, z * width : (z + 1) * width]
            out_ref[...] = value.astype(jnp.bfloat16).reshape(out_ref.shape)


def second_product(places, mid, own_weight, weight, bias_row):
    group, local_count, pair_cols, width = weight.shape
    cols = pair_cols // 2
    node_count = 2 * group
    half_rows = mid.shape[1]
    joined = width % LANES == 0

    def column(z, place):
        return lax.rem(place[0] + z, local_count)

    def fetched(z, place):
        return lax.rem(place[0] + jnp.maximum(z, 1), local_count)

    if joined:
        out_shape = (half_rows, local_count * width)
        out_block = pl.BlockSpec((half_rows, width), lambda z, place: (0, column(z, place)))
    else:
        out_shape = (local_count, half_rows, width)
        out_block = pl.BlockSpec((1, half_rows, width), lambda z, place: (column(z, place), 0, 0))
    product = pl.pallas_call(
        functools.partial(second_kernel, local_count),
        grid_spec=pltpu.PrefetchScalarGridSpec(
            num_scalar_prefetch=1,
            grid=(local_count,),
            in_specs=[
                pl.BlockSpec(mid.shape, lambda z, place: (0, 0, 0)),
                pl.BlockSpec((node_count, cols, width), lambda z, place: (0, 0, 0)),
                pl.BlockSpec(
                    (group, 1, pair_cols, width), lambda z, place: (0, fetched(z, place), 0, 0)
                ),
                pl.BlockSpec((1, local_count * width + 8 * LANES), lambda z, place: (0, 0)),
            ],
            out_specs=out_block,
            scratch_shapes=[pltpu.VMEM((half_rows, width), jnp.float32)],
        ),
        out_shape=jax.ShapeDtypeStruct(out_shape, jnp.bfloat16),
        compiler_params=pltpu.CompilerParams(vmem_limit_bytes=48 * 2**20),
        cost_estimate=pl.CostEstimate(
            flops=2 * half_rows * weight.size, bytes_accessed=2 * weight.size, transcendentals=0
        ),
    )(
        places,
        mid,
        own_weight.reshape(node_count, cols, width),
        weight,
        jnp.pad(bias_row, (0, 8 * LANES))[None, :],
    )
    if joined:
        return product
    return jnp.transpose(product, (1, 0, 2)).reshape(half_rows, local_count * width)


def row_grads(hidden_f, grad_rows, weight, gain, keep):
    inv_rms = lax.rsqrt(jnp.mean(hidden_f * hidden_f, -1, keepdims=True) + 1e-06)
    unit = hidden_f * inv_rms
    normed = (unit * gain * keep).astype(jnp.bfloat16)
    grad_normed = lax.dot_general(
        grad_rows, weight, (((1,), (1,)), ((), ())), preferred_element_type=jnp.float32
    )
    part = jnp.sum(grad_normed * unit, 0, keepdims=True) * keep
    scaled = grad_normed * gain
    moment = jnp.mean(scaled * hidden_f, -1, keepdims=True)
    grad_hidden = inv_rms * scaled - hidden_f * (inv_rms * inv_rms * inv_rms * moment)
    return normed, part, grad_hidden.astype(jnp.bfloat16)


def add_part(part_ref, part):
    @pl.when(pl.program_id(0) == 0)
    def _():
        part_ref[...] = part

    @pl.when(pl.program_id(0) > 0)
    def _():
        part_ref[...] += part


def text_kernel(
    image_ref, text_ref, grad_ref, weight_ref, gain_ref, out_ref, normed_ref, part_ref
):
    keep = jnp.where(image_ref[pl.program_id(0)] > 0, 0.0, 1.0)
    normed_ref[0], part, out_ref[0] = row_grads(
        text_ref[0].astype(jnp.float32), grad_ref[0], weight_ref[...], gain_ref[...], keep
    )
    add_part(part_ref, part)


def image_kernel(
    block_ref,
    filled_ref,
    arrived_ref,
    grad_ref,
    weight_ref,
    gain_ref,
    text_out_ref,
    out_ref,
    normed_ref,
    part_ref,
):
    filled = filled_ref[pl.program_id(0)] > 0
    normed_ref[0], part, grad_hidden = row_grads(
        arrived_ref[0].astype(jnp.float32),
        grad_ref[0],
        weight_ref[...],
        gain_ref[...],
        jnp.where(filled, 1.0, 0.0),
    )
    add_part(part_ref, part)

    @pl.when(filled)
    def _():
        out_ref[0] = grad_hidden

    @pl.when(jnp.logical_not(filled))
    def _():
        out_ref[0] = text_out_ref[0]


def cost(steps, rows, width, values):
    return pl.CostEstimate(
        flops=2 * steps * rows * width * values,
        bytes_accessed=6 * steps * rows * width + 2 * width * values,
        transcendentals=0,
    )


def text_grads(is_image, text, value_grad, v_full, gain):
    blocks, rows, width = text.shape
    values = value_grad.shape[2]
    row_block = pl.BlockSpec((1, rows, width), lambda b, image: (b, 0, 0))
    one_row = pl.BlockSpec((1, width), lambda b, image: (0, 0))
    return pl.pallas_call(
        text_kernel,
        grid_spec=pltpu.PrefetchScalarGridSpec(
            num_scalar_prefetch=1,
            grid=(blocks,),
            in_specs=[
                row_block,
                pl.BlockSpec((1, rows, values), lambda b, image: (b, 0, 0)),
                pl.BlockSpec((width, values), lambda b, image: (0, 0)),
                one_row,
            ],
            out_specs=[row_block, row_block, one_row],
        ),
        out_shape=[
            jax.ShapeDtypeStruct((blocks, rows, width), jnp.bfloat16),
            jax.ShapeDtypeStruct((blocks, rows, width), jnp.bfloat16),
            jax.ShapeDtypeStruct((1, width), jnp.float32),
        ],
        cost_estimate=cost(blocks, rows, width, values),
    )(is_image, text, value_grad, v_full, gain)


def image_grads(block_of_piece, filled, arrived, value_grad, v_full, gain, text_out):
    pieces, rows, width = arrived.shape
    values = value_grad.shape[2]
    piece_rows = pl.BlockSpec((1, rows, width), lambda p, block, full: (p, 0, 0))
    block_rows = pl.BlockSpec((1, rows, width), lambda p, block, full: (block[p], 0, 0))
    one_row = pl.BlockSpec((1, width), lambda p, block, full: (0, 0))
    return pl.pallas_call(
        image_kernel,
        grid_spec=pltpu.PrefetchScalarGridSpec(
            num_scalar_prefetch=2,
            grid=(pieces,),
            in_specs=[
                piece_rows,
                pl.BlockSpec((1, rows, values), lambda p, block, full: (p, 0, 0)),
                pl.BlockSpec((width, values), lambda p, block, full: (0, 0)),
                one_row,
                block_rows,
            ],
            out_specs=[block_rows, piece_rows, one_row],
        ),
        out_shape=[
            jax.ShapeDtypeStruct(text_out.shape, jnp.bfloat16),
            jax.ShapeDtypeStruct((pieces, rows, width), jnp.bfloat16),
            jax.ShapeDtypeStruct((1, width), jnp.float32),
        ],
        input_output_aliases={6: 0},
        cost_estimate=cost(pieces, rows, width, values),
    )(block_of_piece, filled, arrived, value_grad, v_full, gain, text_out)


def weight_grad(normed, grad_rows):
    return lax.dot_general(
        normed, grad_rows, (((0,), (0,)), ((), ())), preferred_element_type=jnp.float32
    )


def per_device(
    vit_tiles,
    tile_counts,
    block_of_piece,
    segment_ids,
    text_rows,
    cotangent,
    proj_weight,
    proj_bias,
    out_weight,
    out_bias,
    ln_gain,
    ln_bias,
    norm_gain,
    v_weight,
):
    local_count = lax.axis_size("local")
    node_count = lax.axis_size("node")
    node = lax.axis_index("node")
    blocks = text_rows.shape[1]
    share_rows = text_rows.shape[2]
    model_width = text_rows.shape[3]
    out_cols = out_weight.shape[1]
    shard_cols = proj_weight.shape[1]
    x_slices = slices(vit_tiles[0, 0], ln_gain, ln_bias, local_count)
    side = lax.rem(lax.div(node, COLUMN_BIT), 2)
    low_shard = node - COLUMN_BIT * side
    bias_pair = jnp.concatenate(
        [
            lax.dynamic_slice_in_dim(proj_bias, shard * shard_cols, shard_cols, 0)
            for shard in (low_shard, low_shard + COLUMN_BIT)
        ]
    )[None, :]
    v_full = lax.all_gather(v_weight, ("node", "local"), axis=0, tiled=True)
    _, masks = row_masks(node_count)
    places = jnp.stack(
        [lax.axis_index("local")]
        + [toggled(low_shard, m) for m in masks]
    )
    doc_ids = segment_ids[0].reshape(-1)
    doc_hits = (doc_ids[:, None] == lax.iota(jnp.int32, DOCS)[None, :]).astype(jnp.float32)
    doc_counts = jnp.pad(jnp.sum(doc_hits, 0)[None, :], ((0, 7), (0, LANES - DOCS)))
    mid, out_spread, doc_sizes = project(
        x_slices,
        jnp.transpose(proj_weight),
        bias_pair,
        out_weight,
        doc_counts,
        node_count,
        local_count,
    )
    doc_sizes = doc_sizes[0, :DOCS]
    doc_weight = blocks * share_rows * local_count / (DOCS * doc_sizes)
    token_weight = jnp.dot(doc_hits, doc_weight, precision=lax.Precision.HIGHEST)
    value_grad = (
        cotangent[0].reshape(-1, cotangent.shape[3]).astype(jnp.float32) * token_weight[:, None]
    ).astype(jnp.bfloat16)
    bias_part = jnp.sum(value_grad.astype(jnp.float32), 0)
    piece_total = local_count // 2
    piece_ids = lax.iota(jnp.int32, piece_total)
    filled = piece_ids % SLOTS < jnp.repeat(tile_counts[0], SLOTS)
    chosen = (block_of_piece[0][None, :] == lax.iota(jnp.int32, blocks)[:, None]) & filled[None, :]
    is_image = jnp.any(chosen, 1).astype(jnp.int32)
    gain_row = norm_gain[None, :]
    value_blocks = value_grad.reshape(blocks, share_rows, -1)
    value_pieces = value_blocks[block_of_piece[0]]
    text_out, text_normed, text_part = text_grads(
        is_image, text_rows[0], value_blocks, v_full, gain_row
    )
    text_sum = weight_grad(text_normed.reshape(-1, model_width), value_grad).astype(jnp.bfloat16)
    flat_pieces = value_pieces.reshape(-1, value_pieces.shape[2])
    pieces_all = lax.all_gather(flat_pieces, "node", axis=0, tiled=True)
    text_sum = lax.psum_scatter(text_sum, "node", scatter_dimension=0, tiled=True)
    arrived = second_product(places, mid, out_weight, out_spread, out_bias)
    arrived = arrived.reshape(piece_total, share_rows, model_width)
    grad_hidden, image_normed, image_part = image_grads(
        block_of_piece[0], filled.astype(jnp.int32), arrived, value_pieces, v_full, gain_row, text_out
    )
    gain_part = text_part + image_part
    image_columns = lax.all_to_all(
        image_normed.reshape(-1, model_width), "node", split_axis=1, concat_axis=0, tiled=True
    )
    partial_sum = (weight_grad(image_columns, pieces_all) + text_sum.astype(jnp.float32)).astype(
        jnp.bfloat16
    )
    grad_bias, grad_gain = lax.psum((bias_part, gain_part[0]), ("node", "local"))
    grad_weight = lax.psum_scatter(partial_sum, "local", scatter_dimension=0, tiled=True).astype(
        jnp.float32
    )
    grad_hidden = grad_hidden[None]
    return (grad_hidden, grad_weight / node_count, grad_bias / node_count, grad_gain / node_count)


def solution(mesh):
    in_specs = (
        P("node", "local", None, None),
        P("node", None),
        P("node", None),
        P("node", None, "local"),
        P("node", None, "local", None),
        P("node", None, "local", None),
        P("local", "node"),
        P(),
        P(None, "local"),
        P(),
        P(),
        P(),
        P(),
        P(("node", "local"), None),
    )
    out_specs = (P("node", None, "local", None), P(("node", "local"), None), P(), P())
    return jax.shard_map(
        per_device, mesh=mesh, in_specs=in_specs, out_specs=out_specs, check_vma=False
    )
```

```python
import functools

import jax
import jax.numpy as jnp
from jax import lax
from jax.experimental import pallas as pl
from jax.experimental.pallas import tpu as pltpu
from jax.sharding import PartitionSpec as P

SLOTS = 2
DOCS = 16
LANES = 128
COLUMN_BIT = 2
SPLITS = 2
SPREAD = 2
MESH = pl.DeviceIdType.MESH


def flip(index, bit):
    return index + bit - 2 * bit * lax.rem(lax.div(index, bit), 2)


def bits_below(count):
    return [1 << b for b in range(count.bit_length() - 1)]


def row_masks(node_count):
    bits = [b for b in bits_below(node_count) if b != COLUMN_BIT]
    masks = [m for m in range(node_count) if not m & COLUMN_BIT]
    return bits, masks


def toggled(index, mask):
    for b in range(mask.bit_length()):
        if mask >> b & 1:
            index = flip(index, 1 << b)
    return index


def visit_order(index, step, count):
    if count == 4:
        middle = lax.rem(lax.div(index + 1, 2), 2)
        step = step + middle * lax.div(step, 2) * (5 - 2 * step)
    total = 0
    for bit in bits_below(count):
        total = total + bit * lax.rem(lax.div(index, bit) + lax.div(step, bit), 2)
    return total


def slice_kernel(local_count, x_ref, scale_ref, shift_ref, out_ref):
    values = x_ref[...].astype(jnp.float32)
    average = jnp.mean(values, -1, keepdims=True)
    centred = values - average
    variance = jnp.mean(centred * centred, -1, keepdims=True)
    normed = centred * lax.rsqrt(variance + 1e-05) * scale_ref[...] + shift_ref[...]
    depth = out_ref.shape[2]
    for k in range(local_count):
        out_ref[k] = normed[:, k * depth : (k + 1) * depth].astype(jnp.bfloat16)


def slices(vit_rows, scale_vec, shift_vec, local_count):
    half_rows, width = vit_rows.shape
    depth = width // local_count
    step_rows = 16
    one_row = pl.BlockSpec((1, width), lambda i: (0, 0))
    return pl.pallas_call(
        functools.partial(slice_kernel, local_count),
        grid=(half_rows // step_rows,),
        in_specs=[pl.BlockSpec((step_rows, width), lambda i: (i, 0)), one_row, one_row],
        out_specs=pl.BlockSpec((local_count, step_rows, depth), lambda i: (0, i, 0)),
        out_shape=jax.ShapeDtypeStruct((local_count, half_rows, depth), jnp.bfloat16),
        cost_estimate=pl.CostEstimate(
            flops=10 * vit_rows.size, bytes_accessed=4 * vit_rows.size, transcendentals=0
        ),
    )(vit_rows, scale_vec[None, :], shift_vec[None, :])


def project_kernel(
    node_count,
    local_count,
    x_ref,
    w_ref,
    bias_ref,
    out_w_ref,
    count_ref,
    mid_ref,
    spread_ref,
    size_ref,
    rows,
    weights,
    part,
    from_low,
    from_high,
    total,
    final,
    landed,
    counts,
    w_sems,
    own_sems,
    hop_sem,
    recv_sem,
    fwd_sem,
    up_send,
    up_recv,
    down_send,
    down_recv,
    swap_send,
    swap_recv,
    line_send,
    spread_send,
    spread_recv,
    count_send,
    count_recv,
):
    node = lax.axis_index("node")
    me = lax.axis_index("local")
    last = local_count - 1
    bits, masks = row_masks(node_count)
    all_bits = bits_below(node_count)
    group = len(masks)
    half_rows = x_ref.shape[1]
    depth = x_ref.shape[2]
    shard = w_ref.shape[0]
    piece = half_rows // SPLITS
    run = half_rows // local_count
    side = lax.rem(lax.div(node, COLUMN_BIT), 2)
    above = lax.rem(me + 1, local_count)
    below = lax.rem(me + last, local_count)
    at_end = (me == 0) | (me == last)

    barrier = pltpu.get_barrier_semaphore()
    for step in range(1, local_count):
        pl.semaphore_signal(
            barrier, 1, device_id={"local": visit_order(me, step, local_count)}, device_id_type=MESH
        )
    for mask in [COLUMN_BIT] + masks[1:]:
        pl.semaphore_signal(
            barrier, 1, device_id={"node": toggled(node, mask)}, device_id_type=MESH
        )
    pl.semaphore_wait(barrier, local_count - 1 + group)

    shard_rows = pl.ds(pl.multiple_of(side * shard, 8), shard)
    w_copy = pltpu.make_async_remote_copy(
        w_ref,
        weights.at[shard_rows],
        w_sems.at[0],
        w_sems.at[1],
        device_id={"node": flip(node, COLUMN_BIT)},
        device_id_type=MESH,
    )
    w_copy.start()

    def count_copy(target, source):
        return pltpu.make_async_remote_copy(
            count_ref,
            counts.at[source],
            count_send.at[target],
            count_recv.at[source],
            device_id={"local": target},
            device_id_type=MESH,
        )

    for step in range(1, local_count):
        count_copy(visit_order(me, step, local_count), me).start()

    def part_rows(s):
        return pl.ds(pl.multiple_of(s * piece, 16), piece)

    def hop(target, source, s):
        return pltpu.make_async_remote_copy(
            x_ref.at[target, part_rows(s)],
            rows.at[source, 0, part_rows(s)],
            hop_sem.at[target, s],
            recv_sem.at[source, 0, s],
            device_id={"local": target},
            device_id_type=MESH,
        )

    def forward_bits(mask):
        return [b for b in reversed(bits) if mask == 0 or b < (mask & -mask)]

    def forward(slot, g, bit, s, origin):
        src = x_ref.at[slot, part_rows(s)] if origin else rows.at[slot, g, part_rows(s)]
        return pltpu.make_async_remote_copy(
            src,
            rows.at[slot, masks.index(masks[g] | bit), part_rows(s)],
            fwd_sem.at[slot, g, bits.index(bit), s],
            recv_sem.at[slot, masks.index(masks[g] | bit), s],
            device_id={"node": flip(node, bit)},
            device_id_type=MESH,
        )

    def wait_rows(slot, g, s):
        pltpu.make_async_remote_copy(
            rows.at[slot, g, part_rows(s)],
            rows.at[slot, g, part_rows(s)],
            hop_sem.at[slot, s],
            recv_sem.at[slot, g, s],
            device_id={"node": flip(node, 1)},
            device_id_type=MESH,
        ).wait_recv()

    for bit in forward_bits(0):
        for s in range(SPLITS):
            forward(me, 0, bit, s, True).start()
    def start_hops(step):
        for s in range(SPLITS):
            hop(visit_order(me, step, local_count), me, s).start()

    paced = local_count == 4
    if paced:
        start_hops(1)

        @pl.when(jnp.logical_not(at_end))
        def _():
            start_hops(2)
    else:
        for step in range(1, local_count):
            start_hops(step)
    own_w = pltpu.make_async_copy(w_ref, weights.at[shard_rows], own_sems.at[0])
    own_w.start()
    own_x = pltpu.make_async_copy(x_ref.at[me], rows.at[me, 0], own_sems.at[1])
    own_x.start()

    strip = shard // SPREAD

    def strip_rows(s, base=0):
        return pl.ds(pl.multiple_of(base + s * strip, 8), strip)

    def held(mask, slot, s, source_mask=None):
        other = (mask if source_mask is None else source_mask) // COLUMN_BIT % 2
        return spread_ref.at[
            masks.index(mask & ~COLUMN_BIT),
            slot,
            strip_rows(s, shard * (other + side * (1 - 2 * other))),
        ]

    def line(source, s, upward, origin):
        src = (
            out_w_ref.at[strip_rows(s, node * shard)]
            if origin
            else held(0, source, s)
        )
        return pltpu.make_async_remote_copy(
            src,
            held(0, source, s),
            line_send.at[source, upward, s],
            spread_recv.at[source, 0, s],
            device_id={"local": above if upward else below},
            device_id_type=MESH,
        )

    def start_lines():
        @pl.when(me < last)
        def _():
            for s in range(SPREAD):
                line(me, s, 1, True).start()

        @pl.when(me > 0)
        def _():
            for s in range(SPREAD):
                line(me, s, 0, True).start()

    def spread_order(s):
        wide = [b for b in all_bits if b > 1]
        return wide[s % len(wide) :] + wide[: s % len(wide)] + [1]

    def spread_bits(mask, s):
        order = spread_order(s)
        held = [i for i, b in enumerate(order) if mask & b]
        return order[held[-1] + 1 :] if held else order

    def spread(slot, mask, bit, s):
        return pltpu.make_async_remote_copy(
            held(mask, slot, s),
            held(mask | bit, slot, s, mask),
            spread_send.at[slot, mask, bit.bit_length() - 1, s],
            spread_recv.at[slot, mask | bit, s],
            device_id={"node": flip(node, bit)},
            device_id_type=MESH,
        )

    def wait_strip(slot, mask, s):
        pltpu.make_async_remote_copy(
            held(mask, slot, s),
            held(mask, slot, s),
            line_send.at[slot, 0, s],
            spread_recv.at[slot, mask, s],
            device_id={"node": flip(node, 1)},
            device_id_type=MESH,
        ).wait_recv()

    def take_line(step):
        slot = visit_order(me, step, local_count)
        for s in range(SPREAD):
            wait_strip(slot, 0, s)

            @pl.when((slot < me) & (me < last))
            def _():
                line(slot, s, 1, False).start()

            @pl.when((slot > me) & (me > 0))
            def _():
                line(slot, s, 0, False).start()

            for bit in spread_bits(0, s):
                spread(slot, 0, bit, s).start()

    def pass_on(step):
        slot = visit_order(me, step, local_count)
        for size in range(1, len(all_bits)):
            for s in range(SPREAD):
                for mask in range(1, node_count):
                    if bin(mask).count("1") == size and spread_bits(mask, s):
                        wait_strip(slot, mask, s)
                        for bit in spread_bits(mask, s):
                            spread(slot, mask, bit, s).start()

    relays = [g for g in range(1, group) if forward_bits(masks[g])]
    leaves = [g for g in range(1, group) if not forward_bits(masks[g])]

    def relay(step):
        slot = visit_order(me, step, local_count)
        for g in sorted(relays, key=lambda g: -(masks[g] & -masks[g])):
            for s in range(SPLITS):
                wait_rows(slot, g, s)
                for bit in forward_bits(masks[g]):
                    forward(slot, g, bit, s, False).start()

    def arrive(step):
        slot = visit_order(me, step, local_count)
        for s in range(SPLITS):
            wait_rows(slot, 0, s)
            for bit in forward_bits(0):
                forward(slot, 0, bit, s, False).start()
        relay(step - 1)

    def up(q, j):
        return pltpu.make_async_remote_copy(
            part.at[q, j],
            from_low.at[q, j],
            up_send.at[q, j],
            up_recv.at[q, j],
            device_id={"local": above},
            device_id_type=MESH,
        )

    def down(q, j):
        return pltpu.make_async_remote_copy(
            part.at[q, j],
            from_high.at[q, j],
            down_send.at[q, j],
            down_recv.at[q, j],
            device_id={"local": below},
            device_id_type=MESH,
        )

    def add_in(q, j, landing):
        part[q, j] = (
            part[q, j].astype(jnp.float32) + landing[q, j].astype(jnp.float32)
        ).astype(jnp.bfloat16)

    def reduce_round(r):
        def one(i, carry):
            q_up = last - i
            q_down = i
            j_up = r
            j_down = last - r

            @pl.when(q_up > me)
            def _():
                @pl.when(me > 0)
                def _():
                    up(q_up, j_up).wait_recv()
                    add_in(q_up, j_up, from_low)

                up(q_up, j_up).start()

            @pl.when(q_down < me)
            def _():
                @pl.when(me < last)
                def _():
                    down(q_down, j_down).wait_recv()
                    add_in(q_down, j_down, from_high)

                down(q_down, j_down).start()

            return carry

        lax.fori_loop(0, last, one, 0)

    def multiply(step, carry):
        slot = visit_order(me, step, local_count)

        @pl.when(step == last)
        def _():
            relay(last)

        for g in leaves:
            for s in range(SPLITS):
                wait_rows(slot, g, s)
        lhs = rows.at[slot]
        main = depth // 256 * 256
        term = jnp.zeros((group * half_rows, 2 * shard), jnp.float32)
        for lower, upper in ((0, main), (main, depth)):
            if upper > lower:
                term += lax.dot_general(
                    lhs[:, :, lower:upper].reshape(group * half_rows, upper - lower),
                    weights[:, lower:upper],
                    (((1,), (1,)), ((), ())),
                    preferred_element_type=jnp.float32,
                )
        term = term.astype(jnp.bfloat16)
        for q in range(local_count):
            for g in range(group):
                part[q, slot, g * run : (g + 1) * run, :] = term[
                    g * half_rows + q * run : g * half_rows + (q + 1) * run
                ]

        @pl.when(at_end)
        def _():
            reduce_round(step)

        return carry

    def arrive_next(step):
        arrive(step)
        if paced and step < last:

            @pl.when(at_end)
            def _():
                start_hops(step + 1)

            if step == 1:

                @pl.when(jnp.logical_not(at_end))
                def _():
                    start_hops(last)

    for step in range(1, max(2, last)):
        arrive_next(step)
    own_w.wait()
    own_x.wait()
    w_copy.wait_recv()
    lax.fori_loop(0, 1, multiply, 0)
    for step in range(max(2, last), local_count):
        arrive_next(step)
    start_lines()
    lax.fori_loop(1, local_count, multiply, 0)

    def middle_round(r):
        @pl.when(jnp.logical_not(at_end))
        def _():
            reduce_round(r)

    for step in range(1, local_count):
        take_line(step)
        middle_round(step - 1)
        if step > 1:
            pass_on(step - 1)
    middle_round(last)
    pass_on(last)

    def swap(j, g):
        return pltpu.make_async_remote_copy(
            final.at[j, pl.ds(g * run, run)],
            landed.at[g, pl.ds(pl.multiple_of(j * run, 16), run)],
            swap_send.at[j, g],
            swap_recv.at[j, g],
            device_id={"node": toggled(node, masks[g])},
            device_id_type=MESH,
        )

    def finish(step, carry):
        j = visit_order(last - me, step, local_count)
        total[...] = part[me, j].astype(jnp.float32)

        @pl.when(me > 0)
        def _():
            up(me, j).wait_recv()
            total[...] += from_low[me, j].astype(jnp.float32)

        @pl.when(me < last)
        def _():
            down(me, j).wait_recv()
            total[...] += from_high[me, j].astype(jnp.float32)

        value = total[...] + bias_ref[...]
        final[j] = (0.5 * value * (1.0 + lax.erf(value * (0.5**0.5)))).astype(jnp.bfloat16)
        for g in reversed(range(1, group)):
            swap(j, g).start()
        mid_ref[0, pl.ds(pl.multiple_of(j * run, 16), run), :] = final[j, 0:run, :]
        return carry

    lax.fori_loop(0, local_count, finish, 0)

    counts_all = count_ref[...]
    for step in range(1, local_count):
        source = visit_order(me, step, local_count)
        count_copy(source, source).wait_recv()
        counts_all += counts[source]
        count_copy(source, me).wait_send()
    size_ref[...] = counts_all

    def settle(j, carry):
        for g in range(1, group):
            swap(j, g).wait()
        return carry

    lax.fori_loop(0, local_count, settle, 0)
    for g in range(1, group):
        mid_ref[g] = landed[g]

    w_copy.wait_send()
    for step in range(1, local_count):
        for s in range(SPLITS):
            hop(visit_order(me, step, local_count), me, s).wait_send()

    def drain(slot, carry):
        for g in range(group):
            for bit in forward_bits(masks[g]):
                for s in range(SPLITS):
                    forward(slot, g, bit, s, False).wait_send()

        for s in range(SPREAD):

            @pl.when((slot <= me) & (me < last))
            def _():
                line(slot, s, 1, False).wait_send()

            @pl.when((slot >= me) & (me > 0))
            def _():
                line(slot, s, 0, False).wait_send()

        @pl.when(slot != me)
        def _():
            for s in range(SPREAD):
                for mask in range(node_count):
                    if mask and not spread_bits(mask, s):
                        wait_strip(slot, mask, s)
                    for bit in spread_bits(mask, s):
                        spread(slot, mask, bit, s).wait_send()

        def drain_sums(j, inner):
            @pl.when(slot > me)
            def _():
                up(slot, j).wait_send()

            @pl.when(slot < me)
            def _():
                down(slot, j).wait_send()

            return inner

        lax.fori_loop(0, local_count, drain_sums, 0)
        return carry

    lax.fori_loop(0, local_count, drain, 0)


def project(x_slices, weight, bias_pair, out_weight, counts, node_count, local_count):
    _, half_rows, depth = x_slices.shape
    cols = weight.shape[0]
    bits, masks = row_masks(node_count)
    group = len(masks)
    run = half_rows // local_count
    sums = (local_count, local_count, group * run, 2 * cols)
    dma = pltpu.SemaphoreType.DMA
    grid = (local_count, local_count)
    anywhere = pl.BlockSpec(memory_space=pl.ANY)
    vmem = pl.BlockSpec(memory_space=pltpu.VMEM)
    all_bits = len(bits_below(node_count))
    return pl.pallas_call(
        functools.partial(project_kernel, node_count, local_count),
        out_shape=[
            jax.ShapeDtypeStruct((group, half_rows, 2 * cols), jnp.bfloat16),
            jax.ShapeDtypeStruct(
                (group, local_count, 2 * cols, out_weight.shape[1]), jnp.bfloat16
            ),
            jax.ShapeDtypeStruct(counts.shape, jnp.float32),
        ],
        in_specs=[anywhere, anywhere, vmem, anywhere, vmem],
        out_specs=[vmem, anywhere, vmem],
        scratch_shapes=[
            pltpu.VMEM((local_count, group, half_rows, depth), jnp.bfloat16),
            pltpu.VMEM((2 * cols, depth), jnp.bfloat16),
            pltpu.VMEM(sums, jnp.bfloat16),
            pltpu.VMEM(sums, jnp.bfloat16),
            pltpu.VMEM(sums, jnp.bfloat16),
            pltpu.VMEM(sums[2:], jnp.float32),
            pltpu.VMEM(sums[1:], jnp.bfloat16),
            pltpu.VMEM((group, half_rows, 2 * cols), jnp.bfloat16),
            pltpu.VMEM((local_count,) + counts.shape, jnp.float32),
            dma((2,)),
            dma((2,)),
            dma((local_count, SPLITS)),
            dma((local_count, group, SPLITS)),
            dma((local_count, group, len(bits), SPLITS)),
            dma(grid),
            dma(grid),
            dma(grid),
            dma(grid),
            dma((local_count, group)),
            dma((local_count, group)),
            dma((local_count, 2, SPREAD)),
            dma((local_count, node_count, all_bits, SPREAD)),
            dma((local_count, node_count, SPREAD)),
            dma((local_count,)),
            dma((local_count,)),
        ],
        compiler_params=pltpu.CompilerParams(
            collective_id=0, has_side_effects=True, vmem_limit_bytes=58 * 2**20
        ),
        cost_estimate=pl.CostEstimate(
            flops=4 * local_count * group * half_rows * depth * cols,
            bytes_accessed=2 * (x_slices.size + weight.size),
            transcendentals=0,
        ),
    )(x_slices, weight, bias_pair, out_weight, counts)


def second_kernel(local_count, place_ref, mid_ref, own_ref, weight_ref, bias_ref, out_ref, total):
    group, _, depth = mid_ref.shape
    width = weight_ref.shape[3]
    column = lax.rem(place_ref[0] + pl.program_id(0), local_count)
    main = depth // 256 * 256

    def product(pick):
        sum_rows = jnp.zeros(total.shape, jnp.float32)
        for g in range(group):
            rhs = pick(g)
            for lower, upper in ((0, main), (main, depth)):
                if upper > lower:
                    sum_rows += jnp.dot(
                        mid_ref[g, :, lower:upper],
                        rhs[lower:upper],
                        preferred_element_type=jnp.float32,
                    )
        total[...] = sum_rows

    @pl.when(pl.program_id(0) == 0)
    def _():
        product(
            lambda g: jnp.concatenate(
                [own_ref[place_ref[1 + g]], own_ref[place_ref[1 + g] + COLUMN_BIT]], 0
            )
        )

    @pl.when(pl.program_id(0) > 0)
    def _():
        product(lambda g: weight_ref[g, 0])

    for z in range(local_count):

        @pl.when(column == z)
        def _():
            value = total[...] + bias_ref[:, z * width : (z + 1) * width]
            out_ref[...] = value.astype(jnp.bfloat16).reshape(out_ref.shape)


def second_product(places, mid, own_weight, weight, bias_row):
    group, local_count, pair_cols, width = weight.shape
    cols = pair_cols // 2
    node_count = 2 * group
    half_rows = mid.shape[1]
    joined = width % LANES == 0

    def column(z, place):
        return lax.rem(place[0] + z, local_count)

    def fetched(z, place):
        return lax.rem(place[0] + jnp.maximum(z, 1), local_count)

    if joined:
        out_shape = (half_rows, local_count * width)
        out_block = pl.BlockSpec((half_rows, width), lambda z, place: (0, column(z, place)))
    else:
        out_shape = (local_count, half_rows, width)
        out_block = pl.BlockSpec((1, half_rows, width), lambda z, place: (column(z, place), 0, 0))
    product = pl.pallas_call(
        functools.partial(second_kernel, local_count),
        grid_spec=pltpu.PrefetchScalarGridSpec(
            num_scalar_prefetch=1,
            grid=(local_count,),
            in_specs=[
                pl.BlockSpec(mid.shape, lambda z, place: (0, 0, 0)),
                pl.BlockSpec((node_count, cols, width), lambda z, place: (0, 0, 0)),
                pl.BlockSpec(
                    (group, 1, pair_cols, width), lambda z, place: (0, fetched(z, place), 0, 0)
                ),
                pl.BlockSpec((1, local_count * width + 8 * LANES), lambda z, place: (0, 0)),
            ],
            out_specs=out_block,
            scratch_shapes=[pltpu.VMEM((half_rows, width), jnp.float32)],
        ),
        out_shape=jax.ShapeDtypeStruct(out_shape, jnp.bfloat16),
        compiler_params=pltpu.CompilerParams(vmem_limit_bytes=48 * 2**20),
        cost_estimate=pl.CostEstimate(
            flops=2 * half_rows * weight.size, bytes_accessed=2 * weight.size, transcendentals=0
        ),
    )(
        places,
        mid,
        own_weight.reshape(node_count, cols, width),
        weight,
        jnp.pad(bias_row, (0, 8 * LANES))[None, :],
    )
    if joined:
        return product
    return jnp.transpose(product, (1, 0, 2)).reshape(half_rows, local_count * width)


def row_grads(hidden_f, grad_rows, weight, gain, keep):
    inv_rms = lax.rsqrt(jnp.mean(hidden_f * hidden_f, -1, keepdims=True) + 1e-06)
    unit = hidden_f * inv_rms
    normed = (unit * gain * keep).astype(jnp.bfloat16)
    grad_normed = lax.dot_general(
        grad_rows, weight, (((1,), (1,)), ((), ())), preferred_element_type=jnp.float32
    )
    part = jnp.sum(grad_normed * unit, 0, keepdims=True) * keep
    scaled = grad_normed * gain
    moment = jnp.mean(scaled * hidden_f, -1, keepdims=True)
    grad_hidden = inv_rms * scaled - hidden_f * (inv_rms * inv_rms * inv_rms * moment)
    return normed, part, grad_hidden.astype(jnp.bfloat16)


def add_part(part_ref, part):
    @pl.when(pl.program_id(0) == 0)
    def _():
        part_ref[...] = part

    @pl.when(pl.program_id(0) > 0)
    def _():
        part_ref[...] += part


def text_kernel(
    image_ref, text_ref, grad_ref, weight_ref, gain_ref, out_ref, normed_ref, part_ref
):
    keep = jnp.where(image_ref[pl.program_id(0)] > 0, 0.0, 1.0)
    normed_ref[0], part, out_ref[0] = row_grads(
        text_ref[0].astype(jnp.float32), grad_ref[0], weight_ref[...], gain_ref[...], keep
    )
    add_part(part_ref, part)


def image_kernel(
    block_ref,
    filled_ref,
    arrived_ref,
    grad_ref,
    weight_ref,
    gain_ref,
    text_out_ref,
    out_ref,
    normed_ref,
    part_ref,
):
    filled = filled_ref[pl.program_id(0)] > 0
    normed_ref[0], part, grad_hidden = row_grads(
        arrived_ref[0].astype(jnp.float32),
        grad_ref[0],
        weight_ref[...],
        gain_ref[...],
        jnp.where(filled, 1.0, 0.0),
    )
    add_part(part_ref, part)

    @pl.when(filled)
    def _():
        out_ref[0] = grad_hidden

    @pl.when(jnp.logical_not(filled))
    def _():
        out_ref[0] = text_out_ref[0]


def cost(steps, rows, width, values):
    return pl.CostEstimate(
        flops=2 * steps * rows * width * values,
        bytes_accessed=6 * steps * rows * width + 2 * width * values,
        transcendentals=0,
    )


def text_grads(is_image, text, value_grad, v_full, gain):
    blocks, rows, width = text.shape
    values = value_grad.shape[2]
    row_block = pl.BlockSpec((1, rows, width), lambda b, image: (b, 0, 0))
    one_row = pl.BlockSpec((1, width), lambda b, image: (0, 0))
    return pl.pallas_call(
        text_kernel,
        grid_spec=pltpu.PrefetchScalarGridSpec(
            num_scalar_prefetch=1,
            grid=(blocks,),
            in_specs=[
                row_block,
                pl.BlockSpec((1, rows, values), lambda b, image: (b, 0, 0)),
                pl.BlockSpec((width, values), lambda b, image: (0, 0)),
                one_row,
            ],
            out_specs=[row_block, row_block, one_row],
        ),
        out_shape=[
            jax.ShapeDtypeStruct((blocks, rows, width), jnp.bfloat16),
            jax.ShapeDtypeStruct((blocks, rows, width), jnp.bfloat16),
            jax.ShapeDtypeStruct((1, width), jnp.float32),
        ],
        cost_estimate=cost(blocks, rows, width, values),
    )(is_image, text, value_grad, v_full, gain)


def image_grads(block_of_piece, filled, arrived, value_grad, v_full, gain, text_out):
    pieces, rows, width = arrived.shape
    values = value_grad.shape[2]
    piece_rows = pl.BlockSpec((1, rows, width), lambda p, block, full: (p, 0, 0))
    block_rows = pl.BlockSpec((1, rows, width), lambda p, block, full: (block[p], 0, 0))
    one_row = pl.BlockSpec((1, width), lambda p, block, full: (0, 0))
    return pl.pallas_call(
        image_kernel,
        grid_spec=pltpu.PrefetchScalarGridSpec(
            num_scalar_prefetch=2,
            grid=(pieces,),
            in_specs=[
                piece_rows,
                pl.BlockSpec((1, rows, values), lambda p, block, full: (p, 0, 0)),
                pl.BlockSpec((width, values), lambda p, block, full: (0, 0)),
                one_row,
                block_rows,
            ],
            out_specs=[block_rows, piece_rows, one_row],
        ),
        out_shape=[
            jax.ShapeDtypeStruct(text_out.shape, jnp.bfloat16),
            jax.ShapeDtypeStruct((pieces, rows, width), jnp.bfloat16),
            jax.ShapeDtypeStruct((1, width), jnp.float32),
        ],
        input_output_aliases={6: 0},
        cost_estimate=cost(pieces, rows, width, values),
    )(block_of_piece, filled, arrived, value_grad, v_full, gain, text_out)


def gather_kernel(
    node_count,
    local_count,
    normed_ref,
    grad_ref,
    text_ref,
    vector_ref,
    out_ref,
    vector_out_ref,
    tot,
    pair_out,
    pair_in,
    chip_out,
    chip_in,
    line_out,
    line_in,
    vec_pair,
    vec_sum,
    vec_chip,
    vec_line,
    pair_sems,
    chip_send,
    chip_recv,
    line_send,
    line_recv,
    vec_pair_sems,
    vec_chip_send,
    vec_chip_recv,
    vec_line_send,
    vec_line_recv,
):
    node = lax.axis_index("node")
    me = lax.axis_index("local")
    chips = node_count // 2
    core = lax.rem(node, 2)
    chip = lax.div(node, 2)
    own_rows = tot.shape[1]

    barrier = pltpu.get_barrier_semaphore()
    for r in [1] + [2 * c for c in range(1, chips)]:
        pl.semaphore_signal(
            barrier, 1, device_id={"node": toggled(node, r)}, device_id_type=MESH
        )
    for step in range(1, local_count):
        pl.semaphore_signal(
            barrier, 1, device_id={"local": toggled(me, step)}, device_id_type=MESH
        )
    pl.semaphore_wait(barrier, chips + local_count - 1)

    def remote(src, dst, send, recv, axis, target):
        return pltpu.make_async_remote_copy(
            src, dst, send, recv, device_id={axis: target}, device_id_type=MESH
        )

    vec_to_pair = remote(
        vector_ref, vec_pair, vec_pair_sems.at[0], vec_pair_sems.at[1], "node", flip(node, 1)
    )
    vec_to_pair.start()

    product = lax.dot_general(
        normed_ref[...], grad_ref[...], (((0,), (0,)), ((), ())), preferred_element_type=jnp.float32
    )
    if own_rows % 8 == 0:
        tot[...] = product.reshape(tot.shape) + text_ref[...].astype(jnp.float32)
    else:
        for i in range(node_count * local_count):
            tot[i] = product[i * own_rows : (i + 1) * own_rows] + text_ref[i].astype(jnp.float32)

    def to_pair(k, q):
        return remote(
            pair_out.at[q, k],
            pair_in.at[q, k],
            pair_sems.at[0, q, k],
            pair_sems.at[1, q, k],
            "node",
            flip(node, 1),
        )

    def to_chip(q, r):
        return remote(
            chip_out.at[q, r],
            chip_in.at[q, r],
            chip_send.at[q, r],
            chip_recv.at[q, r],
            "node",
            toggled(node, 2 * r),
        )

    def to_line(step):
        return remote(
            line_out.at[step],
            line_in.at[step],
            line_send.at[step],
            line_recv.at[step],
            "local",
            toggled(me, step),
        )

    def vec_to_chip(r):
        return remote(
            vec_sum.at[0],
            vec_chip.at[chip],
            vec_chip_send.at[r],
            vec_chip_recv.at[r],
            "node",
            toggled(node, 2 * r),
        )

    def vec_to_line(step):
        return remote(
            vec_sum.at[1],
            vec_line.at[me],
            vec_line_send.at[step],
            vec_line_recv.at[step],
            "local",
            toggled(me, step),
        )

    def place(k, side, q):
        return (2 * k + side) * local_count + q

    steps = list(range(1, local_count)) + [0]
    for step in steps:
        q = toggled(me, step)
        for r in list(range(1, chips)) + [0]:
            k = toggled(chip, r)
            pair_out[q, k] = tot[place(k, 1 - core, q)].astype(jnp.bfloat16)
            to_pair(k, q).start()
    vec_to_pair.wait()
    vec_sum[0] = vector_ref[...] + vec_pair[...]
    vec_chip[chip] = vec_sum[0]
    for r in range(1, chips):
        vec_to_chip(r).start()
    for step in steps:
        q = toggled(me, step)
        for r in reversed(range(1, chips)):
            k = toggled(chip, r)
            to_pair(k, q).wait()
            chip_out[q, r] = (
                tot[place(k, core, q)] + pair_in[q, k].astype(jnp.float32)
            ).astype(jnp.bfloat16)
            to_chip(q, r).start()
        to_pair(chip, q).wait()
    for r in range(1, chips):
        source = toggled(chip, r)
        remote(
            vec_sum.at[0],
            vec_chip.at[source],
            vec_chip_send.at[r],
            vec_chip_recv.at[r],
            "node",
            toggled(node, 2 * r),
        ).wait()
    vec_total = vec_chip[0]
    for c in range(1, chips):
        vec_total += vec_chip[c]
    vec_sum[1] = vec_total
    vec_line[me] = vec_total
    for step in range(1, local_count):
        vec_to_line(step).start()
    for step in steps:
        q = toggled(me, step)
        value = tot[place(chip, core, q)] + pair_in[q, chip].astype(jnp.float32)
        for r in range(1, chips):
            to_chip(q, r).wait()
            value += chip_in[q, r].astype(jnp.float32)
        if step:
            line_out[step] = value.astype(jnp.bfloat16)
            to_line(step).start()
    for step in range(1, local_count):
        source = toggled(me, step)
        remote(
            vec_sum.at[1],
            vec_line.at[source],
            vec_line_send.at[step],
            vec_line_recv.at[step],
            "local",
            source,
        ).wait()
    vec_total = vec_line[0]
    for z in range(1, local_count):
        vec_total += vec_line[z]
    vector_out_ref[...] = vec_total / node_count
    for step in range(1, local_count):
        to_line(step).wait()
        value += line_in[step].astype(jnp.float32)
    out_ref[...] = value / node_count


def gather_grads(normed, grads, text_sum, vector, node_count, local_count):
    rows, values = text_sum.shape
    own_rows = rows // (node_count * local_count)
    chips = node_count // 2
    dma = pltpu.SemaphoreType.DMA
    tile = (own_rows, values)
    vec = vector.shape
    return pl.pallas_call(
        functools.partial(gather_kernel, node_count, local_count),
        out_shape=[
            jax.ShapeDtypeStruct(tile, jnp.float32),
            jax.ShapeDtypeStruct(vec, jnp.float32),
        ],
        in_specs=[pl.BlockSpec(memory_space=pltpu.VMEM)] * 4,
        out_specs=[pl.BlockSpec(memory_space=pltpu.VMEM)] * 2,
        scratch_shapes=[
            pltpu.VMEM((node_count * local_count,) + tile, jnp.float32),
            pltpu.VMEM((local_count, chips) + tile, jnp.bfloat16),
            pltpu.VMEM((local_count, chips) + tile, jnp.bfloat16),
            pltpu.VMEM((local_count, chips) + tile, jnp.bfloat16),
            pltpu.VMEM((local_count, chips) + tile, jnp.bfloat16),
            pltpu.VMEM((local_count,) + tile, jnp.bfloat16),
            pltpu.VMEM((local_count,) + tile, jnp.bfloat16),
            pltpu.VMEM(vec, jnp.float32),
            pltpu.VMEM((2,) + vec, jnp.float32),
            pltpu.VMEM((chips,) + vec, jnp.float32),
            pltpu.VMEM((local_count,) + vec, jnp.float32),
            dma((2, local_count, chips)),
            dma((local_count, chips)),
            dma((local_count, chips)),
            dma((local_count,)),
            dma((local_count,)),
            dma((2,)),
            dma((chips,)),
            dma((chips,)),
            dma((local_count,)),
            dma((local_count,)),
        ],
        compiler_params=pltpu.CompilerParams(
            collective_id=1, has_side_effects=True, vmem_limit_bytes=48 * 2**20
        ),
        cost_estimate=pl.CostEstimate(
            flops=2 * normed.size * values, bytes_accessed=2 * text_sum.size, transcendentals=0
        ),
    )(normed, grads, text_sum.reshape((node_count * local_count,) + tile), vector)


def weight_grad(normed, grad_rows):
    return lax.dot_general(
        normed, grad_rows, (((0,), (0,)), ((), ())), preferred_element_type=jnp.float32
    )


def per_device(
    vit_tiles,
    tile_counts,
    block_of_piece,
    segment_ids,
    text_rows,
    cotangent,
    proj_weight,
    proj_bias,
    out_weight,
    out_bias,
    ln_gain,
    ln_bias,
    norm_gain,
    v_weight,
):
    local_count = lax.axis_size("local")
    node_count = lax.axis_size("node")
    node = lax.axis_index("node")
    blocks = text_rows.shape[1]
    share_rows = text_rows.shape[2]
    model_width = text_rows.shape[3]
    out_cols = out_weight.shape[1]
    shard_cols = proj_weight.shape[1]
    x_slices = slices(vit_tiles[0, 0], ln_gain, ln_bias, local_count)
    side = lax.rem(lax.div(node, COLUMN_BIT), 2)
    low_shard = node - COLUMN_BIT * side
    bias_pair = jnp.concatenate(
        [
            lax.dynamic_slice_in_dim(proj_bias, shard * shard_cols, shard_cols, 0)
            for shard in (low_shard, low_shard + COLUMN_BIT)
        ]
    )[None, :]
    v_full = lax.all_gather(v_weight, ("node", "local"), axis=0, tiled=True)
    _, masks = row_masks(node_count)
    places = jnp.stack(
        [lax.axis_index("local")]
        + [toggled(low_shard, m) for m in masks]
    )
    doc_ids = segment_ids[0].reshape(-1)
    doc_hits = (doc_ids[:, None] == lax.iota(jnp.int32, DOCS)[None, :]).astype(jnp.float32)
    doc_counts = jnp.pad(jnp.sum(doc_hits, 0)[None, :], ((0, 7), (0, LANES - DOCS)))
    mid, out_spread, doc_sizes = project(
        x_slices,
        jnp.transpose(proj_weight),
        bias_pair,
        out_weight,
        doc_counts,
        node_count,
        local_count,
    )
    doc_sizes = doc_sizes[0, :DOCS]
    doc_weight = blocks * share_rows * local_count / (DOCS * doc_sizes)
    token_weight = jnp.dot(doc_hits, doc_weight, precision=lax.Precision.HIGHEST)
    value_grad = (
        cotangent[0].reshape(-1, cotangent.shape[3]).astype(jnp.float32) * token_weight[:, None]
    ).astype(jnp.bfloat16)
    bias_part = jnp.sum(value_grad.astype(jnp.float32), 0)
    piece_total = local_count // 2
    piece_ids = lax.iota(jnp.int32, piece_total)
    filled = piece_ids % SLOTS < jnp.repeat(tile_counts[0], SLOTS)
    chosen = (block_of_piece[0][None, :] == lax.iota(jnp.int32, blocks)[:, None]) & filled[None, :]
    is_image = jnp.any(chosen, 1).astype(jnp.int32)
    gain_row = norm_gain[None, :]
    value_blocks = value_grad.reshape(blocks, share_rows, -1)
    value_pieces = value_blocks[block_of_piece[0]]
    text_out, text_normed, text_part = text_grads(
        is_image, text_rows[0], value_blocks, v_full, gain_row
    )
    text_sum = weight_grad(text_normed.reshape(-1, model_width), value_grad).astype(jnp.bfloat16)
    flat_pieces = value_pieces.reshape(-1, value_pieces.shape[2])
    arrived = second_product(places, mid, out_weight, out_spread, out_bias)
    arrived = arrived.reshape(piece_total, share_rows, model_width)
    grad_hidden, image_normed, image_part = image_grads(
        block_of_piece[0], filled.astype(jnp.int32), arrived, value_pieces, v_full, gain_row, text_out
    )
    gain_part = text_part + image_part
    vector = jnp.concatenate([bias_part, gain_part[0]])
    length = vector.shape[0]
    vector = jnp.pad(vector, (0, -length % (8 * LANES))).reshape(8, -1)
    grad_weight, vector = gather_grads(
        image_normed.reshape(-1, model_width),
        flat_pieces,
        text_sum,
        vector,
        node_count,
        local_count,
    )
    vector = vector.reshape(-1)
    values = bias_part.shape[0]
    return (grad_hidden[None], grad_weight, vector[:values], vector[values:length])


def solution(mesh):
    in_specs = (
        P("node", "local", None, None),
        P("node", None),
        P("node", None),
        P("node", None, "local"),
        P("node", None, "local", None),
        P("node", None, "local", None),
        P("local", "node"),
        P(),
        P(None, "local"),
        P(),
        P(),
        P(),
        P(),
        P(("node", "local"), None),
    )
    out_specs = (P("node", None, "local", None), P(("node", "local"), None), P(), P())
    return jax.shard_map(
        per_device, mesh=mesh, in_specs=in_specs, out_specs=out_specs, check_vma=False
    )
```

```python
import functools

import jax
import jax.numpy as jnp
from jax import lax
from jax.experimental import pallas as pl
from jax.experimental.pallas import tpu as pltpu
from jax.sharding import PartitionSpec as P

SLOTS = 2
DOCS = 16
LANES = 128
COLUMN_BIT = 2
SPLITS = 2
SPREAD_PIECES = 32
MESH = pl.DeviceIdType.MESH


def flip(index, bit):
    return index + bit - 2 * bit * lax.rem(lax.div(index, bit), 2)


def bits_below(count):
    return [1 << b for b in range(count.bit_length() - 1)]


def row_masks(node_count):
    bits = [b for b in bits_below(node_count) if b != COLUMN_BIT]
    masks = [m for m in range(node_count) if not m & COLUMN_BIT]
    return bits, masks


def toggled(index, mask):
    for b in range(mask.bit_length()):
        if mask >> b & 1:
            index = flip(index, 1 << b)
    return index


def visit_order(index, step, count):
    if count == 4:
        middle = lax.rem(lax.div(index + 1, 2), 2)
        step = step + middle * lax.div(step, 2) * (5 - 2 * step)
    total = 0
    for bit in bits_below(count):
        total = total + bit * lax.rem(lax.div(index, bit) + lax.div(step, bit), 2)
    return total


def slice_kernel(local_count, x_ref, scale_ref, shift_ref, out_ref):
    values = x_ref[...].astype(jnp.float32)
    average = jnp.mean(values, -1, keepdims=True)
    centred = values - average
    variance = jnp.mean(centred * centred, -1, keepdims=True)
    normed = centred * lax.rsqrt(variance + 1e-05) * scale_ref[...] + shift_ref[...]
    depth = out_ref.shape[2]
    for k in range(local_count):
        out_ref[k] = normed[:, k * depth : (k + 1) * depth].astype(jnp.bfloat16)


def slices(vit_rows, scale_vec, shift_vec, local_count):
    half_rows, width = vit_rows.shape
    depth = width // local_count
    step_rows = 16
    one_row = pl.BlockSpec((1, width), lambda i: (0, 0))
    return pl.pallas_call(
        functools.partial(slice_kernel, local_count),
        grid=(half_rows // step_rows,),
        in_specs=[pl.BlockSpec((step_rows, width), lambda i: (i, 0)), one_row, one_row],
        out_specs=pl.BlockSpec((local_count, step_rows, depth), lambda i: (0, i, 0)),
        out_shape=jax.ShapeDtypeStruct((local_count, half_rows, depth), jnp.bfloat16),
        cost_estimate=pl.CostEstimate(
            flops=10 * vit_rows.size, bytes_accessed=4 * vit_rows.size, transcendentals=0
        ),
    )(vit_rows, scale_vec[None, :], shift_vec[None, :])


def project_kernel(
    node_count,
    local_count,
    x_ref,
    w_ref,
    bias_ref,
    out_w_ref,
    count_ref,
    v_ref,
    mid_ref,
    spread_ref,
    size_ref,
    v_out,
    rows,
    weights,
    part,
    from_low,
    from_high,
    total,
    final,
    landed,
    counts,
    w_sems,
    own_sems,
    hop_sem,
    recv_sem,
    fwd_sem,
    up_send,
    up_recv,
    down_send,
    down_recv,
    swap_send,
    swap_recv,
    line_send,
    spread_send,
    spread_recv,
    count_send,
    count_recv,
    v_line_send,
    v_send,
    v_recv,
):
    node = lax.axis_index("node")
    me = lax.axis_index("local")
    last = local_count - 1
    bits, masks = row_masks(node_count)
    all_bits = bits_below(node_count)
    group = len(masks)
    half_rows = x_ref.shape[1]
    depth = x_ref.shape[2]
    shard = w_ref.shape[0]
    piece = half_rows // SPLITS
    run = half_rows // local_count
    side = lax.rem(lax.div(node, COLUMN_BIT), 2)
    split = SPREAD_PIECES // node_count
    above = lax.rem(me + 1, local_count)
    below = lax.rem(me + last, local_count)
    at_end = (me == 0) | (me == last)

    barrier = pltpu.get_barrier_semaphore()
    for step in range(1, local_count):
        pl.semaphore_signal(
            barrier, 1, device_id={"local": visit_order(me, step, local_count)}, device_id_type=MESH
        )
    for mask in [COLUMN_BIT] + masks[1:]:
        pl.semaphore_signal(
            barrier, 1, device_id={"node": toggled(node, mask)}, device_id_type=MESH
        )
    pl.semaphore_wait(barrier, local_count - 1 + group)

    shard_rows = pl.ds(pl.multiple_of(side * shard, 8), shard)
    w_copy = pltpu.make_async_remote_copy(
        w_ref,
        weights.at[shard_rows],
        w_sems.at[0],
        w_sems.at[1],
        device_id={"node": flip(node, COLUMN_BIT)},
        device_id_type=MESH,
    )
    w_copy.start()

    def count_copy(target, source):
        return pltpu.make_async_remote_copy(
            count_ref,
            counts.at[source],
            count_send.at[target],
            count_recv.at[source],
            device_id={"local": target},
            device_id_type=MESH,
        )

    for step in range(1, local_count):
        count_copy(visit_order(me, step, local_count), me).start()

    def part_rows(s):
        return pl.ds(pl.multiple_of(s * piece, 16), piece)

    def hop(target, source, s):
        return pltpu.make_async_remote_copy(
            x_ref.at[target, part_rows(s)],
            rows.at[source, 0, part_rows(s)],
            hop_sem.at[target, s],
            recv_sem.at[source, 0, s],
            device_id={"local": target},
            device_id_type=MESH,
        )

    def forward_bits(mask):
        return [b for b in reversed(bits) if mask == 0 or b < (mask & -mask)]

    def forward(slot, g, bit, s, origin):
        src = x_ref.at[slot, part_rows(s)] if origin else rows.at[slot, g, part_rows(s)]
        return pltpu.make_async_remote_copy(
            src,
            rows.at[slot, masks.index(masks[g] | bit), part_rows(s)],
            fwd_sem.at[slot, g, bits.index(bit), s],
            recv_sem.at[slot, masks.index(masks[g] | bit), s],
            device_id={"node": flip(node, bit)},
            device_id_type=MESH,
        )

    def wait_rows(slot, g, s):
        pltpu.make_async_remote_copy(
            rows.at[slot, g, part_rows(s)],
            rows.at[slot, g, part_rows(s)],
            hop_sem.at[slot, s],
            recv_sem.at[slot, g, s],
            device_id={"node": flip(node, 1)},
            device_id_type=MESH,
        ).wait_recv()

    strip = shard // split

    def strip_rows(s, base=0):
        return pl.ds(pl.multiple_of(base + s * strip, 8), strip)

    def held(mask, slot, s, source_mask=None):
        other = (mask if source_mask is None else source_mask) // COLUMN_BIT % 2
        return spread_ref.at[
            masks.index(mask & ~COLUMN_BIT),
            slot,
            strip_rows(s, shard * (other + side * (1 - 2 * other))),
        ]

    def line(source, s, upward, origin):
        src = (
            out_w_ref.at[strip_rows(s, node * shard)]
            if origin
            else held(0, source, s)
        )
        return pltpu.make_async_remote_copy(
            src,
            held(0, source, s),
            line_send.at[source, upward, s],
            spread_recv.at[source, 0, s],
            device_id={"local": above if upward else below},
            device_id_type=MESH,
        )

    def start_lines():
        @pl.when(me < last)
        def _():
            for s in range(split):
                line(me, s, 1, True).start()

        @pl.when(me > 0)
        def _():
            for s in range(split):
                line(me, s, 0, True).start()

    def spread_order(s):
        wide = [b for b in all_bits if b > 1]
        return wide[s % len(wide) :] + wide[: s % len(wide)] + [1]

    def spread_bits(mask, s):
        order = spread_order(s)
        held = [i for i, b in enumerate(order) if mask & b]
        return order[held[-1] + 1 :] if held else order

    def spread(slot, mask, bit, s):
        return pltpu.make_async_remote_copy(
            held(mask, slot, s),
            held(mask | bit, slot, s, mask),
            spread_send.at[slot, mask, bit.bit_length() - 1, s],
            spread_recv.at[slot, mask | bit, s],
            device_id={"node": flip(node, bit)},
            device_id_type=MESH,
        )

    def wait_strip(slot, mask, s):
        pltpu.make_async_remote_copy(
            held(mask, slot, s),
            held(mask, slot, s),
            line_send.at[slot, 0, s],
            spread_recv.at[slot, mask, s],
            device_id={"node": flip(node, 1)},
            device_id_type=MESH,
        ).wait_recv()

    def take_line(step):
        slot = visit_order(me, step, local_count)
        for s in range(split):
            wait_strip(slot, 0, s)

            @pl.when((slot < me) & (me < last))
            def _():
                line(slot, s, 1, False).start()

            @pl.when((slot > me) & (me > 0))
            def _():
                line(slot, s, 0, False).start()

            for bit in spread_bits(0, s):
                spread(slot, 0, bit, s).start()

    def pass_on(step):
        slot = visit_order(me, step, local_count)
        for size in range(1, len(all_bits)):
            for s in range(split):
                for mask in range(1, node_count):
                    if bin(mask).count("1") == size and spread_bits(mask, s):
                        wait_strip(slot, mask, s)
                        for bit in spread_bits(mask, s):
                            spread(slot, mask, bit, s).start()

    def v_place(mask, slot):
        return v_out.at[toggled(node, mask) * local_count + slot]

    def v_line(source, upward, origin):
        return pltpu.make_async_remote_copy(
            v_ref if origin else v_place(0, source),
            v_place(0, source),
            v_line_send.at[source, upward],
            v_recv.at[source, 0],
            device_id={"local": above if upward else below},
            device_id_type=MESH,
        )

    def v_spread(slot, mask, bit, origin):
        return pltpu.make_async_remote_copy(
            v_ref if origin else v_place(mask, slot),
            v_place(mask, slot),
            v_send.at[slot, mask, bit.bit_length() - 1],
            v_recv.at[slot, mask | bit],
            device_id={"node": flip(node, bit)},
            device_id_type=MESH,
        )

    def v_wait(slot, mask):
        pltpu.make_async_remote_copy(
            v_place(mask, slot),
            v_place(mask, slot),
            v_line_send.at[slot, 0],
            v_recv.at[slot, mask],
            device_id={"node": flip(node, 1)},
            device_id_type=MESH,
        ).wait_recv()

    def take_values(step):
        slot = visit_order(me, step, local_count)
        v_wait(slot, 0)

        @pl.when((slot < me) & (me < last))
        def _():
            v_line(slot, 1, False).start()

        @pl.when((slot > me) & (me > 0))
        def _():
            v_line(slot, 0, False).start()

        for bit in spread_bits(0, 0):
            v_spread(slot, 0, bit, False).start()

    def pass_values(step):
        slot = visit_order(me, step, local_count)
        for size in range(1, len(all_bits)):
            for mask in range(1, node_count):
                if bin(mask).count("1") == size and spread_bits(mask, 0):
                    v_wait(slot, mask)
                    for bit in spread_bits(mask, 0):
                        v_spread(slot, mask, bit, False).start()

    @pl.when(me < last)
    def _():
        v_line(me, 1, True).start()

    @pl.when(me > 0)
    def _():
        v_line(me, 0, True).start()

    for bit in spread_bits(0, 0):
        v_spread(me, 0, bit, True).start()
    own_v = pltpu.make_async_copy(v_ref, v_place(0, me), own_sems.at[2])
    own_v.start()

    for bit in forward_bits(0):
        for s in range(SPLITS):
            forward(me, 0, bit, s, True).start()
    def start_hops(step):
        for s in range(SPLITS):
            hop(visit_order(me, step, local_count), me, s).start()

    paced = local_count == 4
    if paced:
        start_hops(1)

        @pl.when(jnp.logical_not(at_end))
        def _():
            start_hops(2)
    else:
        for step in range(1, local_count):
            start_hops(step)
    own_w = pltpu.make_async_copy(w_ref, weights.at[shard_rows], own_sems.at[0])
    own_w.start()
    own_x = pltpu.make_async_copy(x_ref.at[me], rows.at[me, 0], own_sems.at[1])
    own_x.start()

    relays = [g for g in range(1, group) if forward_bits(masks[g])]
    leaves = [g for g in range(1, group) if not forward_bits(masks[g])]

    def relay(step):
        slot = visit_order(me, step, local_count)
        for g in sorted(relays, key=lambda g: -(masks[g] & -masks[g])):
            for s in range(SPLITS):
                wait_rows(slot, g, s)
                for bit in forward_bits(masks[g]):
                    forward(slot, g, bit, s, False).start()

    def arrive(step):
        slot = visit_order(me, step, local_count)
        for s in range(SPLITS):
            wait_rows(slot, 0, s)
            for bit in forward_bits(0):
                forward(slot, 0, bit, s, False).start()
        relay(step - 1)

    def up(q, j):
        return pltpu.make_async_remote_copy(
            part.at[q, j],
            from_low.at[q, j],
            up_send.at[q, j],
            up_recv.at[q, j],
            device_id={"local": above},
            device_id_type=MESH,
        )

    def down(q, j):
        return pltpu.make_async_remote_copy(
            part.at[q, j],
            from_high.at[q, j],
            down_send.at[q, j],
            down_recv.at[q, j],
            device_id={"local": below},
            device_id_type=MESH,
        )

    def add_in(q, j, landing):
        part[q, j] = (
            part[q, j].astype(jnp.float32) + landing[q, j].astype(jnp.float32)
        ).astype(jnp.bfloat16)

    def reduce_round(r):
        def one(i, carry):
            q_up = last - i
            q_down = i
            j_up = r
            j_down = last - r

            @pl.when(q_up > me)
            def _():
                @pl.when(me > 0)
                def _():
                    up(q_up, j_up).wait_recv()
                    add_in(q_up, j_up, from_low)

                up(q_up, j_up).start()

            @pl.when(q_down < me)
            def _():
                @pl.when(me < last)
                def _():
                    down(q_down, j_down).wait_recv()
                    add_in(q_down, j_down, from_high)

                down(q_down, j_down).start()

            return carry

        lax.fori_loop(0, last, one, 0)

    def multiply(step, carry):
        slot = visit_order(me, step, local_count)

        @pl.when(step == last)
        def _():
            relay(last)

        for g in leaves:
            for s in range(SPLITS):
                wait_rows(slot, g, s)
        lhs = rows.at[slot]
        main = depth // 256 * 256
        term = jnp.zeros((group * half_rows, 2 * shard), jnp.float32)
        for lower, upper in ((0, main), (main, depth)):
            if upper > lower:
                term += lax.dot_general(
                    lhs[:, :, lower:upper].reshape(group * half_rows, upper - lower),
                    weights[:, lower:upper],
                    (((1,), (1,)), ((), ())),
                    preferred_element_type=jnp.float32,
                )
        term = term.astype(jnp.bfloat16)
        for q in range(local_count):
            for g in range(group):
                part[q, slot, g * run : (g + 1) * run, :] = term[
                    g * half_rows + q * run : g * half_rows + (q + 1) * run
                ]

        @pl.when(at_end)
        def _():
            reduce_round(step)

        return carry

    def arrive_next(step):
        arrive(step)
        if paced and step < last:

            @pl.when(at_end)
            def _():
                start_hops(step + 1)

            if step == 1:

                @pl.when(jnp.logical_not(at_end))
                def _():
                    start_hops(last)

    for step in range(1, max(2, last)):
        arrive_next(step)
    pass_values(0)
    take_values(1)
    own_w.wait()
    own_x.wait()
    own_v.wait()
    w_copy.wait_recv()
    lax.fori_loop(0, 1, multiply, 0)
    for step in range(max(2, last), local_count):
        arrive_next(step)
    start_lines()
    lax.fori_loop(1, local_count, multiply, 0)

    def middle_round(r):
        @pl.when(jnp.logical_not(at_end))
        def _():
            reduce_round(r)

    for step in range(1, local_count):
        if step > 1:
            pass_values(step - 1)
            take_values(step)
        take_line(step)
        middle_round(step - 1)
        if step > 1:
            pass_on(step - 1)
    middle_round(last)
    pass_values(last)

    def swap(j, g):
        return pltpu.make_async_remote_copy(
            final.at[j, pl.ds(g * run, run)],
            landed.at[g, pl.ds(pl.multiple_of(j * run, 16), run)],
            swap_send.at[j, g],
            swap_recv.at[j, g],
            device_id={"node": toggled(node, masks[g])},
            device_id_type=MESH,
        )

    def finish(step, carry):
        j = visit_order(last - me, step, local_count)
        total[...] = part[me, j].astype(jnp.float32)

        @pl.when(me > 0)
        def _():
            up(me, j).wait_recv()
            total[...] += from_low[me, j].astype(jnp.float32)

        @pl.when(me < last)
        def _():
            down(me, j).wait_recv()
            total[...] += from_high[me, j].astype(jnp.float32)

        value = total[...] + bias_ref[...]
        final[j] = (0.5 * value * (1.0 + lax.erf(value * (0.5**0.5)))).astype(jnp.bfloat16)
        for g in reversed(range(1, group)):
            swap(j, g).start()
        mid_ref[0, pl.ds(pl.multiple_of(j * run, 16), run), :] = final[j, 0:run, :]
        return carry

    lax.fori_loop(0, local_count, finish, 0)
    pass_on(last)

    counts_all = count_ref[...]
    for step in range(1, local_count):
        source = visit_order(me, step, local_count)
        count_copy(source, source).wait_recv()
        counts_all += counts[source]
        count_copy(source, me).wait_send()
    size_ref[...] = counts_all

    def settle(j, carry):
        for g in range(1, group):
            swap(j, g).wait()
        return carry

    lax.fori_loop(0, local_count, settle, 0)
    for g in range(1, group):
        mid_ref[g] = landed[g]

    w_copy.wait_send()
    for step in range(1, local_count):
        for s in range(SPLITS):
            hop(visit_order(me, step, local_count), me, s).wait_send()

    def drain(slot, carry):
        for g in range(group):
            for bit in forward_bits(masks[g]):
                for s in range(SPLITS):
                    forward(slot, g, bit, s, False).wait_send()

        @pl.when((slot <= me) & (me < last))
        def _():
            v_line(slot, 1, False).wait_send()

        @pl.when((slot >= me) & (me > 0))
        def _():
            v_line(slot, 0, False).wait_send()

        for mask in range(node_count):
            if mask and not spread_bits(mask, 0):
                v_wait(slot, mask)
            for bit in spread_bits(mask, 0):
                v_spread(slot, mask, bit, False).wait_send()

        for s in range(split):

            @pl.when((slot <= me) & (me < last))
            def _():
                line(slot, s, 1, False).wait_send()

            @pl.when((slot >= me) & (me > 0))
            def _():
                line(slot, s, 0, False).wait_send()

        @pl.when(slot != me)
        def _():
            for s in range(split):
                for mask in range(node_count):
                    if mask and not spread_bits(mask, s):
                        wait_strip(slot, mask, s)
                    for bit in spread_bits(mask, s):
                        spread(slot, mask, bit, s).wait_send()

        def drain_sums(j, inner):
            @pl.when(slot > me)
            def _():
                up(slot, j).wait_send()

            @pl.when(slot < me)
            def _():
                down(slot, j).wait_send()

            return inner

        lax.fori_loop(0, local_count, drain_sums, 0)
        return carry

    lax.fori_loop(0, local_count, drain, 0)


def project(x_slices, weight, bias_pair, out_weight, counts, values, node_count, local_count):
    _, half_rows, depth = x_slices.shape
    cols = weight.shape[0]
    bits, masks = row_masks(node_count)
    group = len(masks)
    run = half_rows // local_count
    split = SPREAD_PIECES // node_count
    sums = (local_count, local_count, group * run, 2 * cols)
    dma = pltpu.SemaphoreType.DMA
    grid = (local_count, local_count)
    anywhere = pl.BlockSpec(memory_space=pl.ANY)
    vmem = pl.BlockSpec(memory_space=pltpu.VMEM)
    all_bits = len(bits_below(node_count))
    return pl.pallas_call(
        functools.partial(project_kernel, node_count, local_count),
        out_shape=[
            jax.ShapeDtypeStruct((group, half_rows, 2 * cols), jnp.bfloat16),
            jax.ShapeDtypeStruct(
                (group, local_count, 2 * cols, out_weight.shape[1]), jnp.bfloat16
            ),
            jax.ShapeDtypeStruct(counts.shape, jnp.float32),
            jax.ShapeDtypeStruct((node_count * local_count,) + values.shape, jnp.bfloat16),
        ],
        in_specs=[anywhere, anywhere, vmem, anywhere, vmem, anywhere],
        out_specs=[vmem, anywhere, vmem, anywhere],
        scratch_shapes=[
            pltpu.VMEM((local_count, group, half_rows, depth), jnp.bfloat16),
            pltpu.VMEM((2 * cols, depth), jnp.bfloat16),
            pltpu.VMEM(sums, jnp.bfloat16),
            pltpu.VMEM(sums, jnp.bfloat16),
            pltpu.VMEM(sums, jnp.bfloat16),
            pltpu.VMEM(sums[2:], jnp.float32),
            pltpu.VMEM(sums[1:], jnp.bfloat16),
            pltpu.VMEM((group, half_rows, 2 * cols), jnp.bfloat16),
            pltpu.VMEM((local_count,) + counts.shape, jnp.float32),
            dma((2,)),
            dma((3,)),
            dma((local_count, SPLITS)),
            dma((local_count, group, SPLITS)),
            dma((local_count, group, len(bits), SPLITS)),
            dma(grid),
            dma(grid),
            dma(grid),
            dma(grid),
            dma((local_count, group)),
            dma((local_count, group)),
            dma((local_count, 2, split)),
            dma((local_count, node_count, all_bits, split)),
            dma((local_count, node_count, split)),
            dma((local_count,)),
            dma((local_count,)),
            dma((local_count, 2)),
            dma((local_count, node_count, all_bits)),
            dma((local_count, node_count)),
        ],
        compiler_params=pltpu.CompilerParams(
            collective_id=0, has_side_effects=True, vmem_limit_bytes=58 * 2**20
        ),
        cost_estimate=pl.CostEstimate(
            flops=4 * local_count * group * half_rows * depth * cols,
            bytes_accessed=2 * (x_slices.size + weight.size),
            transcendentals=0,
        ),
    )(x_slices, weight, bias_pair, out_weight, counts, values)


def second_kernel(local_count, place_ref, mid_ref, own_ref, weight_ref, bias_ref, out_ref, total):
    group, _, depth = mid_ref.shape
    width = weight_ref.shape[3]
    column = lax.rem(place_ref[0] + pl.program_id(0), local_count)
    main = depth // 256 * 256

    def product(pick):
        sum_rows = jnp.zeros(total.shape, jnp.float32)
        for g in range(group):
            rhs = pick(g)
            for lower, upper in ((0, main), (main, depth)):
                if upper > lower:
                    sum_rows += jnp.dot(
                        mid_ref[g, :, lower:upper],
                        rhs[lower:upper],
                        preferred_element_type=jnp.float32,
                    )
        total[...] = sum_rows

    @pl.when(pl.program_id(0) == 0)
    def _():
        product(
            lambda g: jnp.concatenate(
                [own_ref[place_ref[1 + g]], own_ref[place_ref[1 + g] + COLUMN_BIT]], 0
            )
        )

    @pl.when(pl.program_id(0) > 0)
    def _():
        product(lambda g: weight_ref[g, 0])

    for z in range(local_count):

        @pl.when(column == z)
        def _():
            value = total[...] + bias_ref[:, z * width : (z + 1) * width]
            out_ref[...] = value.astype(jnp.bfloat16).reshape(out_ref.shape)


def second_product(places, mid, own_weight, weight, bias_row):
    group, local_count, pair_cols, width = weight.shape
    cols = pair_cols // 2
    node_count = 2 * group
    half_rows = mid.shape[1]
    joined = width % LANES == 0

    def column(z, place):
        return lax.rem(place[0] + z, local_count)

    def fetched(z, place):
        return lax.rem(place[0] + jnp.maximum(z, 1), local_count)

    if joined:
        out_shape = (half_rows, local_count * width)
        out_block = pl.BlockSpec((half_rows, width), lambda z, place: (0, column(z, place)))
    else:
        out_shape = (local_count, half_rows, width)
        out_block = pl.BlockSpec((1, half_rows, width), lambda z, place: (column(z, place), 0, 0))
    product = pl.pallas_call(
        functools.partial(second_kernel, local_count),
        grid_spec=pltpu.PrefetchScalarGridSpec(
            num_scalar_prefetch=1,
            grid=(local_count,),
            in_specs=[
                pl.BlockSpec(mid.shape, lambda z, place: (0, 0, 0)),
                pl.BlockSpec((node_count, cols, width), lambda z, place: (0, 0, 0)),
                pl.BlockSpec(
                    (group, 1, pair_cols, width), lambda z, place: (0, fetched(z, place), 0, 0)
                ),
                pl.BlockSpec((1, local_count * width + 8 * LANES), lambda z, place: (0, 0)),
            ],
            out_specs=out_block,
            scratch_shapes=[pltpu.VMEM((half_rows, width), jnp.float32)],
        ),
        out_shape=jax.ShapeDtypeStruct(out_shape, jnp.bfloat16),
        compiler_params=pltpu.CompilerParams(vmem_limit_bytes=48 * 2**20),
        cost_estimate=pl.CostEstimate(
            flops=2 * half_rows * weight.size, bytes_accessed=2 * weight.size, transcendentals=0
        ),
    )(
        places,
        mid,
        own_weight.reshape(node_count, cols, width),
        weight,
        jnp.pad(bias_row, (0, 8 * LANES))[None, :],
    )
    if joined:
        return product
    return jnp.transpose(product, (1, 0, 2)).reshape(half_rows, local_count * width)


def row_grads(hidden_f, grad_rows, weight, gain, keep):
    inv_rms = lax.rsqrt(jnp.mean(hidden_f * hidden_f, -1, keepdims=True) + 1e-06)
    unit = hidden_f * inv_rms
    normed = (unit * gain * keep).astype(jnp.bfloat16)
    grad_normed = lax.dot_general(
        grad_rows, weight, (((1,), (1,)), ((), ())), preferred_element_type=jnp.float32
    )
    part = jnp.sum(grad_normed * unit, 0, keepdims=True) * keep
    scaled = grad_normed * gain
    moment = jnp.mean(scaled * hidden_f, -1, keepdims=True)
    grad_hidden = inv_rms * scaled - hidden_f * (inv_rms * inv_rms * inv_rms * moment)
    return normed, part, grad_hidden.astype(jnp.bfloat16)


def add_part(part_ref, part):
    @pl.when(pl.program_id(0) == 0)
    def _():
        part_ref[...] = part

    @pl.when(pl.program_id(0) > 0)
    def _():
        part_ref[...] += part


def text_kernel(
    image_ref, text_ref, grad_ref, weight_ref, gain_ref, out_ref, normed_ref, part_ref
):
    keep = jnp.where(image_ref[pl.program_id(0)] > 0, 0.0, 1.0)
    normed_ref[0], part, out_ref[0] = row_grads(
        text_ref[0].astype(jnp.float32), grad_ref[0], weight_ref[...], gain_ref[...], keep
    )
    add_part(part_ref, part)


def image_kernel(
    block_ref,
    filled_ref,
    arrived_ref,
    grad_ref,
    weight_ref,
    gain_ref,
    text_out_ref,
    out_ref,
    normed_ref,
    part_ref,
):
    filled = filled_ref[pl.program_id(0)] > 0
    normed_ref[0], part, grad_hidden = row_grads(
        arrived_ref[0].astype(jnp.float32),
        grad_ref[0],
        weight_ref[...],
        gain_ref[...],
        jnp.where(filled, 1.0, 0.0),
    )
    add_part(part_ref, part)

    @pl.when(filled)
    def _():
        out_ref[0] = grad_hidden

    @pl.when(jnp.logical_not(filled))
    def _():
        out_ref[0] = text_out_ref[0]


def cost(steps, rows, width, values):
    return pl.CostEstimate(
        flops=2 * steps * rows * width * values,
        bytes_accessed=6 * steps * rows * width + 2 * width * values,
        transcendentals=0,
    )


def text_grads(is_image, text, value_grad, v_full, gain):
    blocks, rows, width = text.shape
    values = value_grad.shape[2]
    row_block = pl.BlockSpec((1, rows, width), lambda b, image: (b, 0, 0))
    one_row = pl.BlockSpec((1, width), lambda b, image: (0, 0))
    return pl.pallas_call(
        text_kernel,
        grid_spec=pltpu.PrefetchScalarGridSpec(
            num_scalar_prefetch=1,
            grid=(blocks,),
            in_specs=[
                row_block,
                pl.BlockSpec((1, rows, values), lambda b, image: (b, 0, 0)),
                pl.BlockSpec((width, values), lambda b, image: (0, 0)),
                one_row,
            ],
            out_specs=[row_block, row_block, one_row],
        ),
        out_shape=[
            jax.ShapeDtypeStruct((blocks, rows, width), jnp.bfloat16),
            jax.ShapeDtypeStruct((blocks, rows, width), jnp.bfloat16),
            jax.ShapeDtypeStruct((1, width), jnp.float32),
        ],
        cost_estimate=cost(blocks, rows, width, values),
    )(is_image, text, value_grad, v_full, gain)


def image_grads(block_of_piece, filled, arrived, value_grad, v_full, gain, text_out):
    pieces, rows, width = arrived.shape
    values = value_grad.shape[2]
    piece_rows = pl.BlockSpec((1, rows, width), lambda p, block, full: (p, 0, 0))
    block_rows = pl.BlockSpec((1, rows, width), lambda p, block, full: (block[p], 0, 0))
    one_row = pl.BlockSpec((1, width), lambda p, block, full: (0, 0))
    return pl.pallas_call(
        image_kernel,
        grid_spec=pltpu.PrefetchScalarGridSpec(
            num_scalar_prefetch=2,
            grid=(pieces,),
            in_specs=[
                piece_rows,
                pl.BlockSpec((1, rows, values), lambda p, block, full: (p, 0, 0)),
                pl.BlockSpec((width, values), lambda p, block, full: (0, 0)),
                one_row,
                block_rows,
            ],
            out_specs=[block_rows, piece_rows, one_row],
        ),
        out_shape=[
            jax.ShapeDtypeStruct(text_out.shape, jnp.bfloat16),
            jax.ShapeDtypeStruct((pieces, rows, width), jnp.bfloat16),
            jax.ShapeDtypeStruct((1, width), jnp.float32),
        ],
        input_output_aliases={6: 0},
        cost_estimate=cost(pieces, rows, width, values),
    )(block_of_piece, filled, arrived, value_grad, v_full, gain, text_out)


def gather_kernel(
    node_count,
    local_count,
    normed_ref,
    grad_ref,
    text_ref,
    vector_ref,
    out_ref,
    vector_out_ref,
    tot,
    pair_out,
    pair_in,
    chip_out,
    chip_in,
    line_out,
    line_in,
    vec_pair,
    vec_sum,
    vec_chip,
    vec_line,
    pair_sems,
    chip_send,
    chip_recv,
    line_send,
    line_recv,
    vec_pair_sems,
    vec_chip_send,
    vec_chip_recv,
    vec_line_send,
    vec_line_recv,
):
    node = lax.axis_index("node")
    me = lax.axis_index("local")
    chips = node_count // 2
    core = lax.rem(node, 2)
    chip = lax.div(node, 2)
    own_rows = tot.shape[1]

    barrier = pltpu.get_barrier_semaphore()
    for r in [1] + [2 * c for c in range(1, chips)]:
        pl.semaphore_signal(
            barrier, 1, device_id={"node": toggled(node, r)}, device_id_type=MESH
        )
    for step in range(1, local_count):
        pl.semaphore_signal(
            barrier, 1, device_id={"local": toggled(me, step)}, device_id_type=MESH
        )
    pl.semaphore_wait(barrier, chips + local_count - 1)

    def remote(src, dst, send, recv, axis, target):
        return pltpu.make_async_remote_copy(
            src, dst, send, recv, device_id={axis: target}, device_id_type=MESH
        )

    vec_to_pair = remote(
        vector_ref, vec_pair, vec_pair_sems.at[0], vec_pair_sems.at[1], "node", flip(node, 1)
    )
    vec_to_pair.start()

    product = lax.dot_general(
        normed_ref[...], grad_ref[...], (((0,), (0,)), ((), ())), preferred_element_type=jnp.float32
    )
    if own_rows % 8 == 0:
        tot[...] = product.reshape(tot.shape) + text_ref[...].astype(jnp.float32)
    else:
        for i in range(node_count * local_count):
            tot[i] = product[i * own_rows : (i + 1) * own_rows] + text_ref[i].astype(jnp.float32)

    def to_pair(k, q):
        return remote(
            pair_out.at[q, k],
            pair_in.at[q, k],
            pair_sems.at[0, q, k],
            pair_sems.at[1, q, k],
            "node",
            flip(node, 1),
        )

    def to_chip(q, r):
        return remote(
            chip_out.at[q, r],
            chip_in.at[q, r],
            chip_send.at[q, r],
            chip_recv.at[q, r],
            "node",
            toggled(node, 2 * r),
        )

    def to_line(step):
        return remote(
            line_out.at[step],
            line_in.at[step],
            line_send.at[step],
            line_recv.at[step],
            "local",
            toggled(me, step),
        )

    def vec_to_chip(r):
        return remote(
            vec_sum.at[0],
            vec_chip.at[chip],
            vec_chip_send.at[r],
            vec_chip_recv.at[r],
            "node",
            toggled(node, 2 * r),
        )

    def vec_to_line(step):
        return remote(
            vec_sum.at[1],
            vec_line.at[me],
            vec_line_send.at[step],
            vec_line_recv.at[step],
            "local",
            toggled(me, step),
        )

    def place(k, side, q):
        return (2 * k + side) * local_count + q

    steps = list(range(1, local_count)) + [0]
    for step in steps:
        q = toggled(me, step)
        for r in list(range(1, chips)) + [0]:
            k = toggled(chip, r)
            pair_out[q, k] = tot[place(k, 1 - core, q)].astype(jnp.bfloat16)
            to_pair(k, q).start()
    vec_to_pair.wait()
    vec_sum[0] = vector_ref[...] + vec_pair[...]
    vec_chip[chip] = vec_sum[0]
    for r in range(1, chips):
        vec_to_chip(r).start()
    for step in steps:
        q = toggled(me, step)
        for r in reversed(range(1, chips)):
            k = toggled(chip, r)
            to_pair(k, q).wait()
            chip_out[q, r] = (
                tot[place(k, core, q)] + pair_in[q, k].astype(jnp.float32)
            ).astype(jnp.bfloat16)
            to_chip(q, r).start()
        to_pair(chip, q).wait()
    for r in range(1, chips):
        source = toggled(chip, r)
        remote(
            vec_sum.at[0],
            vec_chip.at[source],
            vec_chip_send.at[r],
            vec_chip_recv.at[r],
            "node",
            toggled(node, 2 * r),
        ).wait()
    vec_total = vec_chip[0]
    for c in range(1, chips):
        vec_total += vec_chip[c]
    vec_sum[1] = vec_total
    vec_line[me] = vec_total
    for step in range(1, local_count):
        vec_to_line(step).start()
    for step in steps:
        q = toggled(me, step)
        value = tot[place(chip, core, q)] + pair_in[q, chip].astype(jnp.float32)
        for r in range(1, chips):
            to_chip(q, r).wait()
            value += chip_in[q, r].astype(jnp.float32)
        if step:
            line_out[step] = value.astype(jnp.bfloat16)
            to_line(step).start()
    for step in range(1, local_count):
        source = toggled(me, step)
        remote(
            vec_sum.at[1],
            vec_line.at[source],
            vec_line_send.at[step],
            vec_line_recv.at[step],
            "local",
            source,
        ).wait()
    vec_total = vec_line[0]
    for z in range(1, local_count):
        vec_total += vec_line[z]
    vector_out_ref[...] = vec_total / node_count
    for step in range(1, local_count):
        to_line(step).wait()
        value += line_in[step].astype(jnp.float32)
    out_ref[...] = value / node_count


def gather_grads(normed, grads, text_sum, vector, node_count, local_count):
    rows, values = text_sum.shape
    own_rows = rows // (node_count * local_count)
    chips = node_count // 2
    dma = pltpu.SemaphoreType.DMA
    tile = (own_rows, values)
    vec = vector.shape
    return pl.pallas_call(
        functools.partial(gather_kernel, node_count, local_count),
        out_shape=[
            jax.ShapeDtypeStruct(tile, jnp.float32),
            jax.ShapeDtypeStruct(vec, jnp.float32),
        ],
        in_specs=[pl.BlockSpec(memory_space=pltpu.VMEM)] * 4,
        out_specs=[pl.BlockSpec(memory_space=pltpu.VMEM)] * 2,
        scratch_shapes=[
            pltpu.VMEM((node_count * local_count,) + tile, jnp.float32),
            pltpu.VMEM((local_count, chips) + tile, jnp.bfloat16),
            pltpu.VMEM((local_count, chips) + tile, jnp.bfloat16),
            pltpu.VMEM((local_count, chips) + tile, jnp.bfloat16),
            pltpu.VMEM((local_count, chips) + tile, jnp.bfloat16),
            pltpu.VMEM((local_count,) + tile, jnp.bfloat16),
            pltpu.VMEM((local_count,) + tile, jnp.bfloat16),
            pltpu.VMEM(vec, jnp.float32),
            pltpu.VMEM((2,) + vec, jnp.float32),
            pltpu.VMEM((chips,) + vec, jnp.float32),
            pltpu.VMEM((local_count,) + vec, jnp.float32),
            dma((2, local_count, chips)),
            dma((local_count, chips)),
            dma((local_count, chips)),
            dma((local_count,)),
            dma((local_count,)),
            dma((2,)),
            dma((chips,)),
            dma((chips,)),
            dma((local_count,)),
            dma((local_count,)),
        ],
        compiler_params=pltpu.CompilerParams(
            collective_id=1, has_side_effects=True, vmem_limit_bytes=48 * 2**20
        ),
        cost_estimate=pl.CostEstimate(
            flops=2 * normed.size * values, bytes_accessed=2 * text_sum.size, transcendentals=0
        ),
    )(normed, grads, text_sum.reshape((node_count * local_count,) + tile), vector)


def weight_grad(normed, grad_rows):
    return lax.dot_general(
        normed, grad_rows, (((0,), (0,)), ((), ())), preferred_element_type=jnp.float32
    )


def per_device(
    vit_tiles,
    tile_counts,
    block_of_piece,
    segment_ids,
    text_rows,
    cotangent,
    proj_weight,
    proj_bias,
    out_weight,
    out_bias,
    ln_gain,
    ln_bias,
    norm_gain,
    v_weight,
):
    local_count = lax.axis_size("local")
    node_count = lax.axis_size("node")
    node = lax.axis_index("node")
    blocks = text_rows.shape[1]
    share_rows = text_rows.shape[2]
    model_width = text_rows.shape[3]
    out_cols = out_weight.shape[1]
    shard_cols = proj_weight.shape[1]
    x_slices = slices(vit_tiles[0, 0], ln_gain, ln_bias, local_count)
    side = lax.rem(lax.div(node, COLUMN_BIT), 2)
    low_shard = node - COLUMN_BIT * side
    bias_pair = jnp.concatenate(
        [
            lax.dynamic_slice_in_dim(proj_bias, shard * shard_cols, shard_cols, 0)
            for shard in (low_shard, low_shard + COLUMN_BIT)
        ]
    )[None, :]
    _, masks = row_masks(node_count)
    places = jnp.stack(
        [lax.axis_index("local")]
        + [toggled(low_shard, m) for m in masks]
    )
    doc_ids = segment_ids[0].reshape(-1)
    doc_hits = (doc_ids[:, None] == lax.iota(jnp.int32, DOCS)[None, :]).astype(jnp.float32)
    doc_counts = jnp.pad(jnp.sum(doc_hits, 0)[None, :], ((0, 7), (0, LANES - DOCS)))
    mid, out_spread, doc_sizes, v_full = project(
        x_slices,
        jnp.transpose(proj_weight),
        bias_pair,
        out_weight,
        doc_counts,
        v_weight,
        node_count,
        local_count,
    )
    doc_sizes = doc_sizes[0, :DOCS]
    v_full = v_full.reshape(model_width, -1)
    doc_weight = blocks * share_rows * local_count / (DOCS * doc_sizes)
    token_weight = jnp.dot(doc_hits, doc_weight, precision=lax.Precision.HIGHEST)
    value_grad = (
        cotangent[0].reshape(-1, cotangent.shape[3]).astype(jnp.float32) * token_weight[:, None]
    ).astype(jnp.bfloat16)
    bias_part = jnp.sum(value_grad.astype(jnp.float32), 0)
    piece_total = local_count // 2
    piece_ids = lax.iota(jnp.int32, piece_total)
    filled = piece_ids % SLOTS < jnp.repeat(tile_counts[0], SLOTS)
    chosen = (block_of_piece[0][None, :] == lax.iota(jnp.int32, blocks)[:, None]) & filled[None, :]
    is_image = jnp.any(chosen, 1).astype(jnp.int32)
    gain_row = norm_gain[None, :]
    value_blocks = value_grad.reshape(blocks, share_rows, -1)
    value_pieces = value_blocks[block_of_piece[0]]
    text_out, text_normed, text_part = text_grads(
        is_image, text_rows[0], value_blocks, v_full, gain_row
    )
    text_sum = weight_grad(text_normed.reshape(-1, model_width), value_grad).astype(jnp.bfloat16)
    flat_pieces = value_pieces.reshape(-1, value_pieces.shape[2])
    arrived = second_product(places, mid, out_weight, out_spread, out_bias)
    arrived = arrived.reshape(piece_total, share_rows, model_width)
    grad_hidden, image_normed, image_part = image_grads(
        block_of_piece[0], filled.astype(jnp.int32), arrived, value_pieces, v_full, gain_row, text_out
    )
    gain_part = text_part + image_part
    vector = jnp.concatenate([bias_part, gain_part[0]])
    length = vector.shape[0]
    vector = jnp.pad(vector, (0, -length % (8 * LANES))).reshape(8, -1)
    grad_weight, vector = gather_grads(
        image_normed.reshape(-1, model_width),
        flat_pieces,
        text_sum,
        vector,
        node_count,
        local_count,
    )
    vector = vector.reshape(-1)
    values = bias_part.shape[0]
    return (grad_hidden[None], grad_weight, vector[:values], vector[values:length])


def solution(mesh):
    in_specs = (
        P("node", "local", None, None),
        P("node", None),
        P("node", None),
        P("node", None, "local"),
        P("node", None, "local", None),
        P("node", None, "local", None),
        P("local", "node"),
        P(),
        P(None, "local"),
        P(),
        P(),
        P(),
        P(),
        P(("node", "local"), None),
    )
    out_specs = (P("node", None, "local", None), P(("node", "local"), None), P(), P())
    return jax.shard_map(
        per_device, mesh=mesh, in_specs=in_specs, out_specs=out_specs, check_vma=False
    )
```

```python
import functools

import jax
import jax.numpy as jnp
from jax import lax
from jax.experimental import pallas as pl
from jax.experimental.pallas import tpu as pltpu
from jax.sharding import PartitionSpec as P

SLOTS = 2
DOCS = 16
LANES = 128
COLUMN_BIT = 2
SPLITS = 2
SPREAD_PIECES = 32
MESH = pl.DeviceIdType.MESH


def flip(index, bit):
    return index + bit - 2 * bit * lax.rem(lax.div(index, bit), 2)


def bits_below(count):
    return [1 << b for b in range(count.bit_length() - 1)]


def row_masks(node_count):
    bits = [b for b in bits_below(node_count) if b != COLUMN_BIT]
    masks = [m for m in range(node_count) if not m & COLUMN_BIT]
    return bits, masks


def toggled(index, mask):
    for b in range(mask.bit_length()):
        if mask >> b & 1:
            index = flip(index, 1 << b)
    return index


def visit_order(index, step, count):
    if count == 4:
        middle = lax.rem(lax.div(index + 1, 2), 2)
        step = step + middle * lax.div(step, 2) * (5 - 2 * step)
    total = 0
    for bit in bits_below(count):
        total = total + bit * lax.rem(lax.div(index, bit) + lax.div(step, bit), 2)
    return total


def slice_kernel(local_count, x_ref, scale_ref, shift_ref, out_ref):
    values = x_ref[...].astype(jnp.float32)
    average = jnp.mean(values, -1, keepdims=True)
    centred = values - average
    variance = jnp.mean(centred * centred, -1, keepdims=True)
    normed = centred * lax.rsqrt(variance + 1e-05) * scale_ref[...] + shift_ref[...]
    depth = out_ref.shape[2]
    for k in range(local_count):
        out_ref[k] = normed[:, k * depth : (k + 1) * depth].astype(jnp.bfloat16)


def slices(vit_rows, scale_vec, shift_vec, local_count):
    half_rows, width = vit_rows.shape
    depth = width // local_count
    step_rows = 16
    one_row = pl.BlockSpec((1, width), lambda i: (0, 0))
    return pl.pallas_call(
        functools.partial(slice_kernel, local_count),
        grid=(half_rows // step_rows,),
        in_specs=[pl.BlockSpec((step_rows, width), lambda i: (i, 0)), one_row, one_row],
        out_specs=pl.BlockSpec((local_count, step_rows, depth), lambda i: (0, i, 0)),
        out_shape=jax.ShapeDtypeStruct((local_count, half_rows, depth), jnp.bfloat16),
        cost_estimate=pl.CostEstimate(
            flops=10 * vit_rows.size, bytes_accessed=4 * vit_rows.size, transcendentals=0
        ),
    )(vit_rows, scale_vec[None, :], shift_vec[None, :])


def project_kernel(
    node_count,
    local_count,
    x_ref,
    w_ref,
    bias_ref,
    out_w_ref,
    count_ref,
    v_ref,
    mid_ref,
    spread_ref,
    size_ref,
    v_out,
    rows,
    weights,
    part,
    from_low,
    from_high,
    total,
    final,
    landed,
    counts,
    w_sems,
    own_sems,
    hop_sem,
    recv_sem,
    fwd_sem,
    up_send,
    up_recv,
    down_send,
    down_recv,
    swap_send,
    swap_recv,
    line_send,
    spread_send,
    spread_recv,
    count_send,
    count_recv,
    v_line_send,
    v_send,
    v_recv,
):
    node = lax.axis_index("node")
    me = lax.axis_index("local")
    last = local_count - 1
    bits, masks = row_masks(node_count)
    all_bits = bits_below(node_count)
    group = len(masks)
    half_rows = x_ref.shape[1]
    depth = x_ref.shape[2]
    shard = w_ref.shape[0]
    piece = half_rows // SPLITS
    run = half_rows // local_count
    side = lax.rem(lax.div(node, COLUMN_BIT), 2)
    split = SPREAD_PIECES // node_count
    above = lax.rem(me + 1, local_count)
    below = lax.rem(me + last, local_count)
    at_end = (me == 0) | (me == last)

    barrier = pltpu.get_barrier_semaphore()
    for step in range(1, local_count):
        pl.semaphore_signal(
            barrier, 1, device_id={"local": visit_order(me, step, local_count)}, device_id_type=MESH
        )
    for mask in [COLUMN_BIT] + masks[1:]:
        pl.semaphore_signal(
            barrier, 1, device_id={"node": toggled(node, mask)}, device_id_type=MESH
        )
    pl.semaphore_wait(barrier, local_count - 1 + group)

    shard_rows = pl.ds(pl.multiple_of(side * shard, 8), shard)
    w_copy = pltpu.make_async_remote_copy(
        w_ref,
        weights.at[shard_rows],
        w_sems.at[0],
        w_sems.at[1],
        device_id={"node": flip(node, COLUMN_BIT)},
        device_id_type=MESH,
    )
    w_copy.start()

    def count_copy(target, source):
        return pltpu.make_async_remote_copy(
            count_ref,
            counts.at[source],
            count_send.at[target],
            count_recv.at[source],
            device_id={"local": target},
            device_id_type=MESH,
        )

    for step in range(1, local_count):
        count_copy(visit_order(me, step, local_count), me).start()

    def part_rows(s):
        return pl.ds(pl.multiple_of(s * piece, 16), piece)

    def hop(target, source, s):
        return pltpu.make_async_remote_copy(
            x_ref.at[target, part_rows(s)],
            rows.at[source, 0, part_rows(s)],
            hop_sem.at[target, s],
            recv_sem.at[source, 0, s],
            device_id={"local": target},
            device_id_type=MESH,
        )

    def forward_bits(mask):
        return [b for b in reversed(bits) if mask == 0 or b < (mask & -mask)]

    def forward(slot, g, bit, s, origin):
        src = x_ref.at[slot, part_rows(s)] if origin else rows.at[slot, g, part_rows(s)]
        return pltpu.make_async_remote_copy(
            src,
            rows.at[slot, masks.index(masks[g] | bit), part_rows(s)],
            fwd_sem.at[slot, g, bits.index(bit), s],
            recv_sem.at[slot, masks.index(masks[g] | bit), s],
            device_id={"node": flip(node, bit)},
            device_id_type=MESH,
        )

    def wait_rows(slot, g, s):
        pltpu.make_async_remote_copy(
            rows.at[slot, g, part_rows(s)],
            rows.at[slot, g, part_rows(s)],
            hop_sem.at[slot, s],
            recv_sem.at[slot, g, s],
            device_id={"node": flip(node, 1)},
            device_id_type=MESH,
        ).wait_recv()

    strip = shard // split

    def strip_rows(s, base=0):
        return pl.ds(pl.multiple_of(base + s * strip, 8), strip)

    def held(mask, slot, s, source_mask=None):
        other = (mask if source_mask is None else source_mask) // COLUMN_BIT % 2
        return spread_ref.at[
            masks.index(mask & ~COLUMN_BIT),
            slot,
            strip_rows(s, shard * (other + side * (1 - 2 * other))),
        ]

    def line(source, s, upward, origin):
        src = (
            out_w_ref.at[strip_rows(s, node * shard)]
            if origin
            else held(0, source, s)
        )
        return pltpu.make_async_remote_copy(
            src,
            held(0, source, s),
            line_send.at[source, upward, s],
            spread_recv.at[source, 0, s],
            device_id={"local": above if upward else below},
            device_id_type=MESH,
        )

    def start_lines():
        @pl.when(me < last)
        def _():
            for s in range(split):
                line(me, s, 1, True).start()

        @pl.when(me > 0)
        def _():
            for s in range(split):
                line(me, s, 0, True).start()

    def spread_order(s):
        wide = [b for b in all_bits if b > 1]
        return wide[s % len(wide) :] + wide[: s % len(wide)] + [1]

    def spread_bits(mask, s):
        order = spread_order(s)
        held = [i for i, b in enumerate(order) if mask & b]
        return order[held[-1] + 1 :] if held else order

    def spread(slot, mask, bit, s):
        return pltpu.make_async_remote_copy(
            held(mask, slot, s),
            held(mask | bit, slot, s, mask),
            spread_send.at[slot, mask, bit.bit_length() - 1, s],
            spread_recv.at[slot, mask | bit, s],
            device_id={"node": flip(node, bit)},
            device_id_type=MESH,
        )

    def wait_strip(slot, mask, s):
        pltpu.make_async_remote_copy(
            held(mask, slot, s),
            held(mask, slot, s),
            line_send.at[slot, 0, s],
            spread_recv.at[slot, mask, s],
            device_id={"node": flip(node, 1)},
            device_id_type=MESH,
        ).wait_recv()

    def take_line(step):
        slot = visit_order(me, step, local_count)
        for s in range(split):
            wait_strip(slot, 0, s)

            @pl.when((slot < me) & (me < last))
            def _():
                line(slot, s, 1, False).start()

            @pl.when((slot > me) & (me > 0))
            def _():
                line(slot, s, 0, False).start()

            for bit in spread_bits(0, s):
                spread(slot, 0, bit, s).start()

    def pass_on(step):
        slot = visit_order(me, step, local_count)
        for size in range(1, len(all_bits)):
            for s in range(split):
                for mask in range(1, node_count):
                    if bin(mask).count("1") == size and spread_bits(mask, s):
                        wait_strip(slot, mask, s)
                        for bit in spread_bits(mask, s):
                            spread(slot, mask, bit, s).start()

    def v_place(mask, slot):
        return v_out.at[toggled(node, mask) * local_count + slot]

    def v_line(source, upward, origin):
        return pltpu.make_async_remote_copy(
            v_ref if origin else v_place(0, source),
            v_place(0, source),
            v_line_send.at[source, upward],
            v_recv.at[source, 0],
            device_id={"local": above if upward else below},
            device_id_type=MESH,
        )

    def v_spread(slot, mask, bit, origin):
        return pltpu.make_async_remote_copy(
            v_ref if origin else v_place(mask, slot),
            v_place(mask, slot),
            v_send.at[slot, mask, bit.bit_length() - 1],
            v_recv.at[slot, mask | bit],
            device_id={"node": flip(node, bit)},
            device_id_type=MESH,
        )

    def v_wait(slot, mask):
        pltpu.make_async_remote_copy(
            v_place(mask, slot),
            v_place(mask, slot),
            v_line_send.at[slot, 0],
            v_recv.at[slot, mask],
            device_id={"node": flip(node, 1)},
            device_id_type=MESH,
        ).wait_recv()

    def take_values(step):
        slot = visit_order(me, step, local_count)
        v_wait(slot, 0)

        @pl.when((slot < me) & (me < last))
        def _():
            v_line(slot, 1, False).start()

        @pl.when((slot > me) & (me > 0))
        def _():
            v_line(slot, 0, False).start()

        for bit in spread_bits(0, 0):
            v_spread(slot, 0, bit, False).start()

    def pass_values(step):
        slot = visit_order(me, step, local_count)
        for size in range(1, len(all_bits)):
            for mask in range(1, node_count):
                if bin(mask).count("1") == size and spread_bits(mask, 0):
                    v_wait(slot, mask)
                    for bit in spread_bits(mask, 0):
                        v_spread(slot, mask, bit, False).start()

    own_v = pltpu.make_async_copy(v_ref, v_place(0, me), own_sems.at[2])
    own_v.start()

    for bit in forward_bits(0):
        for s in range(SPLITS):
            forward(me, 0, bit, s, True).start()
    def start_hops(step):
        for s in range(SPLITS):
            hop(visit_order(me, step, local_count), me, s).start()

    paced = local_count == 4
    if paced:
        start_hops(1)

        @pl.when(jnp.logical_not(at_end))
        def _():
            start_hops(2)
    else:
        for step in range(1, local_count):
            start_hops(step)
    own_w = pltpu.make_async_copy(w_ref, weights.at[shard_rows], own_sems.at[0])
    own_w.start()
    own_x = pltpu.make_async_copy(x_ref.at[me], rows.at[me, 0], own_sems.at[1])
    own_x.start()

    relays = [g for g in range(1, group) if forward_bits(masks[g])]
    leaves = [g for g in range(1, group) if not forward_bits(masks[g])]

    def relay(step):
        slot = visit_order(me, step, local_count)
        for g in sorted(relays, key=lambda g: -(masks[g] & -masks[g])):
            for s in range(SPLITS):
                wait_rows(slot, g, s)
                for bit in forward_bits(masks[g]):
                    forward(slot, g, bit, s, False).start()

    def arrive(step):
        slot = visit_order(me, step, local_count)
        for s in range(SPLITS):
            wait_rows(slot, 0, s)
            for bit in forward_bits(0):
                forward(slot, 0, bit, s, False).start()
        relay(step - 1)

    def up(q, j):
        return pltpu.make_async_remote_copy(
            part.at[q, j],
            from_low.at[q, j],
            up_send.at[q, j],
            up_recv.at[q, j],
            device_id={"local": above},
            device_id_type=MESH,
        )

    def down(q, j):
        return pltpu.make_async_remote_copy(
            part.at[q, j],
            from_high.at[q, j],
            down_send.at[q, j],
            down_recv.at[q, j],
            device_id={"local": below},
            device_id_type=MESH,
        )

    def add_in(q, j, landing):
        part[q, j] = (
            part[q, j].astype(jnp.float32) + landing[q, j].astype(jnp.float32)
        ).astype(jnp.bfloat16)

    def reduce_round(r):
        def one(i, carry):
            q_up = last - i
            q_down = i
            j_up = r
            j_down = last - r

            @pl.when(q_up > me)
            def _():
                @pl.when(me > 0)
                def _():
                    up(q_up, j_up).wait_recv()
                    add_in(q_up, j_up, from_low)

                up(q_up, j_up).start()

            @pl.when(q_down < me)
            def _():
                @pl.when(me < last)
                def _():
                    down(q_down, j_down).wait_recv()
                    add_in(q_down, j_down, from_high)

                down(q_down, j_down).start()

            return carry

        lax.fori_loop(0, last, one, 0)

    def multiply(step, carry):
        slot = visit_order(me, step, local_count)

        @pl.when(step == last)
        def _():
            relay(last)

        for g in leaves:
            for s in range(SPLITS):
                wait_rows(slot, g, s)
        lhs = rows.at[slot]
        main = depth // 256 * 256
        term = jnp.zeros((group * half_rows, 2 * shard), jnp.float32)
        for lower, upper in ((0, main), (main, depth)):
            if upper > lower:
                term += lax.dot_general(
                    lhs[:, :, lower:upper].reshape(group * half_rows, upper - lower),
                    weights[:, lower:upper],
                    (((1,), (1,)), ((), ())),
                    preferred_element_type=jnp.float32,
                )
        term = term.astype(jnp.bfloat16)
        for q in range(local_count):
            for g in range(group):
                part[q, slot, g * run : (g + 1) * run, :] = term[
                    g * half_rows + q * run : g * half_rows + (q + 1) * run
                ]

        @pl.when(at_end)
        def _():
            reduce_round(step)

        return carry

    def arrive_next(step):
        arrive(step)
        if paced and step < last:

            @pl.when(at_end)
            def _():
                start_hops(step + 1)

            if step == 1:

                @pl.when(jnp.logical_not(at_end))
                def _():
                    start_hops(last)

    for step in range(1, max(2, last)):
        arrive_next(step)
    own_w.wait()
    own_x.wait()
    own_v.wait()
    w_copy.wait_recv()

    @pl.when(me < last)
    def _():
        v_line(me, 1, True).start()

    @pl.when(me > 0)
    def _():
        v_line(me, 0, True).start()

    for bit in spread_bits(0, 0):
        v_spread(me, 0, bit, True).start()
    lax.fori_loop(0, 1, multiply, 0)
    for step in range(max(2, last), local_count):
        arrive_next(step)
    start_lines()
    lax.fori_loop(1, local_count, multiply, 0)

    def middle_round(r):
        @pl.when(jnp.logical_not(at_end))
        def _():
            reduce_round(r)

    for step in range(1, local_count):
        pass_values(step - 1)
        take_values(step)
        take_line(step)
        middle_round(step - 1)
        if step > 1:
            pass_on(step - 1)
    middle_round(last)
    pass_values(last)

    def swap(j, g):
        return pltpu.make_async_remote_copy(
            final.at[j, pl.ds(g * run, run)],
            landed.at[g, pl.ds(pl.multiple_of(j * run, 16), run)],
            swap_send.at[j, g],
            swap_recv.at[j, g],
            device_id={"node": toggled(node, masks[g])},
            device_id_type=MESH,
        )

    def finish(step, carry):
        j = visit_order(last - me, step, local_count)
        total[...] = part[me, j].astype(jnp.float32)

        @pl.when(me > 0)
        def _():
            up(me, j).wait_recv()
            total[...] += from_low[me, j].astype(jnp.float32)

        @pl.when(me < last)
        def _():
            down(me, j).wait_recv()
            total[...] += from_high[me, j].astype(jnp.float32)

        value = total[...] + bias_ref[...]
        final[j] = (0.5 * value * (1.0 + lax.erf(value * (0.5**0.5)))).astype(jnp.bfloat16)
        for g in reversed(range(1, group)):
            swap(j, g).start()
        mid_ref[0, pl.ds(pl.multiple_of(j * run, 16), run), :] = final[j, 0:run, :]
        return carry

    lax.fori_loop(0, local_count, finish, 0)
    pass_on(last)

    counts_all = count_ref[...]
    for step in range(1, local_count):
        source = visit_order(me, step, local_count)
        count_copy(source, source).wait_recv()
        counts_all += counts[source]
        count_copy(source, me).wait_send()
    size_ref[...] = counts_all

    def settle(j, carry):
        for g in range(1, group):
            swap(j, g).wait()
        return carry

    lax.fori_loop(0, local_count, settle, 0)
    for g in range(1, group):
        mid_ref[g] = landed[g]

    w_copy.wait_send()
    for step in range(1, local_count):
        for s in range(SPLITS):
            hop(visit_order(me, step, local_count), me, s).wait_send()

    def drain(slot, carry):
        for g in range(group):
            for bit in forward_bits(masks[g]):
                for s in range(SPLITS):
                    forward(slot, g, bit, s, False).wait_send()

        @pl.when((slot <= me) & (me < last))
        def _():
            v_line(slot, 1, False).wait_send()

        @pl.when((slot >= me) & (me > 0))
        def _():
            v_line(slot, 0, False).wait_send()

        for mask in range(node_count):
            if mask and not spread_bits(mask, 0):
                v_wait(slot, mask)
            for bit in spread_bits(mask, 0):
                v_spread(slot, mask, bit, False).wait_send()

        for s in range(split):

            @pl.when((slot <= me) & (me < last))
            def _():
                line(slot, s, 1, False).wait_send()

            @pl.when((slot >= me) & (me > 0))
            def _():
                line(slot, s, 0, False).wait_send()

        @pl.when(slot != me)
        def _():
            for s in range(split):
                for mask in range(node_count):
                    if mask and not spread_bits(mask, s):
                        wait_strip(slot, mask, s)
                    for bit in spread_bits(mask, s):
                        spread(slot, mask, bit, s).wait_send()

        def drain_sums(j, inner):
            @pl.when(slot > me)
            def _():
                up(slot, j).wait_send()

            @pl.when(slot < me)
            def _():
                down(slot, j).wait_send()

            return inner

        lax.fori_loop(0, local_count, drain_sums, 0)
        return carry

    lax.fori_loop(0, local_count, drain, 0)


def project(x_slices, weight, bias_pair, out_weight, counts, values, node_count, local_count):
    _, half_rows, depth = x_slices.shape
    cols = weight.shape[0]
    bits, masks = row_masks(node_count)
    group = len(masks)
    run = half_rows // local_count
    split = SPREAD_PIECES // node_count
    sums = (local_count, local_count, group * run, 2 * cols)
    dma = pltpu.SemaphoreType.DMA
    grid = (local_count, local_count)
    anywhere = pl.BlockSpec(memory_space=pl.ANY)
    vmem = pl.BlockSpec(memory_space=pltpu.VMEM)
    all_bits = len(bits_below(node_count))
    return pl.pallas_call(
        functools.partial(project_kernel, node_count, local_count),
        out_shape=[
            jax.ShapeDtypeStruct((group, half_rows, 2 * cols), jnp.bfloat16),
            jax.ShapeDtypeStruct(
                (group, local_count, 2 * cols, out_weight.shape[1]), jnp.bfloat16
            ),
            jax.ShapeDtypeStruct(counts.shape, jnp.float32),
            jax.ShapeDtypeStruct((node_count * local_count,) + values.shape, jnp.bfloat16),
        ],
        in_specs=[anywhere, anywhere, vmem, anywhere, vmem, anywhere],
        out_specs=[vmem, anywhere, vmem, anywhere],
        scratch_shapes=[
            pltpu.VMEM((local_count, group, half_rows, depth), jnp.bfloat16),
            pltpu.VMEM((2 * cols, depth), jnp.bfloat16),
            pltpu.VMEM(sums, jnp.bfloat16),
            pltpu.VMEM(sums, jnp.bfloat16),
            pltpu.VMEM(sums, jnp.bfloat16),
            pltpu.VMEM(sums[2:], jnp.float32),
            pltpu.VMEM(sums[1:], jnp.bfloat16),
            pltpu.VMEM((group, half_rows, 2 * cols), jnp.bfloat16),
            pltpu.VMEM((local_count,) + counts.shape, jnp.float32),
            dma((2,)),
            dma((3,)),
            dma((local_count, SPLITS)),
            dma((local_count, group, SPLITS)),
            dma((local_count, group, len(bits), SPLITS)),
            dma(grid),
            dma(grid),
            dma(grid),
            dma(grid),
            dma((local_count, group)),
            dma((local_count, group)),
            dma((local_count, 2, split)),
            dma((local_count, node_count, all_bits, split)),
            dma((local_count, node_count, split)),
            dma((local_count,)),
            dma((local_count,)),
            dma((local_count, 2)),
            dma((local_count, node_count, all_bits)),
            dma((local_count, node_count)),
        ],
        compiler_params=pltpu.CompilerParams(
            collective_id=0, has_side_effects=True, vmem_limit_bytes=58 * 2**20
        ),
        cost_estimate=pl.CostEstimate(
            flops=4 * local_count * group * half_rows * depth * cols,
            bytes_accessed=2 * (x_slices.size + weight.size),
            transcendentals=0,
        ),
    )(x_slices, weight, bias_pair, out_weight, counts, values)


def second_kernel(local_count, place_ref, mid_ref, own_ref, weight_ref, bias_ref, out_ref, total):
    group, _, depth = mid_ref.shape
    width = weight_ref.shape[3]
    column = lax.rem(place_ref[0] + pl.program_id(0), local_count)
    main = depth // 256 * 256

    def product(pick):
        sum_rows = jnp.zeros(total.shape, jnp.float32)
        for g in range(group):
            rhs = pick(g)
            for lower, upper in ((0, main), (main, depth)):
                if upper > lower:
                    sum_rows += jnp.dot(
                        mid_ref[g, :, lower:upper],
                        rhs[lower:upper],
                        preferred_element_type=jnp.float32,
                    )
        total[...] = sum_rows

    @pl.when(pl.program_id(0) == 0)
    def _():
        product(
            lambda g: jnp.concatenate(
                [own_ref[place_ref[1 + g]], own_ref[place_ref[1 + g] + COLUMN_BIT]], 0
            )
        )

    @pl.when(pl.program_id(0) > 0)
    def _():
        product(lambda g: weight_ref[g, 0])

    for z in range(local_count):

        @pl.when(column == z)
        def _():
            value = total[...] + bias_ref[:, z * width : (z + 1) * width]
            out_ref[...] = value.astype(jnp.bfloat16).reshape(out_ref.shape)


def second_product(places, mid, own_weight, weight, bias_row):
    group, local_count, pair_cols, width = weight.shape
    cols = pair_cols // 2
    node_count = 2 * group
    half_rows = mid.shape[1]
    joined = width % LANES == 0

    def column(z, place):
        return lax.rem(place[0] + z, local_count)

    def fetched(z, place):
        return lax.rem(place[0] + jnp.maximum(z, 1), local_count)

    if joined:
        out_shape = (half_rows, local_count * width)
        out_block = pl.BlockSpec((half_rows, width), lambda z, place: (0, column(z, place)))
    else:
        out_shape = (local_count, half_rows, width)
        out_block = pl.BlockSpec((1, half_rows, width), lambda z, place: (column(z, place), 0, 0))
    product = pl.pallas_call(
        functools.partial(second_kernel, local_count),
        grid_spec=pltpu.PrefetchScalarGridSpec(
            num_scalar_prefetch=1,
            grid=(local_count,),
            in_specs=[
                pl.BlockSpec(mid.shape, lambda z, place: (0, 0, 0)),
                pl.BlockSpec((node_count, cols, width), lambda z, place: (0, 0, 0)),
                pl.BlockSpec(
                    (group, 1, pair_cols, width), lambda z, place: (0, fetched(z, place), 0, 0)
                ),
                pl.BlockSpec((1, local_count * width + 8 * LANES), lambda z, place: (0, 0)),
            ],
            out_specs=out_block,
            scratch_shapes=[pltpu.VMEM((half_rows, width), jnp.float32)],
        ),
        out_shape=jax.ShapeDtypeStruct(out_shape, jnp.bfloat16),
        compiler_params=pltpu.CompilerParams(vmem_limit_bytes=48 * 2**20),
        cost_estimate=pl.CostEstimate(
            flops=2 * half_rows * weight.size, bytes_accessed=2 * weight.size, transcendentals=0
        ),
    )(
        places,
        mid,
        own_weight.reshape(node_count, cols, width),
        weight,
        jnp.pad(bias_row, (0, 8 * LANES))[None, :],
    )
    if joined:
        return product
    return jnp.transpose(product, (1, 0, 2)).reshape(half_rows, local_count * width)


def row_grads(hidden_f, grad_rows, weight, gain, keep):
    inv_rms = lax.rsqrt(jnp.mean(hidden_f * hidden_f, -1, keepdims=True) + 1e-06)
    unit = hidden_f * inv_rms
    normed = (unit * gain * keep).astype(jnp.bfloat16)
    grad_normed = lax.dot_general(
        grad_rows, weight, (((1,), (1,)), ((), ())), preferred_element_type=jnp.float32
    )
    part = jnp.sum(grad_normed * unit * keep, 0, keepdims=True)
    scaled = grad_normed * gain
    moment = jnp.mean(scaled * hidden_f, -1, keepdims=True)
    grad_hidden = inv_rms * scaled - hidden_f * (inv_rms * inv_rms * inv_rms * moment)
    return normed, part, grad_hidden.astype(jnp.bfloat16)


def add_part(part_ref, part):
    @pl.when(pl.program_id(0) == 0)
    def _():
        part_ref[...] = part

    @pl.when(pl.program_id(0) > 0)
    def _():
        part_ref[...] += part


def text_kernel(
    image_ref, text_ref, grad_ref, weight_ref, gain_ref, out_ref, normed_ref, part_ref
):
    count, rows, width = text_ref.shape
    first = count * pl.program_id(0)
    row = lax.broadcasted_iota(jnp.int32, (count * rows, 1), 0)
    keep = jnp.zeros(row.shape, jnp.float32)
    for i in range(count):
        held = jnp.where(image_ref[first + i] > 0, 0.0, 1.0)
        keep = jnp.where((row >= i * rows) & (row < (i + 1) * rows), held, keep)
    normed, part, grad_hidden = row_grads(
        text_ref[...].reshape(count * rows, width).astype(jnp.float32),
        grad_ref[...].reshape(count * rows, grad_ref.shape[2]),
        weight_ref[...],
        gain_ref[...],
        keep,
    )
    normed_ref[...] = normed.reshape(normed_ref.shape)
    out_ref[...] = grad_hidden.reshape(out_ref.shape)
    add_part(part_ref, part)


def image_kernel(
    block_ref,
    filled_ref,
    arrived_ref,
    grad_ref,
    weight_ref,
    gain_ref,
    text_out_ref,
    out_ref,
    normed_ref,
    part_ref,
):
    filled = filled_ref[pl.program_id(0)] > 0
    normed_ref[0], part, grad_hidden = row_grads(
        arrived_ref[0].astype(jnp.float32),
        grad_ref[0],
        weight_ref[...],
        gain_ref[...],
        jnp.where(filled, 1.0, 0.0),
    )
    add_part(part_ref, part)

    @pl.when(filled)
    def _():
        out_ref[0] = grad_hidden

    @pl.when(jnp.logical_not(filled))
    def _():
        out_ref[0] = text_out_ref[0]


def cost(steps, rows, width, values):
    return pl.CostEstimate(
        flops=2 * steps * rows * width * values,
        bytes_accessed=6 * steps * rows * width + 2 * width * values,
        transcendentals=0,
    )


def text_grads(is_image, text, value_grad, v_full, gain):
    blocks, rows, width = text.shape
    values = value_grad.shape[2]
    count = max(c for c in (1, 2) if blocks % c == 0)
    row_block = pl.BlockSpec((count, rows, width), lambda b, image: (b, 0, 0))
    one_row = pl.BlockSpec((1, width), lambda b, image: (0, 0))
    return pl.pallas_call(
        text_kernel,
        grid_spec=pltpu.PrefetchScalarGridSpec(
            num_scalar_prefetch=1,
            grid=(blocks // count,),
            in_specs=[
                row_block,
                pl.BlockSpec((count, rows, values), lambda b, image: (b, 0, 0)),
                pl.BlockSpec((width, values), lambda b, image: (0, 0)),
                one_row,
            ],
            out_specs=[row_block, row_block, one_row],
        ),
        out_shape=[
            jax.ShapeDtypeStruct((blocks, rows, width), jnp.bfloat16),
            jax.ShapeDtypeStruct((blocks, rows, width), jnp.bfloat16),
            jax.ShapeDtypeStruct((1, width), jnp.float32),
        ],
        cost_estimate=cost(blocks, rows, width, values),
    )(is_image, text, value_grad, v_full, gain)


def image_grads(block_of_piece, filled, arrived, value_grad, v_full, gain, text_out):
    pieces, rows, width = arrived.shape
    values = value_grad.shape[2]
    piece_rows = pl.BlockSpec((1, rows, width), lambda p, block, full: (p, 0, 0))
    block_rows = pl.BlockSpec((1, rows, width), lambda p, block, full: (block[p], 0, 0))
    one_row = pl.BlockSpec((1, width), lambda p, block, full: (0, 0))
    return pl.pallas_call(
        image_kernel,
        grid_spec=pltpu.PrefetchScalarGridSpec(
            num_scalar_prefetch=2,
            grid=(pieces,),
            in_specs=[
                piece_rows,
                pl.BlockSpec((1, rows, values), lambda p, block, full: (p, 0, 0)),
                pl.BlockSpec((width, values), lambda p, block, full: (0, 0)),
                one_row,
                block_rows,
            ],
            out_specs=[block_rows, piece_rows, one_row],
        ),
        out_shape=[
            jax.ShapeDtypeStruct(text_out.shape, jnp.bfloat16),
            jax.ShapeDtypeStruct((pieces, rows, width), jnp.bfloat16),
            jax.ShapeDtypeStruct((1, width), jnp.float32),
        ],
        input_output_aliases={6: 0},
        cost_estimate=cost(pieces, rows, width, values),
    )(block_of_piece, filled, arrived, value_grad, v_full, gain, text_out)


def gather_kernel(
    node_count,
    local_count,
    normed_ref,
    grad_ref,
    text_ref,
    vector_ref,
    out_ref,
    vector_out_ref,
    tot,
    pair_out,
    pair_in,
    chip_out,
    chip_in,
    line_out,
    line_in,
    vec_pair,
    vec_sum,
    vec_chip,
    vec_line,
    pair_sems,
    chip_send,
    chip_recv,
    line_send,
    line_recv,
    vec_pair_sems,
    vec_chip_send,
    vec_chip_recv,
    vec_line_send,
    vec_line_recv,
):
    node = lax.axis_index("node")
    me = lax.axis_index("local")
    chips = node_count // 2
    core = lax.rem(node, 2)
    chip = lax.div(node, 2)
    own_rows = tot.shape[1]

    barrier = pltpu.get_barrier_semaphore()
    for r in [1] + [2 * c for c in range(1, chips)]:
        pl.semaphore_signal(
            barrier, 1, device_id={"node": toggled(node, r)}, device_id_type=MESH
        )
    for step in range(1, local_count):
        pl.semaphore_signal(
            barrier, 1, device_id={"local": toggled(me, step)}, device_id_type=MESH
        )
    pl.semaphore_wait(barrier, chips + local_count - 1)

    def remote(src, dst, send, recv, axis, target):
        return pltpu.make_async_remote_copy(
            src, dst, send, recv, device_id={axis: target}, device_id_type=MESH
        )

    vec_to_pair = remote(
        vector_ref, vec_pair, vec_pair_sems.at[0], vec_pair_sems.at[1], "node", flip(node, 1)
    )
    vec_to_pair.start()

    product = lax.dot_general(
        normed_ref[...], grad_ref[...], (((0,), (0,)), ((), ())), preferred_element_type=jnp.float32
    )
    if own_rows % 8 == 0:
        tot[...] = product.reshape(tot.shape) + text_ref[...].astype(jnp.float32)
    else:
        for i in range(node_count * local_count):
            tot[i] = product[i * own_rows : (i + 1) * own_rows] + text_ref[i].astype(jnp.float32)

    def to_pair(k, q):
        return remote(
            pair_out.at[q, k],
            pair_in.at[q, k],
            pair_sems.at[0, q, k],
            pair_sems.at[1, q, k],
            "node",
            flip(node, 1),
        )

    def to_chip(q, r):
        return remote(
            chip_out.at[q, r],
            chip_in.at[q, r],
            chip_send.at[q, r],
            chip_recv.at[q, r],
            "node",
            toggled(node, 2 * r),
        )

    def to_line(step):
        return remote(
            line_out.at[step],
            line_in.at[step],
            line_send.at[step],
            line_recv.at[step],
            "local",
            toggled(me, step),
        )

    def vec_to_chip(r):
        return remote(
            vec_sum.at[0],
            vec_chip.at[chip],
            vec_chip_send.at[r],
            vec_chip_recv.at[r],
            "node",
            toggled(node, 2 * r),
        )

    def vec_to_line(step):
        return remote(
            vec_sum.at[1],
            vec_line.at[me],
            vec_line_send.at[step],
            vec_line_recv.at[step],
            "local",
            toggled(me, step),
        )

    def place(k, side, q):
        return (2 * k + side) * local_count + q

    steps = list(range(1, local_count)) + [0]
    for step in steps:
        q = toggled(me, step)
        for r in list(range(1, chips)) + [0]:
            k = toggled(chip, r)
            pair_out[q, k] = tot[place(k, 1 - core, q)].astype(jnp.bfloat16)
            to_pair(k, q).start()
    vec_to_pair.wait()
    vec_sum[0] = vector_ref[...] + vec_pair[...]
    vec_chip[chip] = vec_sum[0]
    for r in range(1, chips):
        vec_to_chip(r).start()
    for step in steps:
        q = toggled(me, step)
        for r in reversed(range(1, chips)):
            k = toggled(chip, r)
            to_pair(k, q).wait()
            chip_out[q, r] = (
                tot[place(k, core, q)] + pair_in[q, k].astype(jnp.float32)
            ).astype(jnp.bfloat16)
            to_chip(q, r).start()
        to_pair(chip, q).wait()
    for r in range(1, chips):
        source = toggled(chip, r)
        remote(
            vec_sum.at[0],
            vec_chip.at[source],
            vec_chip_send.at[r],
            vec_chip_recv.at[r],
            "node",
            toggled(node, 2 * r),
        ).wait()
    vec_total = vec_chip[0]
    for c in range(1, chips):
        vec_total += vec_chip[c]
    vec_sum[1] = vec_total
    vec_line[me] = vec_total
    for step in range(1, local_count):
        vec_to_line(step).start()
    for step in steps:
        q = toggled(me, step)
        value = tot[place(chip, core, q)] + pair_in[q, chip].astype(jnp.float32)
        for r in range(1, chips):
            to_chip(q, r).wait()
            value += chip_in[q, r].astype(jnp.float32)
        if step:
            line_out[step] = value.astype(jnp.bfloat16)
            to_line(step).start()
    for step in range(1, local_count):
        source = toggled(me, step)
        remote(
            vec_sum.at[1],
            vec_line.at[source],
            vec_line_send.at[step],
            vec_line_recv.at[step],
            "local",
            source,
        ).wait()
    vec_total = vec_line[0]
    for z in range(1, local_count):
        vec_total += vec_line[z]
    vector_out_ref[...] = vec_total / node_count
    for step in range(1, local_count):
        to_line(step).wait()
        value += line_in[step].astype(jnp.float32)
    out_ref[...] = value / node_count


def gather_grads(normed, grads, text_sum, vector, node_count, local_count):
    rows, values = text_sum.shape
    own_rows = rows // (node_count * local_count)
    chips = node_count // 2
    dma = pltpu.SemaphoreType.DMA
    tile = (own_rows, values)
    vec = vector.shape
    return pl.pallas_call(
        functools.partial(gather_kernel, node_count, local_count),
        out_shape=[
            jax.ShapeDtypeStruct(tile, jnp.float32),
            jax.ShapeDtypeStruct(vec, jnp.float32),
        ],
        in_specs=[pl.BlockSpec(memory_space=pltpu.VMEM)] * 4,
        out_specs=[pl.BlockSpec(memory_space=pltpu.VMEM)] * 2,
        scratch_shapes=[
            pltpu.VMEM((node_count * local_count,) + tile, jnp.float32),
            pltpu.VMEM((local_count, chips) + tile, jnp.bfloat16),
            pltpu.VMEM((local_count, chips) + tile, jnp.bfloat16),
            pltpu.VMEM((local_count, chips) + tile, jnp.bfloat16),
            pltpu.VMEM((local_count, chips) + tile, jnp.bfloat16),
            pltpu.VMEM((local_count,) + tile, jnp.bfloat16),
            pltpu.VMEM((local_count,) + tile, jnp.bfloat16),
            pltpu.VMEM(vec, jnp.float32),
            pltpu.VMEM((2,) + vec, jnp.float32),
            pltpu.VMEM((chips,) + vec, jnp.float32),
            pltpu.VMEM((local_count,) + vec, jnp.float32),
            dma((2, local_count, chips)),
            dma((local_count, chips)),
            dma((local_count, chips)),
            dma((local_count,)),
            dma((local_count,)),
            dma((2,)),
            dma((chips,)),
            dma((chips,)),
            dma((local_count,)),
            dma((local_count,)),
        ],
        compiler_params=pltpu.CompilerParams(
            collective_id=1, has_side_effects=True, vmem_limit_bytes=48 * 2**20
        ),
        cost_estimate=pl.CostEstimate(
            flops=2 * normed.size * values, bytes_accessed=2 * text_sum.size, transcendentals=0
        ),
    )(normed, grads, text_sum.reshape((node_count * local_count,) + tile), vector)


def weight_grad(normed, grad_rows):
    return lax.dot_general(
        normed, grad_rows, (((0,), (0,)), ((), ())), preferred_element_type=jnp.float32
    )


def per_device(
    vit_tiles,
    tile_counts,
    block_of_piece,
    segment_ids,
    text_rows,
    cotangent,
    proj_weight,
    proj_bias,
    out_weight,
    out_bias,
    ln_gain,
    ln_bias,
    norm_gain,
    v_weight,
):
    local_count = lax.axis_size("local")
    node_count = lax.axis_size("node")
    node = lax.axis_index("node")
    blocks = text_rows.shape[1]
    share_rows = text_rows.shape[2]
    model_width = text_rows.shape[3]
    out_cols = out_weight.shape[1]
    shard_cols = proj_weight.shape[1]
    x_slices = slices(vit_tiles[0, 0], ln_gain, ln_bias, local_count)
    side = lax.rem(lax.div(node, COLUMN_BIT), 2)
    low_shard = node - COLUMN_BIT * side
    bias_pair = jnp.concatenate(
        [
            lax.dynamic_slice_in_dim(proj_bias, shard * shard_cols, shard_cols, 0)
            for shard in (low_shard, low_shard + COLUMN_BIT)
        ]
    )[None, :]
    _, masks = row_masks(node_count)
    places = jnp.stack(
        [lax.axis_index("local")]
        + [toggled(low_shard, m) for m in masks]
    )
    doc_ids = segment_ids[0].reshape(-1)
    doc_hits = (doc_ids[:, None] == lax.iota(jnp.int32, DOCS)[None, :]).astype(jnp.float32)
    doc_counts = jnp.pad(jnp.sum(doc_hits, 0)[None, :], ((0, 7), (0, LANES - DOCS)))
    mid, out_spread, doc_sizes, v_full = project(
        x_slices,
        jnp.transpose(proj_weight),
        bias_pair,
        out_weight,
        doc_counts,
        v_weight,
        node_count,
        local_count,
    )
    doc_sizes = doc_sizes[0, :DOCS]
    v_full = v_full.reshape(model_width, -1)
    doc_weight = blocks * share_rows * local_count / (DOCS * doc_sizes)
    token_weight = jnp.dot(doc_hits, doc_weight, precision=lax.Precision.HIGHEST)
    value_grad = (
        cotangent[0].reshape(-1, cotangent.shape[3]).astype(jnp.float32) * token_weight[:, None]
    ).astype(jnp.bfloat16)
    bias_part = jnp.sum(value_grad.astype(jnp.float32), 0)
    piece_total = local_count // 2
    piece_ids = lax.iota(jnp.int32, piece_total)
    filled = piece_ids % SLOTS < jnp.repeat(tile_counts[0], SLOTS)
    chosen = (block_of_piece[0][None, :] == lax.iota(jnp.int32, blocks)[:, None]) & filled[None, :]
    is_image = jnp.any(chosen, 1).astype(jnp.int32)
    gain_row = norm_gain[None, :]
    value_blocks = value_grad.reshape(blocks, share_rows, -1)
    value_pieces = value_blocks[block_of_piece[0]]
    text_out, text_normed, text_part = text_grads(
        is_image, text_rows[0], value_blocks, v_full, gain_row
    )
    text_sum = weight_grad(text_normed.reshape(-1, model_width), value_grad).astype(jnp.bfloat16)
    flat_pieces = value_pieces.reshape(-1, value_pieces.shape[2])
    arrived = second_product(places, mid, out_weight, out_spread, out_bias)
    arrived = arrived.reshape(piece_total, share_rows, model_width)
    grad_hidden, image_normed, image_part = image_grads(
        block_of_piece[0], filled.astype(jnp.int32), arrived, value_pieces, v_full, gain_row, text_out
    )
    gain_part = text_part + image_part
    vector = jnp.concatenate([bias_part, gain_part[0]])
    length = vector.shape[0]
    vector = jnp.pad(vector, (0, -length % (8 * LANES))).reshape(8, -1)
    grad_weight, vector = gather_grads(
        image_normed.reshape(-1, model_width),
        flat_pieces,
        text_sum,
        vector,
        node_count,
        local_count,
    )
    vector = vector.reshape(-1)
    values = bias_part.shape[0]
    return (grad_hidden[None], grad_weight, vector[:values], vector[values:length])


def solution(mesh):
    in_specs = (
        P("node", "local", None, None),
        P("node", None),
        P("node", None),
        P("node", None, "local"),
        P("node", None, "local", None),
        P("node", None, "local", None),
        P("local", "node"),
        P(),
        P(None, "local"),
        P(),
        P(),
        P(),
        P(),
        P(("node", "local"), None),
    )
    out_specs = (P("node", None, "local", None), P(("node", "local"), None), P(), P())
    return jax.shard_map(
        per_device, mesh=mesh, in_specs=in_specs, out_specs=out_specs, check_vma=False
    )
```

```python
import functools

import jax
import jax.numpy as jnp
from jax import lax
from jax.experimental import pallas as pl
from jax.experimental.pallas import tpu as pltpu
from jax.sharding import PartitionSpec as P

SLOTS = 2
DOCS = 16
LANES = 128
COLUMN_BIT = 2
SPLITS = 2
SPREAD_PIECES = 32
MESH = pl.DeviceIdType.MESH


def flip(index, bit):
    return index + bit - 2 * bit * lax.rem(lax.div(index, bit), 2)


def bits_below(count):
    return [1 << b for b in range(count.bit_length() - 1)]


def row_masks(node_count):
    bits = [b for b in bits_below(node_count) if b != COLUMN_BIT]
    masks = [m for m in range(node_count) if not m & COLUMN_BIT]
    return bits, masks


def toggled(index, mask):
    for b in range(mask.bit_length()):
        if mask >> b & 1:
            index = flip(index, 1 << b)
    return index


def visit_order(index, step, count):
    if count == 4:
        middle = lax.rem(lax.div(index + 1, 2), 2)
        step = step + middle * lax.div(step, 2) * (5 - 2 * step)
    total = 0
    for bit in bits_below(count):
        total = total + bit * lax.rem(lax.div(index, bit) + lax.div(step, bit), 2)
    return total


def slice_kernel(local_count, x_ref, affine_ref, out_ref):
    values = x_ref[...].astype(jnp.float32)
    average = jnp.mean(values, -1, keepdims=True)
    centred = values - average
    variance = jnp.mean(centred * centred, -1, keepdims=True)
    normed = centred * lax.rsqrt(variance + 1e-05) * affine_ref[0:1] + affine_ref[1:2]
    depth = out_ref.shape[2]
    for k in range(local_count):
        out_ref[k] = normed[:, k * depth : (k + 1) * depth].astype(jnp.bfloat16)


def slices(vit_rows, scale_vec, shift_vec, local_count):
    half_rows, width = vit_rows.shape
    depth = width // local_count
    step_rows = 32
    two_rows = pl.BlockSpec((2, width), lambda i: (0, 0))
    return pl.pallas_call(
        functools.partial(slice_kernel, local_count),
        grid=(half_rows // step_rows,),
        in_specs=[pl.BlockSpec((step_rows, width), lambda i: (i, 0)), two_rows],
        out_specs=pl.BlockSpec((local_count, step_rows, depth), lambda i: (0, i, 0)),
        out_shape=jax.ShapeDtypeStruct((local_count, half_rows, depth), jnp.bfloat16),
        cost_estimate=pl.CostEstimate(
            flops=10 * vit_rows.size, bytes_accessed=4 * vit_rows.size, transcendentals=0
        ),
    )(vit_rows, jnp.stack([scale_vec, shift_vec]))


def project_kernel(
    node_count,
    local_count,
    x_ref,
    w_ref,
    bias_ref,
    out_w_ref,
    count_ref,
    v_ref,
    mid_ref,
    spread_ref,
    size_ref,
    v_out,
    rows,
    weights,
    part,
    from_low,
    from_high,
    total,
    final,
    landed,
    counts,
    w_sems,
    own_sems,
    hop_sem,
    recv_sem,
    fwd_sem,
    up_send,
    up_recv,
    down_send,
    down_recv,
    swap_send,
    swap_recv,
    line_send,
    spread_send,
    spread_recv,
    count_send,
    count_recv,
    v_line_send,
    v_send,
    v_recv,
):
    node = lax.axis_index("node")
    me = lax.axis_index("local")
    last = local_count - 1
    bits, masks = row_masks(node_count)
    all_bits = bits_below(node_count)
    group = len(masks)
    half_rows = x_ref.shape[1]
    depth = x_ref.shape[2]
    shard = w_ref.shape[0]
    piece = half_rows // SPLITS
    run = half_rows // local_count
    side = lax.rem(lax.div(node, COLUMN_BIT), 2)
    split = SPREAD_PIECES // node_count
    above = lax.rem(me + 1, local_count)
    below = lax.rem(me + last, local_count)
    at_end = (me == 0) | (me == last)

    barrier = pltpu.get_barrier_semaphore()
    for step in range(1, local_count):
        pl.semaphore_signal(
            barrier, 1, device_id={"local": visit_order(me, step, local_count)}, device_id_type=MESH
        )
    for mask in [COLUMN_BIT] + masks[1:]:
        pl.semaphore_signal(
            barrier, 1, device_id={"node": toggled(node, mask)}, device_id_type=MESH
        )
    pl.semaphore_wait(barrier, local_count - 1 + group)

    shard_rows = pl.ds(pl.multiple_of(side * shard, 8), shard)
    w_copy = pltpu.make_async_remote_copy(
        w_ref,
        weights.at[shard_rows],
        w_sems.at[0],
        w_sems.at[1],
        device_id={"node": flip(node, COLUMN_BIT)},
        device_id_type=MESH,
    )
    w_copy.start()

    def count_copy(target, source):
        return pltpu.make_async_remote_copy(
            count_ref,
            counts.at[source],
            count_send.at[target],
            count_recv.at[source],
            device_id={"local": target},
            device_id_type=MESH,
        )

    for step in range(1, local_count):
        count_copy(visit_order(me, step, local_count), me).start()

    def part_rows(s):
        return pl.ds(pl.multiple_of(s * piece, 16), piece)

    def hop(target, source, s):
        return pltpu.make_async_remote_copy(
            x_ref.at[target, part_rows(s)],
            rows.at[source, 0, part_rows(s)],
            hop_sem.at[target, s],
            recv_sem.at[source, 0, s],
            device_id={"local": target},
            device_id_type=MESH,
        )

    def forward_bits(mask):
        return [b for b in reversed(bits) if mask == 0 or b < (mask & -mask)]

    def forward(slot, g, bit, s, origin):
        src = x_ref.at[slot, part_rows(s)] if origin else rows.at[slot, g, part_rows(s)]
        return pltpu.make_async_remote_copy(
            src,
            rows.at[slot, masks.index(masks[g] | bit), part_rows(s)],
            fwd_sem.at[slot, g, bits.index(bit), s],
            recv_sem.at[slot, masks.index(masks[g] | bit), s],
            device_id={"node": flip(node, bit)},
            device_id_type=MESH,
        )

    def wait_rows(slot, g, s):
        pltpu.make_async_remote_copy(
            rows.at[slot, g, part_rows(s)],
            rows.at[slot, g, part_rows(s)],
            hop_sem.at[slot, s],
            recv_sem.at[slot, g, s],
            device_id={"node": flip(node, 1)},
            device_id_type=MESH,
        ).wait_recv()

    strip = shard // split

    def strip_rows(s, base=0):
        return pl.ds(pl.multiple_of(base + s * strip, 8), strip)

    def held(mask, slot, s, source_mask=None):
        other = (mask if source_mask is None else source_mask) // COLUMN_BIT % 2
        return spread_ref.at[
            masks.index(mask & ~COLUMN_BIT),
            slot,
            strip_rows(s, shard * (other + side * (1 - 2 * other))),
        ]

    def line(source, s, upward, origin):
        src = (
            out_w_ref.at[strip_rows(s, node * shard)]
            if origin
            else held(0, source, s)
        )
        return pltpu.make_async_remote_copy(
            src,
            held(0, source, s),
            line_send.at[source, upward, s],
            spread_recv.at[source, 0, s],
            device_id={"local": above if upward else below},
            device_id_type=MESH,
        )

    def start_lines():
        @pl.when(me < last)
        def _():
            for s in range(split):
                line(me, s, 1, True).start()

        @pl.when(me > 0)
        def _():
            for s in range(split):
                line(me, s, 0, True).start()

    def spread_order(s):
        wide = [b for b in all_bits if b > 1]
        return wide[s % len(wide) :] + wide[: s % len(wide)] + [1]

    def spread_bits(mask, s):
        order = spread_order(s)
        held = [i for i, b in enumerate(order) if mask & b]
        return order[held[-1] + 1 :] if held else order

    def spread(slot, mask, bit, s):
        return pltpu.make_async_remote_copy(
            held(mask, slot, s),
            held(mask | bit, slot, s, mask),
            spread_send.at[slot, mask, bit.bit_length() - 1, s],
            spread_recv.at[slot, mask | bit, s],
            device_id={"node": flip(node, bit)},
            device_id_type=MESH,
        )

    def wait_strip(slot, mask, s):
        pltpu.make_async_remote_copy(
            held(mask, slot, s),
            held(mask, slot, s),
            line_send.at[slot, 0, s],
            spread_recv.at[slot, mask, s],
            device_id={"node": flip(node, 1)},
            device_id_type=MESH,
        ).wait_recv()

    def take_line(step):
        slot = visit_order(me, step, local_count)
        for s in range(split):
            wait_strip(slot, 0, s)

            @pl.when((slot < me) & (me < last))
            def _():
                line(slot, s, 1, False).start()

            @pl.when((slot > me) & (me > 0))
            def _():
                line(slot, s, 0, False).start()

            for bit in spread_bits(0, s):
                spread(slot, 0, bit, s).start()

    def pass_on(step):
        slot = visit_order(me, step, local_count)
        for size in range(1, len(all_bits)):
            for s in range(split):
                for mask in range(1, node_count):
                    if bin(mask).count("1") == size and spread_bits(mask, s):
                        wait_strip(slot, mask, s)
                        for bit in spread_bits(mask, s):
                            spread(slot, mask, bit, s).start()

    def v_place(mask, slot):
        return v_out.at[toggled(node, mask) * local_count + slot]

    def v_line(source, upward, origin):
        return pltpu.make_async_remote_copy(
            v_ref if origin else v_place(0, source),
            v_place(0, source),
            v_line_send.at[source, upward],
            v_recv.at[source, 0],
            device_id={"local": above if upward else below},
            device_id_type=MESH,
        )

    def v_spread(slot, mask, bit, origin):
        return pltpu.make_async_remote_copy(
            v_ref if origin else v_place(mask, slot),
            v_place(mask, slot),
            v_send.at[slot, mask, bit.bit_length() - 1],
            v_recv.at[slot, mask | bit],
            device_id={"node": flip(node, bit)},
            device_id_type=MESH,
        )

    def v_wait(slot, mask):
        pltpu.make_async_remote_copy(
            v_place(mask, slot),
            v_place(mask, slot),
            v_line_send.at[slot, 0],
            v_recv.at[slot, mask],
            device_id={"node": flip(node, 1)},
            device_id_type=MESH,
        ).wait_recv()

    def take_values(step):
        slot = visit_order(me, step, local_count)
        v_wait(slot, 0)

        @pl.when((slot < me) & (me < last))
        def _():
            v_line(slot, 1, False).start()

        @pl.when((slot > me) & (me > 0))
        def _():
            v_line(slot, 0, False).start()

        for bit in spread_bits(0, 0):
            v_spread(slot, 0, bit, False).start()

    def pass_values(step):
        slot = visit_order(me, step, local_count)
        for size in range(1, len(all_bits)):
            for mask in range(1, node_count):
                if bin(mask).count("1") == size and spread_bits(mask, 0):
                    v_wait(slot, mask)
                    for bit in spread_bits(mask, 0):
                        v_spread(slot, mask, bit, False).start()

    own_v = pltpu.make_async_copy(v_ref, v_place(0, me), own_sems.at[2])
    own_v.start()

    for bit in forward_bits(0):
        for s in range(SPLITS):
            forward(me, 0, bit, s, True).start()
    def start_hops(step):
        for s in range(SPLITS):
            hop(visit_order(me, step, local_count), me, s).start()

    paced = local_count == 4
    if paced:
        start_hops(1)

        @pl.when(jnp.logical_not(at_end))
        def _():
            start_hops(2)
    else:
        for step in range(1, local_count):
            start_hops(step)
    own_w = pltpu.make_async_copy(w_ref, weights.at[shard_rows], own_sems.at[0])
    own_w.start()
    own_x = pltpu.make_async_copy(x_ref.at[me], rows.at[me, 0], own_sems.at[1])
    own_x.start()

    relays = [g for g in range(1, group) if forward_bits(masks[g])]
    leaves = [g for g in range(1, group) if not forward_bits(masks[g])]

    def relay(step):
        slot = visit_order(me, step, local_count)
        for g in sorted(relays, key=lambda g: -(masks[g] & -masks[g])):
            for s in range(SPLITS):
                wait_rows(slot, g, s)
                for bit in forward_bits(masks[g]):
                    forward(slot, g, bit, s, False).start()

    def arrive(step):
        slot = visit_order(me, step, local_count)
        for s in range(SPLITS):
            wait_rows(slot, 0, s)
            for bit in forward_bits(0):
                forward(slot, 0, bit, s, False).start()
        relay(step - 1)

    def up(q, j):
        return pltpu.make_async_remote_copy(
            part.at[q, j],
            from_low.at[q, j],
            up_send.at[q, j],
            up_recv.at[q, j],
            device_id={"local": above},
            device_id_type=MESH,
        )

    def down(q, j):
        return pltpu.make_async_remote_copy(
            part.at[q, j],
            from_high.at[q, j],
            down_send.at[q, j],
            down_recv.at[q, j],
            device_id={"local": below},
            device_id_type=MESH,
        )

    def add_in(q, j, landing):
        part[q, j] = (
            part[q, j].astype(jnp.float32) + landing[q, j].astype(jnp.float32)
        ).astype(jnp.bfloat16)

    def reduce_round(r):
        def one(i, carry):
            q_up = last - i
            q_down = i
            j_up = r
            j_down = last - r

            @pl.when(q_up > me)
            def _():
                @pl.when(me > 0)
                def _():
                    up(q_up, j_up).wait_recv()
                    add_in(q_up, j_up, from_low)

                up(q_up, j_up).start()

            @pl.when(q_down < me)
            def _():
                @pl.when(me < last)
                def _():
                    down(q_down, j_down).wait_recv()
                    add_in(q_down, j_down, from_high)

                down(q_down, j_down).start()

            return carry

        lax.fori_loop(0, last, one, 0)

    def multiply(step, carry):
        slot = visit_order(me, step, local_count)

        @pl.when(step == last)
        def _():
            relay(last)

        for g in leaves:
            for s in range(SPLITS):
                wait_rows(slot, g, s)
        lhs = rows.at[slot]
        main = depth // 256 * 256
        term = jnp.zeros((group * half_rows, 2 * shard), jnp.float32)
        for lower, upper in ((0, main), (main, depth)):
            if upper > lower:
                term += lax.dot_general(
                    lhs[:, :, lower:upper].reshape(group * half_rows, upper - lower),
                    weights[:, lower:upper],
                    (((1,), (1,)), ((), ())),
                    preferred_element_type=jnp.float32,
                )
        term = term.astype(jnp.bfloat16)
        for q in range(local_count):
            for g in range(group):
                part[q, slot, g * run : (g + 1) * run, :] = term[
                    g * half_rows + q * run : g * half_rows + (q + 1) * run
                ]

        @pl.when(at_end)
        def _():
            reduce_round(step)

        return carry

    def arrive_next(step):
        arrive(step)
        if paced and step < last:

            @pl.when(at_end)
            def _():
                start_hops(step + 1)

            if step == 1:

                @pl.when(jnp.logical_not(at_end))
                def _():
                    start_hops(last)

    for step in range(1, max(2, last)):
        arrive_next(step)
    own_w.wait()
    own_x.wait()
    own_v.wait()
    w_copy.wait_recv()

    @pl.when(me < last)
    def _():
        v_line(me, 1, True).start()

    @pl.when(me > 0)
    def _():
        v_line(me, 0, True).start()

    for bit in spread_bits(0, 0):
        v_spread(me, 0, bit, True).start()
    lax.fori_loop(0, 1, multiply, 0)
    for step in range(max(2, last), local_count):
        arrive_next(step)
    start_lines()
    lax.fori_loop(1, local_count, multiply, 0)

    def middle_round(r):
        @pl.when(jnp.logical_not(at_end))
        def _():
            reduce_round(r)

    for step in range(1, local_count):
        pass_values(step - 1)
        take_values(step)
        take_line(step)
        middle_round(step - 1)
        if step > 1:
            pass_on(step - 1)
    middle_round(last)
    pass_values(last)

    def swap(j, g):
        return pltpu.make_async_remote_copy(
            final.at[j, pl.ds(g * run, run)],
            landed.at[g, pl.ds(pl.multiple_of(j * run, 16), run)],
            swap_send.at[j, g],
            swap_recv.at[j, g],
            device_id={"node": toggled(node, masks[g])},
            device_id_type=MESH,
        )

    def finish(step, carry):
        j = visit_order(last - me, step, local_count)
        total[...] = part[me, j].astype(jnp.float32)

        @pl.when(me > 0)
        def _():
            up(me, j).wait_recv()
            total[...] += from_low[me, j].astype(jnp.float32)

        @pl.when(me < last)
        def _():
            down(me, j).wait_recv()
            total[...] += from_high[me, j].astype(jnp.float32)

        value = total[...] + bias_ref[...]
        final[j] = (0.5 * value * (1.0 + lax.erf(value * (0.5**0.5)))).astype(jnp.bfloat16)
        for g in reversed(range(1, group)):
            swap(j, g).start()
        mid_ref[0, pl.ds(pl.multiple_of(j * run, 16), run), :] = final[j, 0:run, :]
        return carry

    lax.fori_loop(0, local_count, finish, 0)
    pass_on(last)

    counts_all = count_ref[...]
    for step in range(1, local_count):
        source = visit_order(me, step, local_count)
        count_copy(source, source).wait_recv()
        counts_all += counts[source]
        count_copy(source, me).wait_send()
    size_ref[...] = counts_all

    def settle(j, carry):
        for g in range(1, group):
            swap(j, g).wait()
        return carry

    lax.fori_loop(0, local_count, settle, 0)
    for g in range(1, group):
        mid_ref[g] = landed[g]

    w_copy.wait_send()
    for step in range(1, local_count):
        for s in range(SPLITS):
            hop(visit_order(me, step, local_count), me, s).wait_send()

    def drain(slot, carry):
        for g in range(group):
            for bit in forward_bits(masks[g]):
                for s in range(SPLITS):
                    forward(slot, g, bit, s, False).wait_send()

        @pl.when((slot <= me) & (me < last))
        def _():
            v_line(slot, 1, False).wait_send()

        @pl.when((slot >= me) & (me > 0))
        def _():
            v_line(slot, 0, False).wait_send()

        for mask in range(node_count):
            if mask and not spread_bits(mask, 0):
                v_wait(slot, mask)
            for bit in spread_bits(mask, 0):
                v_spread(slot, mask, bit, False).wait_send()

        for s in range(split):

            @pl.when((slot <= me) & (me < last))
            def _():
                line(slot, s, 1, False).wait_send()

            @pl.when((slot >= me) & (me > 0))
            def _():
                line(slot, s, 0, False).wait_send()

        @pl.when(slot != me)
        def _():
            for s in range(split):
                for mask in range(node_count):
                    if mask and not spread_bits(mask, s):
                        wait_strip(slot, mask, s)
                    for bit in spread_bits(mask, s):
                        spread(slot, mask, bit, s).wait_send()

        def drain_sums(j, inner):
            @pl.when(slot > me)
            def _():
                up(slot, j).wait_send()

            @pl.when(slot < me)
            def _():
                down(slot, j).wait_send()

            return inner

        lax.fori_loop(0, local_count, drain_sums, 0)
        return carry

    lax.fori_loop(0, local_count, drain, 0)


def project(x_slices, weight, bias_pair, out_weight, counts, values, node_count, local_count):
    _, half_rows, depth = x_slices.shape
    cols = weight.shape[0]
    bits, masks = row_masks(node_count)
    group = len(masks)
    run = half_rows // local_count
    split = SPREAD_PIECES // node_count
    sums = (local_count, local_count, group * run, 2 * cols)
    dma = pltpu.SemaphoreType.DMA
    grid = (local_count, local_count)
    anywhere = pl.BlockSpec(memory_space=pl.ANY)
    vmem = pl.BlockSpec(memory_space=pltpu.VMEM)
    all_bits = len(bits_below(node_count))
    return pl.pallas_call(
        functools.partial(project_kernel, node_count, local_count),
        out_shape=[
            jax.ShapeDtypeStruct((group, half_rows, 2 * cols), jnp.bfloat16),
            jax.ShapeDtypeStruct(
                (group, local_count, 2 * cols, out_weight.shape[1]), jnp.bfloat16
            ),
            jax.ShapeDtypeStruct(counts.shape, jnp.float32),
            jax.ShapeDtypeStruct((node_count * local_count,) + values.shape, jnp.bfloat16),
        ],
        in_specs=[anywhere, anywhere, vmem, anywhere, vmem, anywhere],
        out_specs=[vmem, anywhere, vmem, anywhere],
        scratch_shapes=[
            pltpu.VMEM((local_count, group, half_rows, depth), jnp.bfloat16),
            pltpu.VMEM((2 * cols, depth), jnp.bfloat16),
            pltpu.VMEM(sums, jnp.bfloat16),
            pltpu.VMEM(sums, jnp.bfloat16),
            pltpu.VMEM(sums, jnp.bfloat16),
            pltpu.VMEM(sums[2:], jnp.float32),
            pltpu.VMEM(sums[1:], jnp.bfloat16),
            pltpu.VMEM((group, half_rows, 2 * cols), jnp.bfloat16),
            pltpu.VMEM((local_count,) + counts.shape, jnp.float32),
            dma((2,)),
            dma((3,)),
            dma((local_count, SPLITS)),
            dma((local_count, group, SPLITS)),
            dma((local_count, group, len(bits), SPLITS)),
            dma(grid),
            dma(grid),
            dma(grid),
            dma(grid),
            dma((local_count, group)),
            dma((local_count, group)),
            dma((local_count, 2, split)),
            dma((local_count, node_count, all_bits, split)),
            dma((local_count, node_count, split)),
            dma((local_count,)),
            dma((local_count,)),
            dma((local_count, 2)),
            dma((local_count, node_count, all_bits)),
            dma((local_count, node_count)),
        ],
        compiler_params=pltpu.CompilerParams(
            collective_id=0, has_side_effects=True, vmem_limit_bytes=58 * 2**20
        ),
        cost_estimate=pl.CostEstimate(
            flops=4 * local_count * group * half_rows * depth * cols,
            bytes_accessed=2 * (x_slices.size + weight.size),
            transcendentals=0,
        ),
    )(x_slices, weight, bias_pair, out_weight, counts, values)


def second_kernel(local_count, place_ref, mid_ref, own_ref, weight_ref, bias_ref, out_ref, total):
    group, _, depth = mid_ref.shape
    width = weight_ref.shape[3]
    column = lax.rem(place_ref[0] + pl.program_id(0), local_count)
    main = depth // 256 * 256

    def product(pick):
        sum_rows = jnp.zeros(total.shape, jnp.float32)
        for g in range(group):
            rhs = pick(g)
            for lower, upper in ((0, main), (main, depth)):
                if upper > lower:
                    sum_rows += jnp.dot(
                        mid_ref[g, :, lower:upper],
                        rhs[lower:upper],
                        preferred_element_type=jnp.float32,
                    )
        total[...] = sum_rows

    @pl.when(pl.program_id(0) == 0)
    def _():
        product(
            lambda g: jnp.concatenate(
                [own_ref[place_ref[1 + g]], own_ref[place_ref[1 + g] + COLUMN_BIT]], 0
            )
        )

    @pl.when(pl.program_id(0) > 0)
    def _():
        product(lambda g: weight_ref[g, 0])

    for z in range(local_count):

        @pl.when(column == z)
        def _():
            value = total[...] + bias_ref[:, z * width : (z + 1) * width]
            out_ref[...] = value.astype(jnp.bfloat16).reshape(out_ref.shape)


def second_product(places, mid, own_weight, weight, bias_row):
    group, local_count, pair_cols, width = weight.shape
    cols = pair_cols // 2
    node_count = 2 * group
    half_rows = mid.shape[1]
    joined = width % LANES == 0

    def column(z, place):
        return lax.rem(place[0] + z, local_count)

    def fetched(z, place):
        return lax.rem(place[0] + jnp.maximum(z, 1), local_count)

    if joined:
        out_shape = (half_rows, local_count * width)
        out_block = pl.BlockSpec((half_rows, width), lambda z, place: (0, column(z, place)))
    else:
        out_shape = (local_count, half_rows, width)
        out_block = pl.BlockSpec((1, half_rows, width), lambda z, place: (column(z, place), 0, 0))
    product = pl.pallas_call(
        functools.partial(second_kernel, local_count),
        grid_spec=pltpu.PrefetchScalarGridSpec(
            num_scalar_prefetch=1,
            grid=(local_count,),
            in_specs=[
                pl.BlockSpec(mid.shape, lambda z, place: (0, 0, 0)),
                pl.BlockSpec((node_count, cols, width), lambda z, place: (0, 0, 0)),
                pl.BlockSpec(
                    (group, 1, pair_cols, width), lambda z, place: (0, fetched(z, place), 0, 0)
                ),
                pl.BlockSpec((1, local_count * width + 8 * LANES), lambda z, place: (0, 0)),
            ],
            out_specs=out_block,
            scratch_shapes=[pltpu.VMEM((half_rows, width), jnp.float32)],
        ),
        out_shape=jax.ShapeDtypeStruct(out_shape, jnp.bfloat16),
        compiler_params=pltpu.CompilerParams(vmem_limit_bytes=48 * 2**20),
        cost_estimate=pl.CostEstimate(
            flops=2 * half_rows * weight.size, bytes_accessed=2 * weight.size, transcendentals=0
        ),
    )(
        places,
        mid,
        own_weight.reshape(node_count, cols, width),
        weight,
        jnp.pad(bias_row, (0, 8 * LANES))[None, :],
    )
    if joined:
        return product
    return jnp.transpose(product, (1, 0, 2)).reshape(half_rows, local_count * width)


def row_grads(hidden_f, grad_rows, weight, gain, keep):
    inv_rms = lax.rsqrt(jnp.mean(hidden_f * hidden_f, -1, keepdims=True) + 1e-06)
    unit = hidden_f * inv_rms
    normed = (unit * gain * keep).astype(jnp.bfloat16)
    grad_normed = lax.dot_general(
        grad_rows, weight, (((1,), (1,)), ((), ())), preferred_element_type=jnp.float32
    )
    part = jnp.sum(grad_normed * unit * keep, 0, keepdims=True)
    scaled = grad_normed * gain
    moment = jnp.mean(scaled * hidden_f, -1, keepdims=True)
    grad_hidden = inv_rms * scaled - hidden_f * (inv_rms * inv_rms * inv_rms * moment)
    return normed, part, grad_hidden.astype(jnp.bfloat16)


def add_part(part_ref, part):
    @pl.when(pl.program_id(0) == 0)
    def _():
        part_ref[...] = part

    @pl.when(pl.program_id(0) > 0)
    def _():
        part_ref[...] += part


def text_kernel(
    image_ref, text_ref, grad_ref, weight_ref, gain_ref, out_ref, normed_ref, part_ref
):
    count, rows, width = text_ref.shape
    first = count * pl.program_id(0)
    row = lax.broadcasted_iota(jnp.int32, (count * rows, 1), 0)
    keep = jnp.zeros(row.shape, jnp.float32)
    for i in range(count):
        held = jnp.where(image_ref[first + i] > 0, 0.0, 1.0)
        keep = jnp.where((row >= i * rows) & (row < (i + 1) * rows), held, keep)
    normed, part, grad_hidden = row_grads(
        text_ref[...].reshape(count * rows, width).astype(jnp.float32),
        grad_ref[...].reshape(count * rows, grad_ref.shape[2]),
        weight_ref[...],
        gain_ref[...],
        keep,
    )
    normed_ref[...] = normed.reshape(normed_ref.shape)
    out_ref[...] = grad_hidden.reshape(out_ref.shape)
    add_part(part_ref, part)


def image_kernel(
    block_ref,
    filled_ref,
    arrived_ref,
    grad_ref,
    weight_ref,
    gain_ref,
    text_out_ref,
    out_ref,
    normed_ref,
    part_ref,
):
    filled = filled_ref[pl.program_id(0)] > 0
    normed_ref[0], part, grad_hidden = row_grads(
        arrived_ref[0].astype(jnp.float32),
        grad_ref[0],
        weight_ref[...],
        gain_ref[...],
        jnp.where(filled, 1.0, 0.0),
    )
    add_part(part_ref, part)

    @pl.when(filled)
    def _():
        out_ref[0] = grad_hidden

    @pl.when(jnp.logical_not(filled))
    def _():
        out_ref[0] = text_out_ref[0]


def cost(steps, rows, width, values):
    return pl.CostEstimate(
        flops=2 * steps * rows * width * values,
        bytes_accessed=6 * steps * rows * width + 2 * width * values,
        transcendentals=0,
    )


def text_grads(is_image, text, value_grad, v_full, gain):
    blocks, rows, width = text.shape
    values = value_grad.shape[2]
    count = max(c for c in (1, 2) if blocks % c == 0)
    row_block = pl.BlockSpec((count, rows, width), lambda b, image: (b, 0, 0))
    one_row = pl.BlockSpec((1, width), lambda b, image: (0, 0))
    return pl.pallas_call(
        text_kernel,
        grid_spec=pltpu.PrefetchScalarGridSpec(
            num_scalar_prefetch=1,
            grid=(blocks // count,),
            in_specs=[
                row_block,
                pl.BlockSpec((count, rows, values), lambda b, image: (b, 0, 0)),
                pl.BlockSpec((width, values), lambda b, image: (0, 0)),
                one_row,
            ],
            out_specs=[row_block, row_block, one_row],
        ),
        out_shape=[
            jax.ShapeDtypeStruct((blocks, rows, width), jnp.bfloat16),
            jax.ShapeDtypeStruct((blocks, rows, width), jnp.bfloat16),
            jax.ShapeDtypeStruct((1, width), jnp.float32),
        ],
        cost_estimate=cost(blocks, rows, width, values),
    )(is_image, text, value_grad, v_full, gain)


def image_grads(block_of_piece, filled, arrived, value_grad, v_full, gain, text_out):
    pieces, rows, width = arrived.shape
    values = value_grad.shape[2]
    piece_rows = pl.BlockSpec((1, rows, width), lambda p, block, full: (p, 0, 0))
    block_rows = pl.BlockSpec((1, rows, width), lambda p, block, full: (block[p], 0, 0))
    one_row = pl.BlockSpec((1, width), lambda p, block, full: (0, 0))
    return pl.pallas_call(
        image_kernel,
        grid_spec=pltpu.PrefetchScalarGridSpec(
            num_scalar_prefetch=2,
            grid=(pieces,),
            in_specs=[
                piece_rows,
                pl.BlockSpec((1, rows, values), lambda p, block, full: (p, 0, 0)),
                pl.BlockSpec((width, values), lambda p, block, full: (0, 0)),
                one_row,
                block_rows,
            ],
            out_specs=[block_rows, piece_rows, one_row],
        ),
        out_shape=[
            jax.ShapeDtypeStruct(text_out.shape, jnp.bfloat16),
            jax.ShapeDtypeStruct((pieces, rows, width), jnp.bfloat16),
            jax.ShapeDtypeStruct((1, width), jnp.float32),
        ],
        input_output_aliases={6: 0},
        cost_estimate=cost(pieces, rows, width, values),
    )(block_of_piece, filled, arrived, value_grad, v_full, gain, text_out)


def gather_kernel(
    node_count,
    local_count,
    normed_ref,
    grad_ref,
    text_ref,
    vector_ref,
    out_ref,
    vector_out_ref,
    tot,
    pair_out,
    pair_in,
    chip_out,
    chip_in,
    line_out,
    line_in,
    vec_pair,
    vec_sum,
    vec_chip,
    vec_line,
    pair_sems,
    chip_send,
    chip_recv,
    line_send,
    line_recv,
    vec_pair_sems,
    vec_chip_send,
    vec_chip_recv,
    vec_line_send,
    vec_line_recv,
):
    node = lax.axis_index("node")
    me = lax.axis_index("local")
    chips = node_count // 2
    core = lax.rem(node, 2)
    chip = lax.div(node, 2)
    own_rows = tot.shape[1]

    barrier = pltpu.get_barrier_semaphore()
    for r in [1] + [2 * c for c in range(1, chips)]:
        pl.semaphore_signal(
            barrier, 1, device_id={"node": toggled(node, r)}, device_id_type=MESH
        )
    for step in range(1, local_count):
        pl.semaphore_signal(
            barrier, 1, device_id={"local": toggled(me, step)}, device_id_type=MESH
        )
    pl.semaphore_wait(barrier, chips + local_count - 1)

    def remote(src, dst, send, recv, axis, target):
        return pltpu.make_async_remote_copy(
            src, dst, send, recv, device_id={axis: target}, device_id_type=MESH
        )

    vec_to_pair = remote(
        vector_ref, vec_pair, vec_pair_sems.at[0], vec_pair_sems.at[1], "node", flip(node, 1)
    )
    vec_to_pair.start()

    product = lax.dot_general(
        normed_ref[...], grad_ref[...], (((0,), (0,)), ((), ())), preferred_element_type=jnp.float32
    )
    if own_rows % 8 == 0:
        tot[...] = product.reshape(tot.shape) + text_ref[...].astype(jnp.float32)
    else:
        for i in range(node_count * local_count):
            tot[i] = product[i * own_rows : (i + 1) * own_rows] + text_ref[i].astype(jnp.float32)

    def to_pair(k, q):
        return remote(
            pair_out.at[q, k],
            pair_in.at[q, k],
            pair_sems.at[0, q, k],
            pair_sems.at[1, q, k],
            "node",
            flip(node, 1),
        )

    def to_chip(q, r):
        return remote(
            chip_out.at[q, r],
            chip_in.at[q, r],
            chip_send.at[q, r],
            chip_recv.at[q, r],
            "node",
            toggled(node, 2 * r),
        )

    def to_line(step):
        return remote(
            line_out.at[step],
            line_in.at[step],
            line_send.at[step],
            line_recv.at[step],
            "local",
            toggled(me, step),
        )

    def vec_to_chip(r):
        return remote(
            vec_sum.at[0],
            vec_chip.at[chip],
            vec_chip_send.at[r],
            vec_chip_recv.at[r],
            "node",
            toggled(node, 2 * r),
        )

    def vec_to_line(step):
        return remote(
            vec_sum.at[1],
            vec_line.at[me],
            vec_line_send.at[step],
            vec_line_recv.at[step],
            "local",
            toggled(me, step),
        )

    def place(k, side, q):
        return (2 * k + side) * local_count + q

    steps = list(range(1, local_count)) + [0]
    for step in steps:
        q = toggled(me, step)
        for r in list(range(1, chips)) + [0]:
            k = toggled(chip, r)
            pair_out[q, k] = tot[place(k, 1 - core, q)].astype(jnp.bfloat16)
            to_pair(k, q).start()
    vec_to_pair.wait()
    vec_sum[0] = vector_ref[...] + vec_pair[...]
    vec_chip[chip] = vec_sum[0]
    for r in range(1, chips):
        vec_to_chip(r).start()
    for step in steps:
        q = toggled(me, step)
        for r in reversed(range(1, chips)):
            k = toggled(chip, r)
            to_pair(k, q).wait()
            chip_out[q, r] = (
                tot[place(k, core, q)] + pair_in[q, k].astype(jnp.float32)
            ).astype(jnp.bfloat16)
            to_chip(q, r).start()
        to_pair(chip, q).wait()
    for r in range(1, chips):
        source = toggled(chip, r)
        remote(
            vec_sum.at[0],
            vec_chip.at[source],
            vec_chip_send.at[r],
            vec_chip_recv.at[r],
            "node",
            toggled(node, 2 * r),
        ).wait()
    vec_total = vec_chip[0]
    for c in range(1, chips):
        vec_total += vec_chip[c]
    vec_sum[1] = vec_total
    vec_line[me] = vec_total
    for step in range(1, local_count):
        vec_to_line(step).start()
    for step in steps:
        q = toggled(me, step)
        value = tot[place(chip, core, q)] + pair_in[q, chip].astype(jnp.float32)
        for r in range(1, chips):
            to_chip(q, r).wait()
            value += chip_in[q, r].astype(jnp.float32)
        if step:
            line_out[step] = value.astype(jnp.bfloat16)
            to_line(step).start()
    for step in range(1, local_count):
        source = toggled(me, step)
        remote(
            vec_sum.at[1],
            vec_line.at[source],
            vec_line_send.at[step],
            vec_line_recv.at[step],
            "local",
            source,
        ).wait()
    vec_total = vec_line[0]
    for z in range(1, local_count):
        vec_total += vec_line[z]
    vector_out_ref[...] = vec_total / node_count
    for step in range(1, local_count):
        to_line(step).wait()
        value += line_in[step].astype(jnp.float32)
    out_ref[...] = value / node_count


def gather_grads(normed, grads, text_sum, vector, node_count, local_count):
    rows, values = text_sum.shape
    own_rows = rows // (node_count * local_count)
    chips = node_count // 2
    dma = pltpu.SemaphoreType.DMA
    tile = (own_rows, values)
    vec = vector.shape
    return pl.pallas_call(
        functools.partial(gather_kernel, node_count, local_count),
        out_shape=[
            jax.ShapeDtypeStruct(tile, jnp.float32),
            jax.ShapeDtypeStruct(vec, jnp.float32),
        ],
        in_specs=[pl.BlockSpec(memory_space=pltpu.VMEM)] * 4,
        out_specs=[pl.BlockSpec(memory_space=pltpu.VMEM)] * 2,
        scratch_shapes=[
            pltpu.VMEM((node_count * local_count,) + tile, jnp.float32),
            pltpu.VMEM((local_count, chips) + tile, jnp.bfloat16),
            pltpu.VMEM((local_count, chips) + tile, jnp.bfloat16),
            pltpu.VMEM((local_count, chips) + tile, jnp.bfloat16),
            pltpu.VMEM((local_count, chips) + tile, jnp.bfloat16),
            pltpu.VMEM((local_count,) + tile, jnp.bfloat16),
            pltpu.VMEM((local_count,) + tile, jnp.bfloat16),
            pltpu.VMEM(vec, jnp.float32),
            pltpu.VMEM((2,) + vec, jnp.float32),
            pltpu.VMEM((chips,) + vec, jnp.float32),
            pltpu.VMEM((local_count,) + vec, jnp.float32),
            dma((2, local_count, chips)),
            dma((local_count, chips)),
            dma((local_count, chips)),
            dma((local_count,)),
            dma((local_count,)),
            dma((2,)),
            dma((chips,)),
            dma((chips,)),
            dma((local_count,)),
            dma((local_count,)),
        ],
        compiler_params=pltpu.CompilerParams(
            collective_id=1, has_side_effects=True, vmem_limit_bytes=48 * 2**20
        ),
        cost_estimate=pl.CostEstimate(
            flops=2 * normed.size * values, bytes_accessed=2 * text_sum.size, transcendentals=0
        ),
    )(normed, grads, text_sum.reshape((node_count * local_count,) + tile), vector)


def weight_grad(normed, grad_rows):
    return lax.dot_general(
        normed, grad_rows, (((0,), (0,)), ((), ())), preferred_element_type=jnp.float32
    )


def per_device(
    vit_tiles,
    tile_counts,
    block_of_piece,
    segment_ids,
    text_rows,
    cotangent,
    proj_weight,
    proj_bias,
    out_weight,
    out_bias,
    ln_gain,
    ln_bias,
    norm_gain,
    v_weight,
):
    local_count = lax.axis_size("local")
    node_count = lax.axis_size("node")
    node = lax.axis_index("node")
    blocks = text_rows.shape[1]
    share_rows = text_rows.shape[2]
    model_width = text_rows.shape[3]
    out_cols = out_weight.shape[1]
    shard_cols = proj_weight.shape[1]
    x_slices = slices(vit_tiles[0, 0], ln_gain, ln_bias, local_count)
    side = lax.rem(lax.div(node, COLUMN_BIT), 2)
    low_shard = node - COLUMN_BIT * side
    bias_pair = jnp.concatenate(
        [
            lax.dynamic_slice_in_dim(proj_bias, shard * shard_cols, shard_cols, 0)
            for shard in (low_shard, low_shard + COLUMN_BIT)
        ]
    )[None, :]
    _, masks = row_masks(node_count)
    places = jnp.stack(
        [lax.axis_index("local")]
        + [toggled(low_shard, m) for m in masks]
    )
    doc_ids = segment_ids[0].reshape(-1)
    doc_hits = (doc_ids[:, None] == lax.iota(jnp.int32, DOCS)[None, :]).astype(jnp.float32)
    doc_counts = jnp.pad(jnp.sum(doc_hits, 0)[None, :], ((0, 7), (0, LANES - DOCS)))
    mid, out_spread, doc_sizes, v_full = project(
        x_slices,
        jnp.transpose(proj_weight),
        bias_pair,
        out_weight,
        doc_counts,
        v_weight,
        node_count,
        local_count,
    )
    doc_sizes = doc_sizes[0, :DOCS]
    v_full = v_full.reshape(model_width, -1)
    doc_weight = blocks * share_rows * local_count / (DOCS * doc_sizes)
    token_weight = jnp.dot(doc_hits, doc_weight, precision=lax.Precision.HIGHEST)
    value_grad = (
        cotangent[0].reshape(-1, cotangent.shape[3]).astype(jnp.float32) * token_weight[:, None]
    ).astype(jnp.bfloat16)
    bias_part = jnp.sum(value_grad.astype(jnp.float32), 0)
    piece_total = local_count // 2
    piece_ids = lax.iota(jnp.int32, piece_total)
    filled = piece_ids % SLOTS < jnp.repeat(tile_counts[0], SLOTS)
    chosen = (block_of_piece[0][None, :] == lax.iota(jnp.int32, blocks)[:, None]) & filled[None, :]
    is_image = jnp.any(chosen, 1).astype(jnp.int32)
    gain_row = norm_gain[None, :]
    value_blocks = value_grad.reshape(blocks, share_rows, -1)
    value_pieces = value_blocks[block_of_piece[0]]
    text_out, text_normed, text_part = text_grads(
        is_image, text_rows[0], value_blocks, v_full, gain_row
    )
    text_sum = weight_grad(text_normed.reshape(-1, model_width), value_grad).astype(jnp.bfloat16)
    flat_pieces = value_pieces.reshape(-1, value_pieces.shape[2])
    arrived = second_product(places, mid, out_weight, out_spread, out_bias)
    arrived = arrived.reshape(piece_total, share_rows, model_width)
    grad_hidden, image_normed, image_part = image_grads(
        block_of_piece[0], filled.astype(jnp.int32), arrived, value_pieces, v_full, gain_row, text_out
    )
    gain_part = text_part + image_part
    vector = jnp.concatenate([bias_part, gain_part[0]])
    length = vector.shape[0]
    vector = jnp.pad(vector, (0, -length % (8 * LANES))).reshape(8, -1)
    grad_weight, vector = gather_grads(
        image_normed.reshape(-1, model_width),
        flat_pieces,
        text_sum,
        vector,
        node_count,
        local_count,
    )
    vector = vector.reshape(-1)
    values = bias_part.shape[0]
    return (grad_hidden[None], grad_weight, vector[:values], vector[values:length])


def solution(mesh):
    in_specs = (
        P("node", "local", None, None),
        P("node", None),
        P("node", None),
        P("node", None, "local"),
        P("node", None, "local", None),
        P("node", None, "local", None),
        P("local", "node"),
        P(),
        P(None, "local"),
        P(),
        P(),
        P(),
        P(),
        P(("node", "local"), None),
    )
    out_specs = (P("node", None, "local", None), P(("node", "local"), None), P(), P())
    return jax.shard_map(
        per_device, mesh=mesh, in_specs=in_specs, out_specs=out_specs, check_vma=False
    )
```
